128 devices in a mesh: rep: 2 (over core), dp: 64 (over x, y, z).
Axes of the slice: x: 4, y: 4, z: 4, core: 2. Of those that a mesh axis runs over, the one named last changes fastest.
Arguments:
- x: bfloat16 [128, 2048, 896], P(('rep', 'dp')), parts along dimension 0
- dy: bfloat16 [128, 2048, 896], P(('rep', 'dp')), parts along dimension 0
- w_gate: bfloat16 [2, 896, 2304], replicated
- w_up: bfloat16 [2, 896, 2304], replicated
- w_down: bfloat16 [2, 2304, 896], replicated
- m_w_gate: float32 [2, 896, 2304], replicated
- m_w_up: float32 [2, 896, 2304], replicated
- m_w_down: float32 [2, 2304, 896], replicated
- v_w_gate: float32 [2, 896, 2304], replicated
- v_w_up: float32 [2, 896, 2304], replicated
- v_w_down: float32 [2, 2304, 896], replicated
Outputs:
- output 1: bfloat16 [4, 896, 2304], P('rep'), parts along dimension 0
- output 2: bfloat16 [4, 896, 2304], P('rep'), parts along dimension 0
- output 3: bfloat16 [4, 2304, 896], P('rep'), parts along dimension 0
- output 4: float32 [4, 896, 2304], P('rep'), parts along dimension 0
- output 5: float32 [4, 896, 2304], P('rep'), parts along dimension 0
- output 6: float32 [4, 2304, 896], P('rep'), parts along dimension 0
- output 7: float32 [4, 896, 2304], P('rep'), parts along dimension 0
- output 8: float32 [4, 896, 2304], P('rep'), parts along dimension 0
- output 9: float32 [4, 2304, 896], P('rep'), parts along dimension 0
There are 2 independent parts. The reference program is written for one: setup_inputs(seed, part) draws one part's arguments, and reference() takes and returns one part's arrays. A program takes and returns all parts, laid end to end along the dimension named above; an argument that names none is the same for every part.
All inputs are finite; a program needn't handle non-finite values.
Results may differ from the reference program's by a relative error of at most 0.022.
Values are sent between devices in bfloat16 or wider.
A program may use at most 1.5 GiB of HBM per device.

```python
import jax
import jax.numpy as jnp
from jax import lax

SEQUENCES = 64
TOKENS = 2048
D = 896
FF = 2304
LAYERS = 2
NAMES = ("w_gate", "w_up", "w_down")
SHAPES = {"w_gate": (LAYERS, D, FF), "w_up": (LAYERS, D, FF), "w_down": (LAYERS, FF, D)}


def bump(key, n, height):
    away = (jnp.arange(n, dtype=jnp.int32) - jax.random.randint(key, (), 0, n, jnp.int32)) % n
    return jnp.where(away < n // 8, height, 1.0)


def together(key, own, strength):
    shared = jax.random.normal(key, own.shape[1:], jnp.float32)
    return (own + strength * shared) * lax.rsqrt(1 + strength * strength)


def setup_inputs(seed: int = 0, part: int = 0) -> dict:
    kx, kdy, ka, kb, kz, kf, kh, kl, *keys = jax.random.split(jax.random.key(seed), 8 + 3 * len(NAMES))
    kx, kdy, ka, kb = (jax.random.fold_in(k, part) for k in (kx, kdy, ka, kb))
    kw, km, kv = (keys[i::3] for i in range(3))
    shape = (SEQUENCES, TOKENS, D)
    much_x, much_dy = jax.random.uniform(kz, (2,), jnp.float32, 0.0, 1.0)
    loud = 2.0 ** jax.random.uniform(jax.random.fold_in(kz, 1), (), jnp.float32, -1.0, 2.0)
    layers = 2.0 ** jax.random.uniform(kl, (LAYERS, 1, 1), jnp.float32, -1.0, 1.0)
    x = together(ka, jax.random.normal(kx, shape, jnp.float32), much_x) * bump(kf, D, 4.0)
    dy = together(kb, jax.random.normal(kdy, shape, jnp.float32), much_dy)
    drawn = {"x": x.astype(jnp.bfloat16), "dy": (loud * dy * (SEQUENCES * TOKENS) ** -0.5).astype(jnp.bfloat16)}
    for key, name in zip(kw, NAMES, strict=True):
        w = jax.random.normal(key, SHAPES[name], jnp.float32) * SHAPES[name][1] ** -0.5
        drawn[name] = (w * {"w_gate": 1.0, "w_up": bump(kh, FF, 4.0), "w_down": layers}[name]).astype(jnp.bfloat16)
    for key, name in zip(km, NAMES, strict=True):
        drawn[f"m_{name}"] = 0.1 * jax.random.normal(key, SHAPES[name], jnp.float32)
    for key, name in zip(kv, NAMES, strict=True):
        drawn[f"v_{name}"] = jax.random.uniform(key, SHAPES[name], jnp.float32, 0.005, 0.015)
    return drawn


def matmul(a, w):
    return jnp.dot(a, w, preferred_element_type=jnp.float32).astype(jnp.bfloat16)


def normed(h):
    wide = h.astype(jnp.float32)
    scale = lax.rsqrt(jnp.mean(wide**2, -1, keepdims=True) + 1e-6)
    return (wide * scale).astype(jnp.bfloat16)


def layer(h, w):
    a = normed(h)
    gate = jnp.dot(a, w["w_gate"], preferred_element_type=jnp.float32)
    up = jnp.dot(a, w["w_up"], preferred_element_type=jnp.float32)
    return h + matmul((jax.nn.silu(gate) * up).astype(jnp.bfloat16), w["w_down"])


def adamw(w, m, v, g):
    m = 0.9 * m + 0.1 * g
    v = 0.95 * v + 0.05 * g * g
    step = m * lax.rsqrt(v + 1e-8) + 0.1 * w
    return (w - 0.02 * step).astype(jnp.bfloat16), m, v


def clipped(gradients, sum_of_squares, count):
    factor = jnp.minimum(1.0, 0.5 * lax.rsqrt(sum_of_squares / count + 1e-30))
    return [g * factor for g in gradients]


def stack(weights, h):
    return lax.scan(lambda h, w: (layer(h, w), None), h, weights)[0]


def reference(x, dy, w_gate, w_up, w_down, m_w_gate, m_w_up, m_w_down, v_w_gate, v_w_up, v_w_down):
    weights = dict(zip(NAMES, (w_gate, w_up, w_down), strict=True))

    def take(so_far, sequence):
        h, by_y = sequence
        _, back = jax.vjp(lambda w: stack(w, h), weights)
        return jax.tree.map(lambda total, term: total + term.astype(jnp.float32), so_far, back(by_y)[0]), None

    none_yet = {name: jnp.zeros(w.shape, jnp.float32) for name, w in weights.items()}
    by_weights, _ = lax.scan(take, none_yet, (x, dy))
    gradients = [by_weights[name].astype(jnp.bfloat16).astype(jnp.float32) for name in NAMES]
    gradients = clipped(gradients, sum(jnp.sum(g * g) for g in gradients), sum(g.size for g in gradients))
    new = [
        adamw(w.astype(jnp.float32), m, v, g)
        for w, m, v, g in zip((w_gate, w_up, w_down), (m_w_gate, m_w_up, m_w_down), (v_w_gate, v_w_up, v_w_down), gradients, strict=True)
    ]
    return tuple(one[which] for which in range(3) for one in new)
```

```python
import functools

import jax
import jax.numpy as jnp
from jax import lax
from jax.experimental import pallas as pl
from jax.experimental.pallas import tpu as pltpu
from jax.sharding import PartitionSpec as P

T, D, F = 2048, 896, 2304
FB = 256
NB = F // FB
LAYERS = 2
NBLK = NB * LAYERS
COUNT = 3 * LAYERS * D * F
TM = 256
f32, bf16 = jnp.float32, jnp.bfloat16
MESH = pl.DeviceIdType.MESH
VMEM_LIMIT = 63 * 2**20
ANY = pl.BlockSpec(memory_space=pl.ANY)
VMEM = pl.BlockSpec(memory_space=pltpu.VMEM)
sds = jax.ShapeDtypeStruct


def dot(a, b):
    return jnp.dot(a, b, preferred_element_type=f32)


def dot_t(a, b):
    return lax.dot_general(a, b, (((1,), (1,)), ((), ())), preferred_element_type=f32)


def norm_scale(h):
    return lax.rsqrt(jnp.mean(h * h, -1, keepdims=True) + 1e-6)


def rows(t):
    return pl.ds(pl.multiple_of(t * TM, TM), TM)


def block(b):
    return pl.ds(pl.multiple_of(b * FB, FB), FB)


def forward(x_ref, wg, wu, wd_hbm, s_hbm, a_hbm, act_hbm, h1_ref, a0t_ref, a0, act, wgb, wub, wd, sb, ab, wsem, wdsem, osem):
    def fetch(b, slot):
        return (
            pltpu.make_async_copy(wg.at[0, :, block(b)], wgb.at[slot], wsem.at[slot, 0]),
            pltpu.make_async_copy(wu.at[0, :, block(b)], wub.at[slot], wsem.at[slot, 1]),
        )

    for c in fetch(0, 0):
        c.start()
    whole = pltpu.make_async_copy(wd_hbm.at[0], wd, wdsem)
    whole.start()

    @pl.loop(0, T // TM)
    def _(t):
        h = x_ref[rows(t), :].astype(f32)
        a0[rows(t), :] = (h * norm_scale(h)).astype(bf16)

    @pl.loop(0, T // TM)
    def _(t):
        a0t_ref[:, rows(t)] = a0[rows(t), :].T

    def outs(b, slot):
        return (
            pltpu.make_async_copy(sb.at[slot], s_hbm.at[b], osem.at[slot, 0]),
            pltpu.make_async_copy(ab.at[slot], a_hbm.at[b], osem.at[slot, 1]),
        )

    @pl.loop(0, NB)
    def _(b):
        slot = lax.rem(b, 2)

        @pl.when(b + 1 < NB)
        def _():
            for c in fetch(b + 1, 1 - slot):
                c.start()

        for c in fetch(b, slot):
            c.wait()

        @pl.when(b >= 2)
        def _():
            for c in outs(b - 2, slot):
                c.wait()

        for t in range(T // TM):
            r = pl.ds(t * TM, TM)
            gate = dot(a0[r, :], wgb[slot])
            up = dot(a0[r, :], wub[slot])
            sg = 1.0 / (1.0 + jnp.exp(-gate))
            s = gate * sg
            act[b, r, :] = (s * up).astype(bf16)
            sb[slot, r, :] = s
            ab[slot, r, :] = up * (sg + s * (1.0 - sg))
        for c in outs(b, slot):
            c.start()

    keep = pltpu.make_async_copy(act, act_hbm, wdsem)
    whole.wait()
    keep.start()

    @pl.loop(0, T // TM)
    def _(t):
        total = dot(act[0, rows(t), :], wd[0:FB, :])
        for b in range(1, NB):
            total += dot(act[b, rows(t), :], wd[b * FB : (b + 1) * FB, :])
        h1_ref[rows(t), :] = x_ref[rows(t), :] + total.astype(bf16)

    for b in (NB - 2, NB - 1):
        for c in outs(b, b % 2):
            c.wait()
    keep.wait()


def run_forward(x, wg, wu, wd):
    return pl.pallas_call(
        forward,
        name="forward",
        out_shape=(sds((NB, T, FB), f32), sds((NB, T, FB), f32), sds((NB, T, FB), bf16), sds((T, D), bf16), sds((D, T), bf16)),
        in_specs=[VMEM, ANY, ANY, ANY],
        out_specs=(ANY, ANY, ANY, VMEM, VMEM),
        scratch_shapes=[
            pltpu.VMEM((T, D), bf16),
            pltpu.VMEM((NB, T, FB), bf16),
            pltpu.VMEM((2, D, FB), bf16),
            pltpu.VMEM((2, D, FB), bf16),
            pltpu.VMEM((F, D), bf16),
            pltpu.VMEM((2, T, FB), f32),
            pltpu.VMEM((2, T, FB), f32),
            pltpu.SemaphoreType.DMA((2, 2)),
            pltpu.SemaphoreType.DMA,
            pltpu.SemaphoreType.DMA((2, 2)),
        ],
        compiler_params=pltpu.CompilerParams(vmem_limit_bytes=VMEM_LIMIT),
    )(x, wg, wu, wd)


STRIDE = (16, 4, 1)
START = (0, 3, 7, 10)
NS, NG, NL = 3, 3, 6
LAST = 14


def comm_scratch():
    def v(*shape):
        return pltpu.VMEM((*shape, 16, 128), bf16)

    return dict(
        blk=v(NS, 3, 56, 2),
        r1=v(2, 3, 2, 7, 2),
        c2=v(3, 2, 28),
        r2=v(2, 3, 2, 28),
        q1=v(2, 3, 28),
        r3a=v(2, 3, 4),
        r3b=v(2, 3, 3),
        c4=v(3, 2, 7),
        r4=v(2, 3, 2, 7),
        q2=v(2, 3, 4, 2),
        r5=v(2, 3, 2, 1),
        c6=v(3, 2, 2),
        r6=v(2, 3, 2, 2),
        g3=v(NG, 3, 4, 2),
        whole=v(NL, 3, 112),
        ssq=pltpu.VMEM((8, 128), f32),
        ssq_to=pltpu.VMEM((6, 8, 128), f32),
        ssq_from=pltpu.VMEM((6, 8, 128), f32),
        send=pltpu.SemaphoreType.DMA((12, 3, 2)),
        recv=pltpu.SemaphoreType.DMA((12, 2, 3, 2)),
        osem=pltpu.SemaphoreType.DMA((2,)),
        qsend=pltpu.SemaphoreType.DMA((6,)),
        qrecv=pltpu.SemaphoreType.DMA((6,)),
    )


def at(p, k):
    return lax.rem(p + k, 4)


def add(*terms):
    total = terms[0].astype(f32)
    for t in terms[1:]:
        total = total + t.astype(f32)
    return total


class Comm:
    def __init__(self, refs, g_hbm):
        self.__dict__.update(refs)
        self.g_hbm = g_hbm
        me = lax.axis_index("dp")
        self.pos = [lax.rem(lax.div(me, s), 4) for s in STRIDE]
        self.near = [(me - p * s + at(p, 1) * s, me - p * s + at(p, 3) * s) for p, s in zip(self.pos, STRIDE)]
        self.ssq[...] = jnp.zeros((8, 128), f32)

    def barrier(self):
        sem = pltpu.get_barrier_semaphore()
        for pair in self.near:
            for device in pair:
                pl.semaphore_signal(sem, inc=1, device_id={"dp": device}, device_id_type=MESH)
        pl.semaphore_wait(sem, 6)

    def place(self, j):
        d = tuple((j + k) % 3 for k in range(3))
        return d, tuple(self.pos[k] for k in d)

    def copies(self, stage, b):
        s, bs, gs, ws = lax.rem(b, 2), lax.rem(b, NS), lax.rem(b, NG), lax.rem(b, NL)
        out = []

        def put(j, way, d, src, dst):
            out.append(
                pltpu.make_async_remote_copy(
                    src_ref=src,
                    dst_ref=dst,
                    send_sem=self.send.at[stage - 1, j, way],
                    recv_sem=self.recv.at[stage - 1, s, j, way],
                    device_id={"dp": self.near[d][way]},
                    device_id_type=MESH,
                )
            )

        for j in range(3):
            (d0, d1, d2), (p0, p1, p2) = self.place(j)
            for w in range(2):
                back = 3 - 2 * w
                if stage == 1:
                    put(j, w, d0, self.blk.at[bs, j, pl.ds(at(p0, 2) * 14 + 7 * w, 7)], self.r1.at[s, j, w])
                elif stage == 2:
                    put(j, w, d0, self.c2.at[j, w], self.r2.at[s, j, w])
                elif stage == 3:
                    put(j, w, d1, self.q1.at[s, j, pl.ds(at(p1, 2) * 7 + 4 * w, 4 - w)], (self.r3b if w else self.r3a).at[s, j])
                elif stage == 4:
                    put(j, w, d1, self.c4.at[j, w], self.r4.at[s, j, w])
                elif stage == 5:
                    put(j, w, d2, self.q2.at[s, j, at(p2, 2), pl.ds(w, 1)], self.r5.at[s, j, w])
                elif stage == 6:
                    put(j, w, d2, self.c6.at[j, w], self.r6.at[s, j, w])
                elif stage == 7:
                    put(j, w, d2, self.g3.at[gs, j, p2], self.g3.at[gs, j, p2])
                elif stage == 8:
                    part = self.g3.at[gs, j, at(p2, back), pl.ds(w, 1)]
                    put(j, w, d2, part, part)
                else:
                    if stage == 9:
                        start, n = p0 * 28 + p1 * 7, 7
                    elif stage == 10:
                        start, n = p0 * 28 + at(p1, back) * 7 + 4 * w, 4 - w
                    elif stage == 11:
                        start, n = p0 * 28, 28
                    else:
                        start, n = at(p0, back) * 28 + 14 * w, 14
                    part = self.whole.at[ws, j, pl.ds(start, n)]
                    put(j, w, d0 if stage > 10 else d1, part, part)
        return out

    def math(self, stage, b):
        s, bs, gs, ws = lax.rem(b, 2), lax.rem(b, NS), lax.rem(b, NG), lax.rem(b, NL)
        for j in range(3):
            _, (p0, p1, p2) = self.place(j)
            if stage == 2:

                def own(k, half):
                    return self.blk[bs, j, pl.ds(at(p0, k) * 14 + 7 * half, 7)].reshape(14, 16, 128)

                def came(w):
                    return self.r1[s, j, w].reshape(14, 16, 128)

                self.c2[j, 0, 0:14] = add(own(1, 0), came(0)).astype(bf16)
                self.c2[j, 0, 14:28] = own(1, 1)
                self.c2[j, 1, 0:14] = own(3, 0)
                self.c2[j, 1, 14:28] = add(own(3, 1), came(1)).astype(bf16)
            elif stage == 3:
                mine = self.blk[bs, j, pl.ds(p0 * 14, 14)].reshape(28, 16, 128)
                self.q1[s, j] = add(mine, self.r2[s, j, 0], self.r2[s, j, 1]).astype(bf16)
            elif stage == 4:

                def own(k, start, n):
                    return self.q1[s, j, pl.ds(at(p1, k) * 7 + start, n)]

                self.c4[j, 0, 0:4] = add(own(1, 0, 4), self.r3a[s, j]).astype(bf16)
                self.c4[j, 0, 4:7] = own(1, 4, 3)
                self.c4[j, 1, 0:4] = own(3, 0, 4)
                self.c4[j, 1, 4:7] = add(own(3, 4, 3), self.r3b[s, j]).astype(bf16)
            elif stage == 5:
                total = add(self.q1[s, j, pl.ds(p1 * 7, 7)], self.r4[s, j, 0], self.r4[s, j, 1]).reshape(14, 8, 128)
                for k, start in enumerate(START):
                    self.q2[s, j, k] = total[start : start + 4].reshape(2, 16, 128).astype(bf16)
            elif stage == 6:

                def own(k, half):
                    return self.q2[s, j, at(p2, k), pl.ds(half, 1)]

                self.c6[j, 0, 0:1] = add(own(1, 0), self.r5[s, j, 0]).astype(bf16)
                self.c6[j, 0, 1:2] = own(1, 1)
                self.c6[j, 1, 0:1] = own(3, 0)
                self.c6[j, 1, 1:2] = add(own(3, 1), self.r5[s, j, 1]).astype(bf16)
            elif stage == 7:
                g = add(self.q2[s, j, p2], self.r6[s, j, 0], self.r6[s, j, 1]).astype(bf16)
                self.g3[gs, j, p2] = g
                square = g.astype(f32).reshape(4, 8, 128)
                square = square * square
                self.ssq[...] += square[0] * jnp.where(lax.rem(p2, 2) == 1, 0.0, 1.0) + square[1] + square[2] + square[3]
            elif stage == 9:
                g = self.g3[gs, j].astype(f32).reshape(4, 4, 8, 128)
                g = jnp.concatenate([g[0], g[1, 1:], g[2], g[3, 1:]], axis=0)
                self.whole[ws, j, pl.ds(p0 * 28 + p1 * 7, 7)] = g.reshape(7, 16, 128).astype(bf16)

    def out(self, b):
        return pltpu.make_async_copy(self.whole.at[lax.rem(b, NL)], self.g_hbm.at[b], self.osem.at[lax.rem(b, 2)])

    def stage(self, k, b):
        if 2 <= k <= 13:
            for c in self.copies(k - 1, b):
                c.wait()
        if k <= 12:
            self.math(k, b)
            for c in self.copies(k, b):
                c.start()
        elif k == 13:
            self.out(b).start()
        else:
            self.out(b).wait()

    def service(self, i):
        for k in range(LAST, 0, -1):
            pl.when((i >= k) & (i - k < NBLK))(functools.partial(self.stage, k, i - k))

    def total(self):
        for step in range(6):
            d, odd = divmod(step, 2)
            forth = lax.rem(self.pos[d], 2) == odd
            self.ssq_to[step] = self.ssq[...]
            c = pltpu.make_async_remote_copy(
                src_ref=self.ssq_to.at[step],
                dst_ref=self.ssq_from.at[step],
                send_sem=self.qsend.at[step],
                recv_sem=self.qrecv.at[step],
                device_id={"dp": jnp.where(forth, *self.near[d])},
                device_id_type=MESH,
            )
            c.start()
            c.wait()
            self.ssq[...] += self.ssq_from[step]


def backward(names, h1_hbm, dy_hbm, a0t_hbm, s_hbm, a_hbm, act_hbm, wg, wu, wd, g_hbm, ssq_out, *scratch):
    refs = dict(zip(names, scratch, strict=True))
    h1, dy, a, a_t, dy_t, da, wgb, wub, wdb, act, dg, du, sb, ab, isem, wsem = (refs.pop(n) for n in OWN)
    comm = Comm(refs, g_hbm)
    first = [pltpu.make_async_copy(src, dst, isem.at[k]) for k, (src, dst) in enumerate(((h1_hbm, h1), (dy_hbm, dy)))]
    for c in first:
        c.start()

    def fetch1(b, slot):
        return (
            pltpu.make_async_copy(wg.at[1, :, block(b)], wgb.at[slot], wsem.at[slot, 0]),
            pltpu.make_async_copy(wu.at[1, :, block(b)], wub.at[slot], wsem.at[slot, 1]),
            pltpu.make_async_copy(wd.at[1, block(b), :], wdb.at[slot], wsem.at[slot, 2]),
        )

    def fetch0(b, slot):
        return (
            pltpu.make_async_copy(s_hbm.at[b], sb.at[slot], wsem.at[slot, 0]),
            pltpu.make_async_copy(a_hbm.at[b], ab.at[slot], wsem.at[slot, 1]),
            pltpu.make_async_copy(act_hbm.at[b], act.at[slot], wsem.at[slot, 3]),
            pltpu.make_async_copy(wd.at[0, block(b), :], wdb.at[slot], wsem.at[slot, 2]),
        )

    for c in fetch1(0, 0):
        c.start()
    comm.barrier()
    for c in first:
        c.wait()

    @pl.loop(0, T // TM)
    def _(t):
        h = h1[rows(t), :].astype(f32)
        a[rows(t), :] = (h * norm_scale(h)).astype(bf16)

    @pl.loop(0, T // TM)
    def _(t):
        a_t[:, rows(t)] = a[rows(t), :].T
        dy_t[:, rows(t)] = dy[rows(t), :].T
        da[rows(t), :] = jnp.zeros((TM, D), f32)

    def give(slot, j, g):
        for half in range(2):
            comm.blk[slot, j, :, half] = g[:, half * 128 : (half + 1) * 128].astype(bf16).reshape(56, 16, 128)

    @pl.loop(0, NB)
    def _(b):
        comm.service(b)
        slot, to = lax.rem(b, 2), lax.rem(b, NS)

        @pl.when(b + 1 < NB)
        def _():
            for c in fetch1(b + 1, 1 - slot):
                c.start()

        for c in fetch1(b, slot):
            c.wait()
        for t in range(T // TM):
            r = pl.ds(t * TM, TM)
            gate = dot(a[r, :], wgb[slot])
            up = dot(a[r, :], wub[slot])
            dact = dot_t(dy[r, :], wdb[slot]).astype(bf16).astype(f32)
            sg = 1.0 / (1.0 + jnp.exp(-gate))
            s = gate * sg
            act[0, r, :] = (s * up).astype(bf16)
            dgate = (dact * up * (sg + s * (1.0 - sg))).astype(bf16)
            dup = (dact * s).astype(bf16)
            dg[r, :] = dgate
            du[r, :] = dup
            da[r, :] += dot_t(dgate, wgb[slot]) + dot_t(dup, wub[slot])
        give(to, 0, dot(a_t[...], dg[...]))
        give(to, 1, dot(a_t[...], du[...]))
        give(to, 2, dot(dy_t[...], act[0]))

    for c in fetch0(0, 0):
        c.start()
    last = pltpu.make_async_copy(a0t_hbm, a_t, isem.at[0])
    last.start()

    @pl.loop(0, T // TM)
    def _(t):
        h = h1[rows(t), :].astype(f32)
        scale = norm_scale(h)
        g = da[rows(t), :].astype(bf16).astype(f32)
        along = jnp.mean(g * h, -1, keepdims=True)
        dh = (g * scale - h * (scale * scale * scale * along)).astype(bf16) + dy[rows(t), :]
        dy[rows(t), :] = dh
        dy_t[:, rows(t)] = dh.T

    last.wait()

    @pl.loop(0, NB)
    def _(b):
        comm.service(b + NB)
        slot, to = lax.rem(b, 2), lax.rem(b + NB, NS)

        @pl.when(b + 1 < NB)
        def _():
            for c in fetch0(b + 1, 1 - slot):
                c.start()

        for c in fetch0(b, slot):
            c.wait()
        for t in range(T // TM):
            r = pl.ds(t * TM, TM)
            dact = dot_t(dy[r, :], wdb[slot]).astype(bf16).astype(f32)
            dg[r, :] = (dact * ab[slot, r, :]).astype(bf16)
            du[r, :] = (dact * sb[slot, r, :]).astype(bf16)
        give(to, 0, dot(a_t[...], dg[...]))
        give(to, 1, dot(a_t[...], du[...]))
        give(to, 2, dot(dy_t[...], act[slot]))

    @pl.loop(NBLK, NBLK + LAST)
    def _(i):
        comm.service(i)

    comm.total()
    ssq_out[...] = comm.ssq[...]


OWN = ("h1", "dy", "a", "a_t", "dy_t", "da", "wgb", "wub", "wdb", "act", "dg", "du", "sb", "ab", "isem", "wsem")


def run_backward(h1, dy, a0t, s, a, act, wg, wu, wd):
    own = dict(
        h1=pltpu.VMEM((T, D), bf16),
        dy=pltpu.VMEM((T, D), bf16),
        a=pltpu.VMEM((T, D), bf16),
        a_t=pltpu.VMEM((D, T), bf16),
        dy_t=pltpu.VMEM((D, T), bf16),
        da=pltpu.VMEM((T, D), f32),
        wgb=pltpu.VMEM((2, D, FB), bf16),
        wub=pltpu.VMEM((2, D, FB), bf16),
        wdb=pltpu.VMEM((2, FB, D), bf16),
        act=pltpu.VMEM((2, T, FB), bf16),
        dg=pltpu.VMEM((T, FB), bf16),
        du=pltpu.VMEM((T, FB), bf16),
        sb=pltpu.VMEM((2, T, FB), f32),
        ab=pltpu.VMEM((2, T, FB), f32),
        isem=pltpu.SemaphoreType.DMA((2,)),
        wsem=pltpu.SemaphoreType.DMA((2, 4)),
    )
    scratch = own | comm_scratch()
    return pl.pallas_call(
        functools.partial(backward, tuple(scratch)),
        name="backward",
        out_shape=(sds((NBLK, 3, 112, 16, 128), bf16), sds((8, 128), f32)),
        in_specs=[ANY] * 9,
        out_specs=(ANY, VMEM),
        scratch_shapes=list(scratch.values()),
        compiler_params=pltpu.CompilerParams(collective_id=0, has_side_effects=True, vmem_limit_bytes=VMEM_LIMIT),
    )(h1, dy, a0t, s, a, act, wg, wu, wd)


def adamw(ssq_ref, g_ref, *refs):
    factor = jnp.minimum(1.0, 0.5 * lax.rsqrt(jnp.sum(ssq_ref[...], keepdims=True) / COUNT + 1e-30))
    ins, outs = refs[:9], refs[9:]

    def update(k, where, g):
        w, m, v = (ins[i + k][where].astype(f32) for i in (0, 3, 6))
        g = g.astype(f32) * factor
        m = 0.9 * m + 0.1 * g
        v = 0.95 * v + 0.05 * g * g
        step = m * lax.rsqrt(v + 1e-8) + 0.1 * w
        outs[k][where] = (w - 0.02 * step).astype(bf16)
        outs[3 + k][where] = m
        outs[6 + k][where] = v

    @pl.loop(0, 7)
    def _(n):
        tiles = pl.ds(n * 16, 16)
        at_rows = pl.ds(pl.multiple_of(n * 128, 128), 128)
        for k in range(3):
            g = g_ref[0, k, tiles].reshape(8, 2, 16, 128)
            for half in range(2):
                cols = pl.ds(half * 128, 128)
                part = g[:, half].reshape(128, 128)
                if k < 2:
                    update(k, (0, at_rows, cols), part)
                else:
                    update(k, (0, cols, at_rows), part.astype(f32).T)


def run_adamw(ssq, g, *arrays):
    def of(i):
        return 1 - i // NB, i % NB

    wide = pl.BlockSpec((1, D, FB), lambda i: (of(i)[0], 0, of(i)[1]))
    tall = pl.BlockSpec((1, FB, D), lambda i: (of(i)[0], of(i)[1], 0))
    specs = [wide, wide, tall] * 3
    return pl.pallas_call(
        adamw,
        name="adamw",
        grid=(NBLK,),
        out_shape=tuple(sds(a.shape, a.dtype) for a in arrays),
        in_specs=[pl.BlockSpec((8, 128), lambda i: (0, 0)), pl.BlockSpec((1, 3, 112, 16, 128), lambda i: (i, 0, 0, 0, 0))] + specs,
        out_specs=tuple(specs),
        compiler_params=pltpu.CompilerParams(vmem_limit_bytes=VMEM_LIMIT, dimension_semantics=("arbitrary",)),
    )(ssq, g, *arrays)


def solution(mesh):
    def step(x, dy, *arrays):
        wg, wu, wd = arrays[:3]
        s, a, act, h1, a0t = run_forward(x[0], wg, wu, wd)
        g, ssq = run_backward(h1, dy[0], a0t, s, a, act, wg, wu, wd)
        return run_adamw(ssq, g, *arrays)

    return jax.shard_map(
        step,
        mesh=mesh,
        in_specs=(P(("rep", "dp"), None, None),) * 2 + (P(None, None, None),) * 9,
        out_specs=(P("rep", None, None),) * 9,
        check_vma=False,
    )
```

```python
import functools

import jax
import jax.numpy as jnp
from jax import lax
from jax.experimental import pallas as pl
from jax.experimental.pallas import tpu as pltpu
from jax.sharding import PartitionSpec as P

T, D, F = 2048, 896, 2304
FB = 256
NB = F // FB
LAYERS = 2
NBLK = NB * LAYERS
COUNT = 3 * LAYERS * D * F
TM = 256
f32, bf16 = jnp.float32, jnp.bfloat16
MESH = pl.DeviceIdType.MESH
VMEM_LIMIT = 63 * 2**20
ANY = pl.BlockSpec(memory_space=pl.ANY)
VMEM = pl.BlockSpec(memory_space=pltpu.VMEM)
sds = jax.ShapeDtypeStruct


def dot(a, b):
    return jnp.dot(a, b, preferred_element_type=f32)


def dot_t(a, b):
    return lax.dot_general(a, b, (((1,), (1,)), ((), ())), preferred_element_type=f32)


def norm_scale(h):
    return lax.rsqrt(jnp.mean(h * h, -1, keepdims=True) + 1e-6)


def rows(t):
    return pl.ds(pl.multiple_of(t * TM, TM), TM)


def block(b):
    return pl.ds(pl.multiple_of(b * FB, FB), FB)


def forward(x_ref, dy_ref, wg, wu, wd_hbm, s_hbm, a_hbm, act_hbm, h1_hbm, a0t_hbm, a1_hbm, a1t_hbm, dyt_hbm, a0, act, wgu, wd, sb, ab, h1, a0t, a1, a1t, dyt, wsem, wdsem, osem, tsem):
    def fetch(b, slot):
        return (
            pltpu.make_async_copy(wg.at[0, :, block(b)], wgu.at[slot, :, 0:FB], wsem.at[slot, 0]),
            pltpu.make_async_copy(wu.at[0, :, block(b)], wgu.at[slot, :, FB : 2 * FB], wsem.at[slot, 1]),
        )

    for c in fetch(0, 0):
        c.start()
    whole = pltpu.make_async_copy(wd_hbm.at[0], wd, wdsem)
    whole.start()

    @pl.loop(0, T // TM)
    def _(t):
        h = x_ref[rows(t), :].astype(f32)
        a0[rows(t), :] = (h * norm_scale(h)).astype(bf16)

    def outs(b, slot):
        return (
            pltpu.make_async_copy(sb.at[slot], s_hbm.at[b], osem.at[slot, 0]),
            pltpu.make_async_copy(ab.at[slot], a_hbm.at[b], osem.at[slot, 1]),
        )

    @pl.loop(0, NB)
    def _(b):
        slot = lax.rem(b, 2)

        @pl.when(b + 1 < NB)
        def _():
            for c in fetch(b + 1, 1 - slot):
                c.start()

        for c in fetch(b, slot):
            c.wait()

        @pl.when(b >= 2)
        def _():
            for c in outs(b - 2, slot):
                c.wait()

        turn = rows(jnp.minimum(b, T // TM - 1))
        a0t[:, turn] = a0[turn, :].T
        dyt[:, turn] = dy_ref[turn, :].T
        for t in range(T // TM):
            r = pl.ds(t * TM, TM)
            both = dot(a0[r, :], wgu[slot])
            gate, up = both[:, :FB], both[:, FB:]
            sg = 1.0 / (1.0 + jnp.exp(-gate))
            s = gate * sg
            act[r, block(b)] = (s * up).astype(bf16)
            sb[slot, r, :] = s
            ab[slot, r, :] = up * (sg + s * (1.0 - sg))
        for c in outs(b, slot):
            c.start()

    keep = [pltpu.make_async_copy(src, dst, tsem.at[k]) for k, (src, dst) in enumerate(((act, act_hbm), (a0t, a0t_hbm), (dyt, dyt_hbm)))]
    for c in keep:
        c.start()
    whole.wait()

    def tail(t):
        return (
            pltpu.make_async_copy(h1.at[rows(t), :], h1_hbm.at[rows(t), :], tsem.at[3]),
            pltpu.make_async_copy(a1.at[rows(t), :], a1_hbm.at[rows(t), :], tsem.at[4]),
            pltpu.make_async_copy(a1t.at[:, rows(t)], a1t_hbm.at[:, rows(t)], tsem.at[5]),
        )

    @pl.loop(0, T // TM)
    def _(t):
        h = x_ref[rows(t), :] + dot(act[rows(t), :], wd[...]).astype(bf16)
        h1[rows(t), :] = h
        h = h.astype(f32)
        n = (h * norm_scale(h)).astype(bf16)
        a1[rows(t), :] = n
        a1t[:, rows(t)] = n.T

        @pl.when(t > 0)
        def _():
            for c in tail(t - 1):
                c.wait()

        for c in tail(t):
            c.start()

    for c in tail(T // TM - 1):
        c.wait()
    for b in (NB - 2, NB - 1):
        for c in outs(b, b % 2):
            c.wait()
    for c in keep:
        c.wait()


def run_forward(x, dy, wg, wu, wd):
    wide, tall = (T, D), (D, T)
    return pl.pallas_call(
        forward,
        name="forward",
        out_shape=(sds((NB, T, FB), f32), sds((NB, T, FB), f32), sds((T, F), bf16), *(sds(s, bf16) for s in (wide, tall, wide, tall, tall))),
        in_specs=[VMEM, VMEM, ANY, ANY, ANY],
        out_specs=(ANY,) * 8,
        scratch_shapes=[
            pltpu.VMEM(wide, bf16),
            pltpu.VMEM((T, F), bf16),
            pltpu.VMEM((2, D, 2 * FB), bf16),
            pltpu.VMEM((F, D), bf16),
            pltpu.VMEM((2, T, FB), f32),
            pltpu.VMEM((2, T, FB), f32),
            *(pltpu.VMEM(s, bf16) for s in (wide, tall, wide, tall, tall)),
            pltpu.SemaphoreType.DMA((2, 2)),
            pltpu.SemaphoreType.DMA,
            pltpu.SemaphoreType.DMA((2, 2)),
            pltpu.SemaphoreType.DMA((6,)),
        ],
        compiler_params=pltpu.CompilerParams(vmem_limit_bytes=VMEM_LIMIT),
    )(x, dy, wg, wu, wd)


STRIDE = (16, 4, 1)
START = (0, 3, 7, 10)
NS, NG, NL = 3, 3, 6
SUMMED, LAST = 6, 12


def ready(b):
    return 2 * b + 1 if b < NB else NB + b


END = ready(NBLK - 1)


def comm_scratch():
    def v(*shape):
        return pltpu.VMEM((*shape, 16, 128), bf16)

    return dict(
        blk=v(NS, 3, 56, 2),
        r1=v(2, 3, 2, 7, 2),
        c2=v(3, 2, 28),
        r2=v(2, 3, 2, 28),
        q1=v(2, 3, 28),
        r3a=v(2, 3, 4),
        r3b=v(2, 3, 3),
        c4=v(3, 2, 7),
        r4=v(2, 3, 2, 7),
        q2=v(2, 3, 4, 2),
        r5=v(2, 3, 3, 2),
        g3=v(NG, 3, 4, 2),
        whole=v(NL, 3, 112),
        ssq=pltpu.VMEM((8, 128), f32),
        ssq_to=pltpu.VMEM((6, 8, 128), f32),
        ssq_from=pltpu.VMEM((6, 8, 128), f32),
        send=pltpu.SemaphoreType.DMA((10, 3, 2)),
        recv=pltpu.SemaphoreType.DMA((10, 2, 3, 2)),
        send3=pltpu.SemaphoreType.DMA((2, 2, 3, 3)),
        recv3=pltpu.SemaphoreType.DMA((2, 3, 3, 3)),
        osem=pltpu.SemaphoreType.DMA((2,)),
        qsend=pltpu.SemaphoreType.DMA((6,)),
        qrecv=pltpu.SemaphoreType.DMA((6,)),
    )


def at(p, k):
    return lax.rem(p + k, 4)


def add(*terms):
    total = terms[0].astype(f32)
    for t in terms[1:]:
        total = total + t.astype(f32)
    return total


class Comm:
    def __init__(self, refs, g_hbm):
        self.__dict__.update(refs)
        self.g_hbm = g_hbm
        me = lax.axis_index("dp")
        self.pos = [lax.rem(lax.div(me, s), 4) for s in STRIDE]
        self.near = [tuple(me - p * s + at(p, k) * s for k in (1, 3, 2)) for p, s in zip(self.pos, STRIDE)]
        self.ssq[...] = jnp.zeros((8, 128), f32)

    def barrier(self):
        sem = pltpu.get_barrier_semaphore()
        for ring in self.near:
            for device in ring:
                pl.semaphore_signal(sem, inc=1, device_id={"dp": device}, device_id_type=MESH)
        pl.semaphore_wait(sem, 9)

    def place(self, j):
        d = tuple((j + k) % 3 for k in range(3))
        return d, tuple(self.pos[k] for k in d)

    def copies(self, stage, b):
        s, bs, gs, ws = lax.rem(b, 2), lax.rem(b, NS), lax.rem(b, NG), lax.rem(b, NL)
        out = []

        def put(j, way, d, src, dst):
            if stage in (5, 6):
                send, recv = self.send3.at[stage - 5, s, j, way], self.recv3.at[stage - 5, lax.rem(b, 3), j, way]
            else:
                send, recv = self.send.at[stage - 1, j, way], self.recv.at[stage - 1, s, j, way]
            device = {"dp": self.near[d][way]}
            out.append(pltpu.make_async_remote_copy(src_ref=src, dst_ref=dst, send_sem=send, recv_sem=recv, device_id=device, device_id_type=MESH))

        for j in range(3):
            (d0, d1, d2), (p0, p1, p2) = self.place(j)
            if stage in (5, 6):
                for w, k in enumerate((1, 3, 2)):
                    if stage == 5:
                        put(j, w, d2, self.q2.at[s, j, at(p2, k)], self.r5.at[s, j, w])
                    else:
                        put(j, w, d2, self.g3.at[gs, j, p2], self.g3.at[gs, j, p2])
                continue
            for w in range(2):
                back = 3 - 2 * w
                if stage == 1:
                    put(j, w, d0, self.blk.at[bs, j, pl.ds(at(p0, 2) * 14 + 7 * w, 7)], self.r1.at[s, j, w])
                elif stage == 2:
                    put(j, w, d0, self.c2.at[j, w], self.r2.at[s, j, w])
                elif stage == 3:
                    put(j, w, d1, self.q1.at[s, j, pl.ds(at(p1, 2) * 7 + 4 * w, 4 - w)], (self.r3b if w else self.r3a).at[s, j])
                elif stage == 4:
                    put(j, w, d1, self.c4.at[j, w], self.r4.at[s, j, w])
                else:
                    if stage == 7:
                        start, n = p0 * 28 + p1 * 7, 7
                    elif stage == 8:
                        start, n = p0 * 28 + at(p1, back) * 7 + 4 * w, 4 - w
                    elif stage == 9:
                        start, n = p0 * 28, 28
                    else:
                        start, n = at(p0, back) * 28 + 14 * w, 14
                    part = self.whole.at[ws, j, pl.ds(start, n)]
                    put(j, w, d0 if stage > 8 else d1, part, part)
        return out

    def math(self, stage, b):
        s, bs, gs, ws = lax.rem(b, 2), lax.rem(b, NS), lax.rem(b, NG), lax.rem(b, NL)
        for j in range(3):
            _, (p0, p1, p2) = self.place(j)
            if stage == 2:

                def own(k, half):
                    return self.blk[bs, j, pl.ds(at(p0, k) * 14 + 7 * half, 7)].reshape(14, 16, 128)

                def came(w):
                    return self.r1[s, j, w].reshape(14, 16, 128)

                self.c2[j, 0, 0:14] = add(own(1, 0), came(0)).astype(bf16)
                self.c2[j, 0, 14:28] = own(1, 1)
                self.c2[j, 1, 0:14] = own(3, 0)
                self.c2[j, 1, 14:28] = add(own(3, 1), came(1)).astype(bf16)
            elif stage == 3:
                mine = self.blk[bs, j, pl.ds(p0 * 14, 14)].reshape(28, 16, 128)
                self.q1[s, j] = add(mine, self.r2[s, j, 0], self.r2[s, j, 1]).astype(bf16)
            elif stage == 4:

                def own(k, start, n):
                    return self.q1[s, j, pl.ds(at(p1, k) * 7 + start, n)]

                self.c4[j, 0, 0:4] = add(own(1, 0, 4), self.r3a[s, j]).astype(bf16)
                self.c4[j, 0, 4:7] = own(1, 4, 3)
                self.c4[j, 1, 0:4] = own(3, 0, 4)
                self.c4[j, 1, 4:7] = add(own(3, 4, 3), self.r3b[s, j]).astype(bf16)
            elif stage == 5:
                total = add(self.q1[s, j, pl.ds(p1 * 7, 7)], self.r4[s, j, 0], self.r4[s, j, 1]).reshape(14, 8, 128)
                for k, start in enumerate(START):
                    self.q2[s, j, k] = total[start : start + 4].reshape(2, 16, 128).astype(bf16)
            elif stage == 6:
                g = add(self.q2[s, j, p2], *(self.r5[s, j, w] for w in range(3))).astype(bf16)
                self.g3[gs, j, p2] = g
                square = g.astype(f32).reshape(4, 8, 128)
                square = square * square
                self.ssq[...] += square[0] * jnp.where(lax.rem(p2, 2) == 1, 0.0, 1.0) + square[1] + square[2] + square[3]
            elif stage == 7:
                g = self.g3[gs, j].astype(f32).reshape(4, 4, 8, 128)
                g = jnp.concatenate([g[0], g[1, 1:], g[2], g[3, 1:]], axis=0)
                self.whole[ws, j, pl.ds(p0 * 28 + p1 * 7, 7)] = g.reshape(7, 16, 128).astype(bf16)

    def out(self, b):
        return pltpu.make_async_copy(self.whole.at[lax.rem(b, NL)], self.g_hbm.at[b], self.osem.at[lax.rem(b, 2)])

    def stage(self, k, b):
        if 2 <= k <= 11:
            for c in self.copies(k - 1, b):
                c.wait()
        if k <= 10:
            self.math(k, b)
            for c in self.copies(k, b):
                c.start()
        elif k == 11:
            self.out(b).start()
        else:
            self.out(b).wait()

    def due(self, tick, low, high):
        for k in range(high, low - 1, -1):
            u = tick - k
            late = u >= ready(NB)
            now = (u >= ready(0)) & (u <= END) & (late | (lax.rem(u, 2) == 1))
            pl.when(now)(functools.partial(self.stage, k, jnp.where(late, u - NB, lax.div(u, 2))))

    def scatter(self, tick):
        self.due(tick, 1, SUMMED)

    def gather(self, tick):
        self.due(tick, SUMMED + 1, LAST)

    def total(self, step):
        def copy(step):
            d, odd = divmod(step, 2)
            peer = jnp.where(lax.rem(self.pos[d], 2) == odd, *self.near[d][:2])
            return pltpu.make_async_remote_copy(
                src_ref=self.ssq_to.at[step],
                dst_ref=self.ssq_from.at[step],
                send_sem=self.qsend.at[step],
                recv_sem=self.qrecv.at[step],
                device_id={"dp": peer},
                device_id_type=MESH,
            )

        if step > 0:
            copy(step - 1).wait()
            self.ssq[...] += self.ssq_from[step - 1]
        if step < 6:
            self.ssq_to[step] = self.ssq[...]
            copy(step).start()


def backward(names, h1_hbm, dy_hbm, a0t_hbm, s_hbm, a_hbm, act_hbm, a1_hbm, a1t_hbm, dyt_hbm, wg, wu, wd, g_hbm, ssq_out, *scratch):
    refs = dict(zip(names, scratch, strict=True))
    h1, dy, a, a_t, dy_t, da, wgu, wdb, act, dgu, sb, ab, isem, wsem = (refs.pop(n) for n in OWN)
    comm = Comm(refs, g_hbm)
    first = [
        pltpu.make_async_copy(src, dst, isem.at[k]) for k, (src, dst) in enumerate(((a1_hbm, a), (dy_hbm, dy), (a1t_hbm, a_t), (dyt_hbm, dy_t), (h1_hbm, h1)))
    ]

    def fetch1(b, slot):
        return (
            pltpu.make_async_copy(wg.at[1, :, block(b)], wgu.at[slot, :, 0:FB], wsem.at[slot, 0]),
            pltpu.make_async_copy(wu.at[1, :, block(b)], wgu.at[slot, :, FB : 2 * FB], wsem.at[slot, 1]),
            pltpu.make_async_copy(wd.at[1, block(b), :], wdb.at[slot], wsem.at[slot, 2]),
        )

    def fetch0(b, slot):
        return (
            pltpu.make_async_copy(s_hbm.at[b], sb.at[slot], wsem.at[slot, 0]),
            pltpu.make_async_copy(a_hbm.at[b], ab.at[slot], wsem.at[slot, 1]),
            pltpu.make_async_copy(act_hbm.at[:, block(b)], act.at[slot], wsem.at[slot, 3]),
            pltpu.make_async_copy(wd.at[0, block(b), :], wdb.at[slot], wsem.at[slot, 2]),
        )

    for c in fetch1(0, 0):
        c.start()
    for c in first:
        c.start()

    @pl.loop(0, T // TM)
    def _(t):
        da[rows(t), :] = jnp.zeros((TM, D), f32)

    comm.barrier()
    for c in first:
        c.wait()

    def give(slot, j, g):
        for half in range(2):
            comm.blk[slot, j, :, half] = g[:, half * 128 : (half + 1) * 128].astype(bf16).reshape(56, 16, 128)

    @pl.loop(0, NB)
    def _(b):
        slot, to = lax.rem(b, 2), lax.rem(b, NS)

        def tokens(tiles):
            for t in tiles:
                r = pl.ds(t * TM, TM)
                both = dot(a[r, :], wgu[slot])
                gate, up = both[:, :FB], both[:, FB:]
                dact = dot_t(dy[r, :], wdb[slot]).astype(bf16).astype(f32)
                sg = 1.0 / (1.0 + jnp.exp(-gate))
                s = gate * sg
                act[0, r, :] = (s * up).astype(bf16)
                dgu[r, :FB] = (dact * up * (sg + s * (1.0 - sg))).astype(bf16)
                dgu[r, FB:] = (dact * s).astype(bf16)
                da[r, :] += dot_t(dgu[r, :], wgu[slot])

        comm.scatter(2 * b)

        @pl.when(b + 1 < NB)
        def _():
            for c in fetch1(b + 1, 1 - slot):
                c.start()

        for c in fetch1(b, slot):
            c.wait()
        tokens(range(0, T // TM // 2))
        comm.gather(2 * b)
        tokens(range(T // TM // 2, T // TM))
        comm.scatter(2 * b + 1)
        both = dot(a_t[...], dgu[...])
        give(to, 0, both[:, :FB])
        give(to, 1, both[:, FB:])
        comm.gather(2 * b + 1)
        give(to, 2, dot(dy_t[...], act[0]))

    for c in fetch0(0, 0):
        c.start()
    last = pltpu.make_async_copy(a0t_hbm, a_t, isem.at[0])
    last.start()

    @pl.loop(0, T // TM)
    def _(t):
        h = h1[rows(t), :].astype(f32)
        scale = norm_scale(h)
        g = da[rows(t), :].astype(bf16).astype(f32)
        along = jnp.mean(g * h, -1, keepdims=True)
        dh = (g * scale - h * (scale * scale * scale * along)).astype(bf16) + dy[rows(t), :]
        dy[rows(t), :] = dh
        dy_t[:, rows(t)] = dh.T

    last.wait()

    @pl.loop(0, NB)
    def _(b):
        tick = b + 2 * NB
        comm.scatter(tick)
        slot, to = lax.rem(b, 2), lax.rem(b + NB, NS)

        @pl.when(b + 1 < NB)
        def _():
            for c in fetch0(b + 1, 1 - slot):
                c.start()

        for c in fetch0(b, slot):
            c.wait()
        for t in range(T // TM):
            r = pl.ds(t * TM, TM)
            dact = dot_t(dy[r, :], wdb[slot]).astype(bf16).astype(f32)
            dgu[r, :FB] = (dact * ab[slot, r, :]).astype(bf16)
            dgu[r, FB:] = (dact * sb[slot, r, :]).astype(bf16)
        give(to, 2, dot(dy_t[...], act[slot]))
        comm.gather(tick)
        both = dot(a_t[...], dgu[...])
        give(to, 0, both[:, :FB])
        give(to, 1, both[:, FB:])

    @pl.loop(END + 1, END + LAST + 1)
    def _(tick):
        comm.scatter(tick)
        comm.gather(tick)
        for step in range(7):
            pl.when(tick == END + SUMMED + step)(functools.partial(comm.total, step))

    ssq_out[...] = comm.ssq[...]


OWN = ("h1", "dy", "a", "a_t", "dy_t", "da", "wgu", "wdb", "act", "dgu", "sb", "ab", "isem", "wsem")


def run_backward(*args):
    own = dict(
        h1=pltpu.VMEM((T, D), bf16),
        dy=pltpu.VMEM((T, D), bf16),
        a=pltpu.VMEM((T, D), bf16),
        a_t=pltpu.VMEM((D, T), bf16),
        dy_t=pltpu.VMEM((D, T), bf16),
        da=pltpu.VMEM((T, D), f32),
        wgu=pltpu.VMEM((2, D, 2 * FB), bf16),
        wdb=pltpu.VMEM((2, FB, D), bf16),
        act=pltpu.VMEM((2, T, FB), bf16),
        dgu=pltpu.VMEM((T, 2 * FB), bf16),
        sb=pltpu.VMEM((2, T, FB), f32),
        ab=pltpu.VMEM((2, T, FB), f32),
        isem=pltpu.SemaphoreType.DMA((5,)),
        wsem=pltpu.SemaphoreType.DMA((2, 4)),
    )
    scratch = own | comm_scratch()
    return pl.pallas_call(
        functools.partial(backward, tuple(scratch)),
        name="backward",
        out_shape=(sds((NBLK, 3, 112, 16, 128), bf16), sds((8, 128), f32)),
        in_specs=[ANY] * 12,
        out_specs=(ANY, VMEM),
        scratch_shapes=list(scratch.values()),
        compiler_params=pltpu.CompilerParams(collective_id=0, has_side_effects=True, vmem_limit_bytes=VMEM_LIMIT),
    )(*args)


def adamw(ssq_ref, g_ref, *refs):
    factor = jnp.minimum(1.0, 0.5 * lax.rsqrt(jnp.sum(ssq_ref[...], keepdims=True) / COUNT + 1e-30))
    ins, outs = refs[:9], refs[9:]

    @pl.loop(0, NB)
    def _(b):
        for k in range(3):
            tiles = g_ref[b, k].reshape(8, 2, 16, 128)
            for half in range(2):
                g = tiles[:, half].reshape(128, 128)
                units = pl.ds(pl.multiple_of(b * FB + half * 128, 128), 128)
                where = (0, slice(None), units)
                if k == 2:
                    g, where = g.T, (0, units, slice(None))
                w, m, v = (ins[i + k][where].astype(f32) for i in (0, 3, 6))
                g = g.astype(f32) * factor
                m = 0.9 * m + 0.1 * g
                v = 0.95 * v + 0.05 * g * g
                step = m * lax.rsqrt(v + 1e-8) + 0.1 * w
                outs[k][where] = (w - 0.02 * step).astype(bf16)
                outs[3 + k][where] = m
                outs[6 + k][where] = v


def run_adamw(ssq, g, *arrays):
    wide = pl.BlockSpec((1, 128, F), lambda n, i: (1 - n, i, 0))
    tall = pl.BlockSpec((1, F, 128), lambda n, i: (1 - n, 0, i))
    specs = [wide, wide, tall] * 3
    return pl.pallas_call(
        adamw,
        name="adamw",
        grid=(LAYERS, D // 128),
        out_shape=tuple(sds(a.shape, a.dtype) for a in arrays),
        in_specs=[pl.BlockSpec((8, 128), lambda n, i: (0, 0)), pl.BlockSpec((NB, 3, 16, 16, 128), lambda n, i: (n, 0, i, 0, 0))] + specs,
        out_specs=tuple(specs),
        compiler_params=pltpu.CompilerParams(vmem_limit_bytes=VMEM_LIMIT, dimension_semantics=("arbitrary", "arbitrary")),
    )(ssq, g, *arrays)


def solution(mesh):
    def step(x, dy, *arrays):
        wg, wu, wd = arrays[:3]
        s, a, act, h1, a0t, a1, a1t, dyt = run_forward(x[0], dy[0], wg, wu, wd)
        g, ssq = run_backward(h1, dy[0], a0t, s, a, act, a1, a1t, dyt, wg, wu, wd)
        return run_adamw(ssq, g, *arrays)

    return jax.shard_map(
        step,
        mesh=mesh,
        in_specs=(P(("rep", "dp"), None, None),) * 2 + (P(None, None, None),) * 9,
        out_specs=(P("rep", None, None),) * 9,
        check_vma=False,
    )
```

```python
import functools

import jax
import jax.numpy as jnp
from jax import lax
from jax.experimental import pallas as pl
from jax.experimental.pallas import tpu as pltpu
from jax.sharding import PartitionSpec as P

T, D, F = 2048, 896, 2304
FB = 256
NB = F // FB
LAYERS = 2
NBLK = NB * LAYERS
COUNT = 3 * LAYERS * D * F
TM = 256
NT = T // TM
f32, bf16 = jnp.float32, jnp.bfloat16
MESH = pl.DeviceIdType.MESH
VMEM_LIMIT = 63 * 2**20
ANY = pl.BlockSpec(memory_space=pl.ANY)
VMEM = pl.BlockSpec(memory_space=pltpu.VMEM)
sds = jax.ShapeDtypeStruct


def dot(a, b):
    return jnp.dot(a, b, preferred_element_type=f32)


def dot_t(a, b):
    return lax.dot_general(a, b, (((1,), (1,)), ((), ())), preferred_element_type=f32)


def sigmoid(x):
    return 1.0 / (1.0 + jnp.exp(-x))


def norm_scale(h):
    return lax.rsqrt(jnp.mean(h * h, -1, keepdims=True) + 1e-6)


def rows(t):
    return pl.ds(pl.multiple_of(t * TM, TM), TM)


def block(b):
    return pl.ds(pl.multiple_of(b * FB, FB), FB)


def forward(x_hbm, dy_hbm, wg, wu, wd_hbm, s_hbm, a_hbm, act_hbm, h1_hbm, a0t_hbm, a1_hbm, a1t_hbm, dyt_hbm, *scratch):
    x, dy, a0, act, wgu, wd, sb, ab, h1, a0t, a1, a1t, dyt, xsem, isem, wsem, osem, tsem = scratch

    def fetch(b, slot):
        return (
            pltpu.make_async_copy(wg.at[0, :, block(b)], wgu.at[slot, :, 0:FB], wsem.at[slot, 0]),
            pltpu.make_async_copy(wu.at[0, :, block(b)], wgu.at[slot, :, FB : 2 * FB], wsem.at[slot, 1]),
        )

    def part(t):
        return pltpu.make_async_copy(x_hbm.at[rows(t), :], x.at[rows(t), :], xsem.at[t])

    for t in range(NT):
        part(t).start()
    for c in fetch(0, 0):
        c.start()
    get_dy = pltpu.make_async_copy(dy_hbm, dy, isem.at[0])
    get_dy.start()
    get_wd = pltpu.make_async_copy(wd_hbm.at[0], wd, isem.at[1])
    get_wd.start()

    @pl.loop(0, NT)
    def _(t):
        part(t).wait()
        h = x[rows(t), :].astype(f32)
        a0[rows(t), :] = (h * norm_scale(h)).astype(bf16)

    get_dy.wait()

    def outs(b, slot):
        return (
            pltpu.make_async_copy(sb.at[slot], s_hbm.at[b], osem.at[slot, 0]),
            pltpu.make_async_copy(ab.at[slot], a_hbm.at[b], osem.at[slot, 1]),
        )

    @pl.loop(0, NB)
    def _(b):
        slot = lax.rem(b, 2)

        @pl.when(b + 1 < NB)
        def _():
            for c in fetch(b + 1, 1 - slot):
                c.start()

        @pl.when(b >= 2)
        def _():
            for c in outs(b - 2, slot):
                c.wait()

        for c in fetch(b, slot):
            c.wait()
        turn = rows(jnp.minimum(b, NT - 1))
        a0t[:, turn] = a0[turn, :].T
        dyt[:, turn] = dy[turn, :].T
        for t in range(NT):
            r = pl.ds(t * TM, TM)
            both = dot(a0[r, :], wgu[slot])
            gate, up = both[:, :FB], both[:, FB:]
            sg = sigmoid(gate)
            s = gate * sg
            act[r, block(b)] = (s * up).astype(bf16)
            sb[slot, r, :] = s
            ab[slot, r, :] = up * (sg + (s - s * sg))
        for c in outs(b, slot):
            c.start()

    keep = [pltpu.make_async_copy(src, dst, tsem.at[k]) for k, (src, dst) in enumerate(((act, act_hbm), (a0t, a0t_hbm), (dyt, dyt_hbm)))]
    for c in keep:
        c.start()
    get_wd.wait()
    for t in range(NT):
        r = pl.ds(t * TM, TM)
        h = x[r, :] + dot(act[r, :], wd[...]).astype(bf16)
        h1[r, :] = h
        h = h.astype(f32)
        n = (h * norm_scale(h)).astype(bf16)
        a1[r, :] = n
        a1t[:, r] = n.T
    tail = [pltpu.make_async_copy(src, dst, tsem.at[3 + k]) for k, (src, dst) in enumerate(((h1, h1_hbm), (a1, a1_hbm), (a1t, a1t_hbm)))]
    for c in tail:
        c.start()
    for b in (NB - 2, NB - 1):
        for c in outs(b, b % 2):
            c.wait()
    for c in keep + tail:
        c.wait()


def run_forward(x, dy, wg, wu, wd):
    wide, tall = (T, D), (D, T)
    return pl.pallas_call(
        forward,
        name="forward",
        out_shape=(sds((NB, T, FB), f32), sds((NB, T, FB), f32), sds((T, F), bf16), *(sds(s, bf16) for s in (wide, tall, wide, tall, tall))),
        in_specs=[ANY] * 5,
        out_specs=(ANY,) * 8,
        scratch_shapes=[
            pltpu.VMEM(wide, bf16),
            pltpu.VMEM(wide, bf16),
            pltpu.VMEM(wide, bf16),
            pltpu.VMEM((T, F), bf16),
            pltpu.VMEM((2, D, 2 * FB), bf16),
            pltpu.VMEM((F, D), bf16),
            pltpu.VMEM((2, T, FB), f32),
            pltpu.VMEM((2, T, FB), f32),
            *(pltpu.VMEM(s, bf16) for s in (wide, tall, wide, tall, tall)),
            pltpu.SemaphoreType.DMA((NT,)),
            pltpu.SemaphoreType.DMA((2,)),
            pltpu.SemaphoreType.DMA((2, 2)),
            pltpu.SemaphoreType.DMA((2, 2)),
            pltpu.SemaphoreType.DMA((6,)),
        ],
        compiler_params=pltpu.CompilerParams(vmem_limit_bytes=VMEM_LIMIT),
    )(x, dy, wg, wu, wd)


STRIDE = (16, 4, 1)
Q = 6
NS, NV, NO = 2, 4, 4
SUMMED, LAST = 6, 11
END = NBLK - 1
HALF = 28
EXCHANGE = {1: 28, 2: 14, 3: 7, 4: 4, 7: 4, 8: 7, 9: 14}


def comm_scratch():
    def v(*shape, dtype=bf16):
        return pltpu.VMEM((*shape, 16, 128), dtype)

    n = len(EXCHANGE)
    return dict(
        blk=v(NS, 3, 112),
        r1=v(2, Q, 28),
        r2=v(2, Q, 14),
        r3=v(2, Q, 7),
        r4=v(2, Q, 4),
        r5=v(2, Q, 3),
        s2=v(Q, 14),
        s3=v(Q, 7),
        s4=v(Q, 4),
        s5=v(Q, 4),
        k2=v(Q, 14, dtype=f32),
        k3=v(Q, 7, dtype=f32),
        k4=v(Q, 4, dtype=f32),
        k5=v(Q, 1, dtype=f32),
        v7=v(NV, Q, 2, 4),
        mine=v(NO, Q, HALF),
        ssq=pltpu.VMEM((8, 128), f32),
        ssq_to=pltpu.VMEM((6, 8, 128), f32),
        ssq_from=pltpu.VMEM((6, 8, 128), f32),
        send=pltpu.SemaphoreType.DMA((n, Q)),
        recv=pltpu.SemaphoreType.DMA((n, 2, Q)),
        send3=pltpu.SemaphoreType.DMA((2, 2, Q, 3)),
        recv3=pltpu.SemaphoreType.DMA((2, 3, Q, 3)),
        osem=pltpu.SemaphoreType.DMA((2, Q)),
        qsend=pltpu.SemaphoreType.DMA((6,)),
        qrecv=pltpu.SemaphoreType.DMA((6,)),
    )


def parity(p):
    return lax.rem(lax.div(p + 1, 2), 2)


def upper(p):
    return lax.div(p, 2)


def position(me):
    return [lax.rem(lax.div(me, s), 4) for s in STRIDE]


def first_bits(me):
    pos = position(me)
    return [(parity, upper)[q % 2](pos[q // 2]) for q in range(Q)]


def add(*terms):
    total = terms[0].astype(f32)
    for t in terms[1:]:
        total = total + t.astype(f32)
    return total


class Comm:
    def __init__(self, refs, outs):
        self.__dict__.update(refs)
        self.outs = outs
        me = lax.axis_index("dp")
        pos = position(me)
        self.pos = pos
        self.near = []
        for p, s in zip(pos, STRIDE):
            base = me - p * s
            self.near.append((base + (p + 1 - 2 * lax.rem(p, 2)) * s, base + (3 - p) * s, base + lax.rem(p + 2, 4) * s))
        self.bits, self.peer = [], []
        for q in range(Q):
            j, w = divmod(q, 2)
            bits, peer = [], []
            for d in (j, (j + 1) % 3):
                for way in (w, 1 - w):
                    bits.append((parity, upper)[way](pos[d]))
                    peer.append(self.near[d][way])
            self.bits.append(bits)
            self.peer.append(peer)
        self.ssq[...] = jnp.zeros((8, 128), f32)

    def barrier(self):
        sem = pltpu.get_barrier_semaphore()
        for ring in self.near:
            for device in ring:
                pl.semaphore_signal(sem, inc=1, device_id={"dp": device}, device_id_type=MESH)
        pl.semaphore_wait(sem, 9)

    def last(self, q):
        d = (q // 2 + 2) % 3
        p = self.pos[d]
        places = (p + 1 - 2 * lax.rem(p, 2), 3 - p, lax.rem(p + 2, 4))
        return p, tuple(zip(self.near[d], places))

    def copies(self, stage, b):
        s, bs, vs, ms = lax.rem(b, 2), lax.rem(b, NS), lax.rem(b, NV), lax.rem(b, NO)
        out = []
        for q in range(Q):
            j, w = divmod(q, 2)
            b1, b2, b3, b4 = self.bits[q]
            if stage in (5, 6):
                p, others = self.last(q)
                for way, (device, place) in enumerate(others):
                    if stage == 5:
                        src, dst = self.s5.at[q, pl.ds(place, 1)], self.r5.at[s, q, pl.ds(way, 1)]
                    else:
                        src = dst = self.v7.at[vs, q, b4, pl.ds(p, 1)]
                    sems = self.send3.at[stage - 5, s, q, way], self.recv3.at[stage - 5, lax.rem(b, 3), q, way]
                    out.append((src, dst, *sems, device))
                continue
            if stage == 1:
                src, dst = self.blk.at[bs, j, pl.ds(56 * w + 28 * (1 - b1), 28)], self.r1.at[s, q]
            elif stage == 2:
                src, dst = self.s2.at[q], self.r2.at[s, q]
            elif stage == 3:
                src, dst = self.s3.at[q], self.r3.at[s, q]
            elif stage == 4:
                src, dst = self.s4.at[q], self.r4.at[s, q]
            elif stage == 7:
                src = dst = self.v7.at[vs, q, b4]
            elif stage == 8:
                src = dst = self.mine.at[ms, q, pl.ds(14 * b2 + 7 * b3, 7)]
            else:
                src = dst = self.mine.at[ms, q, pl.ds(14 * b2, 14)]
            i = list(EXCHANGE).index(stage)
            which = stage - 1 if stage < 5 else 10 - stage
            out.append((src, dst, self.send.at[i, q], self.recv.at[i, s, q], self.peer[q][which]))
        return [
            pltpu.make_async_remote_copy(src_ref=src, dst_ref=dst, send_sem=send, recv_sem=recv, device_id={"dp": device}, device_id_type=MESH)
            for src, dst, send, recv, device in out
        ]

    def math(self, stage, b):
        s, bs, vs, ms = lax.rem(b, 2), lax.rem(b, NS), lax.rem(b, NV), lax.rem(b, NO)
        for q in range(Q):
            j, w = divmod(q, 2)
            b1, b2, b3, b4 = self.bits[q]
            if stage == 2:
                for keep, at in ((True, 14 * b2), (False, 14 * (1 - b2))):
                    total = add(self.blk[bs, j, pl.ds(56 * w + 28 * b1 + at, 14)], self.r1[s, q, pl.ds(at, 14)])
                    if keep:
                        self.k2[q] = total
                    else:
                        self.s2[q] = total.astype(bf16)
            elif stage == 3:
                for keep, at in ((True, 7 * b3), (False, 7 * (1 - b3))):
                    total = add(self.k2[q, pl.ds(at, 7)], self.r2[s, q, pl.ds(at, 7)])
                    if keep:
                        self.k3[q] = total
                    else:
                        self.s3[q] = total.astype(bf16)
            elif stage == 4:
                for keep, at in ((True, 3 * b4), (False, 3 * (1 - b4))):
                    total = add(self.k3[q, pl.ds(at, 4)], self.r3[s, q, pl.ds(at, 4)])
                    if keep:
                        self.k4[q] = total
                    else:
                        self.s4[q] = total.astype(bf16)
            elif stage == 5:
                p, _ = self.last(q)
                self.k5[q] = add(self.k4[q, pl.ds(p, 1)], self.r4[s, q, pl.ds(p, 1)])
                self.s5[q] = add(self.k4[q], self.r4[s, q]).astype(bf16)
            elif stage == 6:
                p, _ = self.last(q)
                g = add(self.k5[q], *(self.r5[s, q, pl.ds(way, 1)] for way in range(3))).astype(bf16)
                self.v7[vs, q, b4, pl.ds(p, 1)] = g
                square = g.astype(f32).reshape(2, 8, 128)
                square = square * square
                counts = jnp.where((b4 == 1) & (p == 0), 0.0, 1.0)
                self.ssq[...] += (square[0] + square[1]) * counts
            elif stage == 8:
                self.mine[ms, q, pl.ds(14 * b2 + 7 * b3, 4)] = self.v7[vs, q, 0]
                self.mine[ms, q, pl.ds(14 * b2 + 7 * b3 + 4, 3)] = self.v7[vs, q, 1, 1:4]

    def out(self, b):
        return [pltpu.make_async_copy(self.mine.at[lax.rem(b, NO), q], self.outs[q].at[b], self.osem.at[lax.rem(b, 2), q]) for q in range(Q)]

    def stage(self, k, b):
        if 2 <= k <= 10:
            for c in self.copies(k - 1, b):
                c.wait()
        if k <= 9:
            self.math(k, b)
            for c in self.copies(k, b):
                c.start()
        elif k == 10:
            for c in self.out(b):
                c.start()
        else:
            for c in self.out(b):
                c.wait()

    def service(self, tick):
        for k in (*range(SUMMED, 0, -1), *range(LAST, SUMMED, -1)):
            pl.when((tick >= k) & (tick - k <= END))(functools.partial(self.stage, k, tick - k))

    def total(self, step):
        def copy(step):
            d, way = divmod(step, 2)
            return pltpu.make_async_remote_copy(
                src_ref=self.ssq_to.at[step],
                dst_ref=self.ssq_from.at[step],
                send_sem=self.qsend.at[step],
                recv_sem=self.qrecv.at[step],
                device_id={"dp": self.near[d][way]},
                device_id_type=MESH,
            )

        if step > 0:
            copy(step - 1).wait()
            self.ssq[...] += self.ssq_from[step - 1]
        if step < 6:
            self.ssq_to[step] = self.ssq[...]
            copy(step).start()


def backward(names, h1_hbm, dy_hbm, a0t_hbm, s_hbm, a_hbm, act_hbm, a1_hbm, a1t_hbm, dyt_hbm, wg, wu, wd, *rest):
    outs, ssq_out, scratch = rest[:Q], rest[Q], rest[Q + 1 :]
    refs = dict(zip(names, scratch, strict=True))
    h1, dy, a, a_t, dy_t, da, wgu, wdb, act, dgu, sb, ab, isem, wsem = (refs.pop(n) for n in OWN)
    comm = Comm(refs, outs)
    first = [
        pltpu.make_async_copy(src, dst, isem.at[k]) for k, (src, dst) in enumerate(((a1_hbm, a), (dy_hbm, dy), (a1t_hbm, a_t), (dyt_hbm, dy_t), (h1_hbm, h1)))
    ]

    def fetch1(b, slot):
        return (
            pltpu.make_async_copy(wg.at[1, :, block(b)], wgu.at[slot, :, 0:FB], wsem.at[slot, 0]),
            pltpu.make_async_copy(wu.at[1, :, block(b)], wgu.at[slot, :, FB : 2 * FB], wsem.at[slot, 1]),
            pltpu.make_async_copy(wd.at[1, block(b), :], wdb.at[slot], wsem.at[slot, 2]),
        )

    def fetch0(b, slot):
        return (
            pltpu.make_async_copy(s_hbm.at[b], sb.at[slot], wsem.at[slot, 0]),
            pltpu.make_async_copy(a_hbm.at[b], ab.at[slot], wsem.at[slot, 1]),
            pltpu.make_async_copy(act_hbm.at[:, block(b)], act.at[slot], wsem.at[slot, 3]),
            pltpu.make_async_copy(wd.at[0, block(b), :], wdb.at[slot], wsem.at[slot, 2]),
        )

    for c in fetch1(0, 0):
        c.start()
    for c in first:
        c.start()

    @pl.loop(0, NT)
    def _(t):
        da[rows(t), :] = jnp.zeros((TM, D), f32)

    comm.barrier()
    for c in first[:4]:
        c.wait()

    def give(slot, gate_up, down):
        g = gate_up.astype(bf16)
        for j in range(2):
            for n in range(112):
                band, half = divmod(n, 2)
                comm.blk[slot, j, n] = g[16 * band : 16 * band + 16, FB * j + 128 * half : FB * j + 128 * half + 128]
        g = down.astype(bf16).T
        for n in range(112):
            band, c = divmod(n, 7)
            comm.blk[slot, 2, n] = g[16 * band : 16 * band + 16, 128 * c : 128 * c + 128]

    @pl.loop(0, NB)
    def _(b):
        comm.service(b)
        slot = lax.rem(b, 2)

        @pl.when(b + 1 < NB)
        def _():
            for c in fetch1(b + 1, 1 - slot):
                c.start()

        for c in fetch1(b, slot):
            c.wait()
        for t in range(NT):
            r = pl.ds(t * TM, TM)
            both = dot(a[r, :], wgu[slot])
            gate, up = both[:, :FB], both[:, FB:]
            dact = dot_t(dy[r, :], wdb[slot]).astype(bf16).astype(f32)
            sg = sigmoid(gate)
            s = gate * sg
            act[0, r, :] = (s * up).astype(bf16)
            dgu[r, :FB] = (dact * up * (sg + (s - s * sg))).astype(bf16)
            dgu[r, FB:] = (dact * s).astype(bf16)
            da[r, :] += dot_t(dgu[r, :], wgu[slot])
        give(lax.rem(b, NS), dot(a_t[...], dgu[...]), dot(dy_t[...], act[0]))

    for c in fetch0(0, 0):
        c.start()
    last = pltpu.make_async_copy(a0t_hbm, a_t, isem.at[0])
    last.start()
    first[4].wait()

    @pl.loop(0, NT)
    def _(t):
        h = h1[rows(t), :].astype(f32)
        scale = norm_scale(h)
        g = da[rows(t), :].astype(bf16).astype(f32)
        along = jnp.mean(g * h, -1, keepdims=True)
        dh = (g * scale - h * (scale * scale * scale * along)).astype(bf16) + dy[rows(t), :]
        dy[rows(t), :] = dh
        dy_t[:, rows(t)] = dh.T

    last.wait()

    @pl.loop(0, NB)
    def _(b):
        comm.service(b + NB)
        slot = lax.rem(b, 2)

        @pl.when(b + 1 < NB)
        def _():
            for c in fetch0(b + 1, 1 - slot):
                c.start()

        for c in fetch0(b, slot):
            c.wait()
        for t in range(NT):
            r = pl.ds(t * TM, TM)
            dact = dot_t(dy[r, :], wdb[slot]).astype(bf16).astype(f32)
            dgu[r, :FB] = (dact * ab[slot, r, :]).astype(bf16)
            dgu[r, FB:] = (dact * sb[slot, r, :]).astype(bf16)
        give(lax.rem(b + NB, NS), dot(a_t[...], dgu[...]), dot(dy_t[...], act[slot]))

    @pl.loop(END + 1, END + LAST + 2)
    def _(tick):
        comm.service(tick)
        for step in range(7):
            pl.when(tick == END + SUMMED + step)(functools.partial(comm.total, step))

    ssq_out[...] = comm.ssq[...]


OWN = ("h1", "dy", "a", "a_t", "dy_t", "da", "wgu", "wdb", "act", "dgu", "sb", "ab", "isem", "wsem")


def run_backward(*args):
    own = dict(
        h1=pltpu.VMEM((T, D), bf16),
        dy=pltpu.VMEM((T, D), bf16),
        a=pltpu.VMEM((T, D), bf16),
        a_t=pltpu.VMEM((D, T), bf16),
        dy_t=pltpu.VMEM((D, T), bf16),
        da=pltpu.VMEM((T, D), f32),
        wgu=pltpu.VMEM((2, D, 2 * FB), bf16),
        wdb=pltpu.VMEM((2, FB, D), bf16),
        act=pltpu.VMEM((2, T, FB), bf16),
        dgu=pltpu.VMEM((T, 2 * FB), bf16),
        sb=pltpu.VMEM((2, T, FB), f32),
        ab=pltpu.VMEM((2, T, FB), f32),
        isem=pltpu.SemaphoreType.DMA((5,)),
        wsem=pltpu.SemaphoreType.DMA((2, 4)),
    )
    scratch = own | comm_scratch()
    return pl.pallas_call(
        functools.partial(backward, tuple(scratch)),
        name="backward",
        out_shape=(*(sds((NBLK, HALF, 16, 128), bf16) for _ in range(Q)), sds((8, 128), f32)),
        in_specs=[ANY] * 12,
        out_specs=(*(ANY for _ in range(Q)), VMEM),
        scratch_shapes=list(scratch.values()),
        compiler_params=pltpu.CompilerParams(collective_id=0, has_side_effects=True, vmem_limit_bytes=VMEM_LIMIT),
    )(*args)


def adamw(half_ref, ssq_ref, *refs):
    del half_ref
    w = pl.program_id(0)
    factor = jnp.minimum(1.0, 0.5 * lax.rsqrt(jnp.sum(ssq_ref[...], keepdims=True) / COUNT + 1e-30))
    gs, ins, outs = refs[:Q], refs[Q : Q + 9], refs[-9:]

    def update(k, where, g):
        weight, m, v = (ins[i + k][where].astype(f32) for i in (0, 3, 6))
        g = g.astype(f32) * factor
        m = 0.9 * m + 0.1 * g
        v = 0.95 * v + 0.05 * g * g
        step = m * lax.rsqrt(v + 1e-8) + 0.1 * weight
        outs[k][where] = (weight - 0.02 * step).astype(bf16)
        outs[3 + k][where] = m
        outs[6 + k][where] = v

    @pl.loop(0, NB)
    def _(b):
        for k in range(3):
            g = jnp.where(w == 0, gs[2 * k][b], gs[2 * k + 1][b])
            if k < 2:
                g = g.reshape(7, 2, 16, 128)
                for half in range(2):
                    update(k, (0, slice(None), pl.ds(pl.multiple_of(b * FB + half * 128, 128), 128)), g[:, half].reshape(112, 128))
            else:
                g = g.reshape(2, 7, 16, 128)
                for c in range(7):
                    update(k, (0, b, slice(None), pl.ds(c * 128, 128)), g[:, c].reshape(32, 128))


def run_adamw(half, ssq, gs, arrays, so_far):
    arrays = [a.reshape(LAYERS, NB, FB, D) if k % 3 == 2 else a for k, a in enumerate(arrays)]

    def wide(j):
        return pl.BlockSpec((1, 112, F), lambda w, n, i, half: (1 - n, 4 * w + 2 * half[2 * j + w] + i, 0))

    tall = pl.BlockSpec((1, NB, 32, D), lambda w, n, i, half: (1 - n, 0, 4 * w + 2 * half[4 + w] + i, 0))
    specs = [wide(0), wide(1), tall] * 3

    def of(q):
        mine = q % 2
        return pl.BlockSpec((NB, 14, 16, 128), lambda w, n, i, half: (jnp.where(w == mine, n, 1 - mine), jnp.where(w == mine, i, 1 - mine), 0, 0))

    return pl.pallas_call(
        adamw,
        name="adamw",
        grid_spec=pltpu.PrefetchScalarGridSpec(
            num_scalar_prefetch=1,
            grid=(2, LAYERS, 2),
            in_specs=[pl.BlockSpec((8, 128), lambda w, n, i, half: (0, 0))] + [of(q) for q in range(Q)] + specs + [ANY] * len(so_far),
            out_specs=tuple(specs),
        ),
        out_shape=tuple(sds(a.shape, a.dtype) for a in arrays),
        input_output_aliases={2 + Q + 9 + k: k for k in range(len(so_far))},
        cost_estimate=pl.CostEstimate(flops=100_000_000_000, bytes_accessed=136_000_000, transcendentals=0),
        compiler_params=pltpu.CompilerParams(vmem_limit_bytes=VMEM_LIMIT, dimension_semantics=("arbitrary",) * 3),
    )(half, ssq, *gs, *arrays, *so_far)


def swaps(q):
    j, w = divmod(q, 2)
    s = STRIDE[j]
    out = []
    for me in range(64):
        p = me // s % 4
        out.append((me, me + ((3 - p if w else p ^ 1) - p) * s))
    return out


def solution(mesh):
    def step(x, dy, *arrays):
        wg, wu, wd = arrays[:3]
        s, a, act, h1, a0t, a1, a1t, dyt = run_forward(x[0], dy[0], wg, wu, wd)
        *mine, ssq = run_backward(h1, dy[0], a0t, s, a, act, a1, a1t, dyt, wg, wu, wd)
        theirs = [lax.ppermute(g, "dp", swaps(q)) for q, g in enumerate(mine)]
        half = jnp.stack(first_bits(lax.axis_index("dp"))).astype(jnp.int32)
        new = run_adamw(half, ssq, mine, arrays, ())
        new = run_adamw(1 - half, ssq, theirs, arrays, new)
        return tuple(n.reshape(a.shape) for n, a in zip(new, arrays, strict=True))

    return jax.shard_map(
        step,
        mesh=mesh,
        in_specs=(P(("rep", "dp"), None, None),) * 2 + (P(None, None, None),) * 9,
        out_specs=(P("rep", None, None),) * 9,
        check_vma=False,
    )
```

```python
import functools

import jax
import jax.numpy as jnp
from jax import lax
from jax.experimental import pallas as pl
from jax.experimental.pallas import tpu as pltpu
from jax.sharding import PartitionSpec as P

T, D, F = 2048, 896, 2304
FB = 256
NB = F // FB
LAYERS = 2
NBLK = NB * LAYERS
COUNT = 3 * LAYERS * D * F
TM = 256
NT = T // TM
TB = 512
f32, bf16 = jnp.float32, jnp.bfloat16
MESH = pl.DeviceIdType.MESH
VMEM_LIMIT = 63 * 2**20
ANY = pl.BlockSpec(memory_space=pl.ANY)
VMEM = pl.BlockSpec(memory_space=pltpu.VMEM)
sds = jax.ShapeDtypeStruct


def dot(a, b):
    return jnp.dot(a, b, preferred_element_type=f32)


def dot_t(a, b):
    return lax.dot_general(a, b, (((1,), (1,)), ((), ())), preferred_element_type=f32)


def sigmoid(x):
    return 1.0 / (1.0 + jnp.exp(-x))


def norm_scale(h):
    return lax.rsqrt(jnp.mean(h * h, -1, keepdims=True) + 1e-6)


def rows(t):
    return pl.ds(pl.multiple_of(t * TM, TM), TM)


def block(b):
    return pl.ds(pl.multiple_of(b * FB, FB), FB)


def forward(x_hbm, dy_hbm, wg, wu, wd_hbm, s_hbm, a_hbm, act_hbm, h1_hbm, a0t_hbm, a1_hbm, a1t_hbm, dyt_hbm, *scratch):
    x, dy, a0, act, wgu, wd, sb, ab, h1, a0t, a1, a1t, dyt, xsem, isem, wsem, osem, tsem = scratch

    def fetch(b, slot):
        return (
            pltpu.make_async_copy(wg.at[0, :, block(b)], wgu.at[slot, :, 0:FB], wsem.at[slot, 0]),
            pltpu.make_async_copy(wu.at[0, :, block(b)], wgu.at[slot, :, FB : 2 * FB], wsem.at[slot, 1]),
        )

    def part(t):
        return pltpu.make_async_copy(x_hbm.at[rows(t), :], x.at[rows(t), :], xsem.at[t])

    for t in range(NT):
        part(t).start()
    for c in fetch(0, 0):
        c.start()
    get_dy = pltpu.make_async_copy(dy_hbm, dy, isem.at[0])
    get_dy.start()
    get_wd = pltpu.make_async_copy(wd_hbm.at[0], wd, isem.at[1])
    get_wd.start()

    @pl.loop(0, NT)
    def _(t):
        part(t).wait()
        h = x[rows(t), :].astype(f32)
        a0[rows(t), :] = (h * norm_scale(h)).astype(bf16)

    get_dy.wait()

    def outs(b, slot):
        return (
            pltpu.make_async_copy(sb.at[slot], s_hbm.at[b], osem.at[slot, 0]),
            pltpu.make_async_copy(ab.at[slot], a_hbm.at[b], osem.at[slot, 1]),
        )

    @pl.loop(0, NB)
    def _(b):
        slot = lax.rem(b, 2)

        @pl.when(b + 1 < NB)
        def _():
            for c in fetch(b + 1, 1 - slot):
                c.start()

        @pl.when(b >= 2)
        def _():
            for c in outs(b - 2, slot):
                c.wait()

        for c in fetch(b, slot):
            c.wait()
        turn = rows(jnp.minimum(b, NT - 1))
        a0t[:, turn] = a0[turn, :].T
        dyt[:, turn] = dy[turn, :].T
        for t in range(NT):
            r = pl.ds(t * TM, TM)
            both = dot(a0[r, :], wgu[slot])
            gate, up = both[:, :FB], both[:, FB:]
            sg = sigmoid(gate)
            s = gate * sg
            act[r, block(b)] = (s * up).astype(bf16)
            sb[slot, r, :] = s
            ab[slot, r, :] = up * (sg + (s - s * sg))
        for c in outs(b, slot):
            c.start()

    keep = [pltpu.make_async_copy(src, dst, tsem.at[k]) for k, (src, dst) in enumerate(((act, act_hbm), (a0t, a0t_hbm), (dyt, dyt_hbm)))]
    for c in keep:
        c.start()
    get_wd.wait()
    for t in range(NT):
        r = pl.ds(t * TM, TM)
        h = x[r, :] + dot(act[r, :], wd[...]).astype(bf16)
        h1[r, :] = h
        h = h.astype(f32)
        n = (h * norm_scale(h)).astype(bf16)
        a1[r, :] = n
        a1t[:, r] = n.T
    tail = [pltpu.make_async_copy(src, dst, tsem.at[3 + k]) for k, (src, dst) in enumerate(((h1, h1_hbm), (a1, a1_hbm), (a1t, a1t_hbm)))]
    for c in tail:
        c.start()
    for b in (NB - 2, NB - 1):
        for c in outs(b, b % 2):
            c.wait()
    for c in keep + tail:
        c.wait()


def run_forward(x, dy, wg, wu, wd):
    wide, tall = (T, D), (D, T)
    return pl.pallas_call(
        forward,
        name="forward",
        out_shape=(sds((NB, T, FB), f32), sds((NB, T, FB), f32), sds((T, F), bf16), *(sds(s, bf16) for s in (wide, tall, wide, tall, tall))),
        in_specs=[ANY] * 5,
        out_specs=(ANY,) * 8,
        scratch_shapes=[
            pltpu.VMEM(wide, bf16),
            pltpu.VMEM(wide, bf16),
            pltpu.VMEM(wide, bf16),
            pltpu.VMEM((T, F), bf16),
            pltpu.VMEM((2, D, 2 * FB), bf16),
            pltpu.VMEM((F, D), bf16),
            pltpu.VMEM((2, T, FB), f32),
            pltpu.VMEM((2, T, FB), f32),
            *(pltpu.VMEM(s, bf16) for s in (wide, tall, wide, tall, tall)),
            pltpu.SemaphoreType.DMA((NT,)),
            pltpu.SemaphoreType.DMA((2,)),
            pltpu.SemaphoreType.DMA((2, 2)),
            pltpu.SemaphoreType.DMA((2, 2)),
            pltpu.SemaphoreType.DMA((6,)),
        ],
        compiler_params=pltpu.CompilerParams(vmem_limit_bytes=VMEM_LIMIT),
    )(x, dy, wg, wu, wd)


STRIDE = (16, 4, 1)
Q = 6
NS, NV, NO = 2, 5, 7
DUE = {1: 1, 2: 2, 3: 3, 4: 4, 5: 5, 6: 6, 7: 7, 8: 9, 9: 11, 10: 13, 11: 14}
SUMMED, LAST = 6, 11
END = NBLK - 1
HALF = 28
EXCHANGE = {1: 28, 2: 14, 3: 7, 4: 4, 7: 4, 8: 7, 9: 14}


def comm_scratch():
    def v(*shape, dtype=bf16):
        return pltpu.VMEM((*shape, 16, 128), dtype)

    n = len(EXCHANGE)
    return dict(
        blk=v(NS, 3, 112),
        r1=v(2, Q, 28),
        r2=v(2, Q, 14),
        r3=v(2, Q, 7),
        r4=v(2, Q, 4),
        r5=v(2, Q, 3),
        s2=v(Q, 14),
        s3=v(Q, 7),
        s4=v(Q, 4),
        s5=v(Q, 4),
        k2=v(Q, 14, dtype=f32),
        k3=v(Q, 7, dtype=f32),
        k4=v(Q, 4, dtype=f32),
        k5=v(Q, 1, dtype=f32),
        v7=v(NV, Q, 2, 4),
        mine=v(NO, Q, HALF),
        ssq=pltpu.VMEM((8, 128), f32),
        ssq_to=pltpu.VMEM((6, 8, 128), f32),
        ssq_from=pltpu.VMEM((6, 8, 128), f32),
        send=pltpu.SemaphoreType.DMA((n, 2, Q)),
        recv=pltpu.SemaphoreType.DMA((n, 4, Q)),
        send3=pltpu.SemaphoreType.DMA((2, 2, Q, 3)),
        recv3=pltpu.SemaphoreType.DMA((2, 3, Q, 3)),
        osem=pltpu.SemaphoreType.DMA((2, Q)),
        qsend=pltpu.SemaphoreType.DMA((6,)),
        qrecv=pltpu.SemaphoreType.DMA((6,)),
    )


def parity(p):
    return lax.rem(lax.div(p + 1, 2), 2)


def upper(p):
    return lax.div(p, 2)


def position(me):
    return [lax.rem(lax.div(me, s), 4) for s in STRIDE]


def first_bits(me):
    pos = position(me)
    return [(parity, upper)[q % 2](pos[q // 2]) for q in range(Q)]


def add(*terms):
    total = terms[0].astype(f32)
    for t in terms[1:]:
        total = total + t.astype(f32)
    return total


class Comm:
    def __init__(self, refs, outs):
        self.__dict__.update(refs)
        self.outs = outs
        me = lax.axis_index("dp")
        pos = position(me)
        self.pos = pos
        self.near = []
        for p, s in zip(pos, STRIDE):
            base = me - p * s
            self.near.append((base + (p + 1 - 2 * lax.rem(p, 2)) * s, base + (3 - p) * s, base + lax.rem(p + 2, 4) * s))
        self.bits, self.peer = [], []
        for q in range(Q):
            j, w = divmod(q, 2)
            bits, peer = [], []
            for d in (j, (j + 1) % 3):
                for way in (w, 1 - w):
                    bits.append((parity, upper)[way](pos[d]))
                    peer.append(self.near[d][way])
            self.bits.append(bits)
            self.peer.append(peer)
        self.ssq[...] = jnp.zeros((8, 128), f32)

    def barrier(self):
        sem = pltpu.get_barrier_semaphore()
        for ring in self.near:
            for device in ring:
                pl.semaphore_signal(sem, inc=1, device_id={"dp": device}, device_id_type=MESH)
        pl.semaphore_wait(sem, 9)

    def last(self, q):
        d = (q // 2 + 2) % 3
        p = self.pos[d]
        places = (p + 1 - 2 * lax.rem(p, 2), 3 - p, lax.rem(p + 2, 4))
        return p, tuple(zip(self.near[d], places))

    def copies(self, stage, b):
        s, bs, vs, ms = lax.rem(b, 2), lax.rem(b, NS), lax.rem(b, NV), lax.rem(b, NO)
        out = []
        for q in range(Q):
            j, w = divmod(q, 2)
            b1, b2, b3, b4 = self.bits[q]
            if stage in (5, 6):
                p, others = self.last(q)
                for way, (device, place) in enumerate(others):
                    if stage == 5:
                        src, dst = self.s5.at[q, pl.ds(place, 1)], self.r5.at[s, q, pl.ds(way, 1)]
                    else:
                        src = dst = self.v7.at[vs, q, b4, pl.ds(p, 1)]
                    sems = self.send3.at[stage - 5, s, q, way], self.recv3.at[stage - 5, lax.rem(b, 3), q, way]
                    out.append((src, dst, *sems, device))
                continue
            if stage == 1:
                src, dst = self.blk.at[bs, j, pl.ds(56 * w + 28 * (1 - b1), 28)], self.r1.at[s, q]
            elif stage == 2:
                src, dst = self.s2.at[q], self.r2.at[s, q]
            elif stage == 3:
                src, dst = self.s3.at[q], self.r3.at[s, q]
            elif stage == 4:
                src, dst = self.s4.at[q], self.r4.at[s, q]
            elif stage == 7:
                src = dst = self.v7.at[vs, q, b4]
            elif stage == 8:
                src = dst = self.mine.at[ms, q, pl.ds(14 * b2 + 7 * b3, 7)]
            else:
                src = dst = self.mine.at[ms, q, pl.ds(14 * b2, 14)]
            i = list(EXCHANGE).index(stage)
            which = stage - 1 if stage < 5 else 10 - stage
            out.append((src, dst, self.send.at[i, s, q], self.recv.at[i, lax.rem(b, 4), q], self.peer[q][which]))
        return [
            pltpu.make_async_remote_copy(src_ref=src, dst_ref=dst, send_sem=send, recv_sem=recv, device_id={"dp": device}, device_id_type=MESH)
            for src, dst, send, recv, device in out
        ]

    def math(self, stage, b):
        s, bs, vs, ms = lax.rem(b, 2), lax.rem(b, NS), lax.rem(b, NV), lax.rem(b, NO)
        for q in range(Q):
            j, w = divmod(q, 2)
            b1, b2, b3, b4 = self.bits[q]
            if stage == 2:
                for keep, at in ((True, 14 * b2), (False, 14 * (1 - b2))):
                    total = add(self.blk[bs, j, pl.ds(56 * w + 28 * b1 + at, 14)], self.r1[s, q, pl.ds(at, 14)])
                    if keep:
                        self.k2[q] = total
                    else:
                        self.s2[q] = total.astype(bf16)
            elif stage == 3:
                for keep, at in ((True, 7 * b3), (False, 7 * (1 - b3))):
                    total = add(self.k2[q, pl.ds(at, 7)], self.r2[s, q, pl.ds(at, 7)])
                    if keep:
                        self.k3[q] = total
                    else:
                        self.s3[q] = total.astype(bf16)
            elif stage == 4:
                for keep, at in ((True, 3 * b4), (False, 3 * (1 - b4))):
                    total = add(self.k3[q, pl.ds(at, 4)], self.r3[s, q, pl.ds(at, 4)])
                    if keep:
                        self.k4[q] = total
                    else:
                        self.s4[q] = total.astype(bf16)
            elif stage == 5:
                p, _ = self.last(q)
                self.k5[q] = add(self.k4[q, pl.ds(p, 1)], self.r4[s, q, pl.ds(p, 1)])
                self.s5[q] = add(self.k4[q], self.r4[s, q]).astype(bf16)
            elif stage == 6:
                p, _ = self.last(q)
                g = add(self.k5[q], *(self.r5[s, q, pl.ds(way, 1)] for way in range(3))).astype(bf16)
                self.v7[vs, q, b4, pl.ds(p, 1)] = g
                square = g.astype(f32).reshape(2, 8, 128)
                square = square * square
                counts = jnp.where((b4 == 1) & (p == 0), 0.0, 1.0)
                self.ssq[...] += (square[0] + square[1]) * counts
            elif stage == 8:
                self.mine[ms, q, pl.ds(14 * b2 + 7 * b3, 4)] = self.v7[vs, q, 0]
                self.mine[ms, q, pl.ds(14 * b2 + 7 * b3 + 4, 3)] = self.v7[vs, q, 1, 1:4]

    def out(self, b):
        return [pltpu.make_async_copy(self.mine.at[lax.rem(b, NO), q], self.outs[q].at[b], self.osem.at[lax.rem(b, 2), q]) for q in range(Q)]

    def stage(self, k, b):
        if 2 <= k <= 10:
            for c in self.copies(k - 1, b):
                c.wait()
        if k <= 9:
            self.math(k, b)
            for c in self.copies(k, b):
                c.start()
        elif k == 10:
            for c in self.out(b):
                c.start()
        else:
            for c in self.out(b):
                c.wait()

    def service(self, tick):
        for k in (*range(SUMMED, 0, -1), *range(LAST, SUMMED, -1)):
            b = tick - DUE[k]
            pl.when((b >= 0) & (b <= END))(functools.partial(self.stage, k, b))

    def total(self, step):
        def copy(step):
            d, way = divmod(step, 2)
            return pltpu.make_async_remote_copy(
                src_ref=self.ssq_to.at[step],
                dst_ref=self.ssq_from.at[step],
                send_sem=self.qsend.at[step],
                recv_sem=self.qrecv.at[step],
                device_id={"dp": self.near[d][way]},
                device_id_type=MESH,
            )

        if step > 0:
            copy(step - 1).wait()
            self.ssq[...] += self.ssq_from[step - 1]
        if step < 6:
            self.ssq_to[step] = self.ssq[...]
            copy(step).start()


def backward(names, h1_hbm, dy_hbm, a0t_hbm, s_hbm, a_hbm, act_hbm, a1_hbm, a1t_hbm, dyt_hbm, wg, wu, wd, *rest):
    outs, ssq_out, scratch = rest[:Q], rest[Q], rest[Q + 1 :]
    refs = dict(zip(names, scratch, strict=True))
    h1, dy, a, a_t, dy_t, da, wgu, wdb, act, dgu, sb, ab, isem, wsem = (refs.pop(n) for n in OWN)
    comm = Comm(refs, outs)
    first = [
        pltpu.make_async_copy(src, dst, isem.at[k]) for k, (src, dst) in enumerate(((a1_hbm, a), (dy_hbm, dy), (a1t_hbm, a_t), (dyt_hbm, dy_t), (h1_hbm, h1)))
    ]

    def fetch1(b, slot):
        return (
            pltpu.make_async_copy(wg.at[1, :, block(b)], wgu.at[slot, :, 0:FB], wsem.at[slot, 0]),
            pltpu.make_async_copy(wu.at[1, :, block(b)], wgu.at[slot, :, FB : 2 * FB], wsem.at[slot, 1]),
            pltpu.make_async_copy(wd.at[1, block(b), :], wdb.at[slot], wsem.at[slot, 2]),
        )

    def fetch0(b, slot):
        return (
            pltpu.make_async_copy(s_hbm.at[b], sb.at[slot], wsem.at[slot, 0]),
            pltpu.make_async_copy(a_hbm.at[b], ab.at[slot], wsem.at[slot, 1]),
            pltpu.make_async_copy(act_hbm.at[:, block(b)], act.at[slot], wsem.at[slot, 3]),
            pltpu.make_async_copy(wd.at[0, block(b), :], wdb.at[slot], wsem.at[slot, 2]),
        )

    for c in fetch1(0, 0):
        c.start()
    for c in first:
        c.start()

    @pl.loop(0, NT)
    def _(t):
        da[rows(t), :] = jnp.zeros((TM, D), f32)

    comm.barrier()
    for c in first[:4]:
        c.wait()

    def give(slot, gate_up, down):
        g = gate_up.astype(bf16)
        for j in range(2):
            for n in range(112):
                band, half = divmod(n, 2)
                comm.blk[slot, j, n] = g[16 * band : 16 * band + 16, FB * j + 128 * half : FB * j + 128 * half + 128]
        g = down.astype(bf16).T
        for n in range(112):
            band, c = divmod(n, 7)
            comm.blk[slot, 2, n] = g[16 * band : 16 * band + 16, 128 * c : 128 * c + 128]

    @pl.loop(0, NB)
    def _(b):
        comm.service(b)
        slot = lax.rem(b, 2)

        @pl.when(b + 1 < NB)
        def _():
            for c in fetch1(b + 1, 1 - slot):
                c.start()

        for c in fetch1(b, slot):
            c.wait()
        for t in range(T // TB):
            r = pl.ds(t * TB, TB)
            both = dot(a[r, :], wgu[slot])
            gate, up = both[:, :FB], both[:, FB:]
            dact = dot_t(dy[r, :], wdb[slot]).astype(bf16).astype(f32)
            sg = sigmoid(gate)
            s = gate * sg
            act[0, r, :] = (s * up).astype(bf16)
            dgu[r, :FB] = (dact * up * (sg + (s - s * sg))).astype(bf16)
            dgu[r, FB:] = (dact * s).astype(bf16)
            da[r, :] += dot_t(dgu[r, :], wgu[slot])
        give(lax.rem(b, NS), dot(a_t[...], dgu[...]), dot(dy_t[...], act[0]))

    for c in fetch0(0, 0):
        c.start()
    last = pltpu.make_async_copy(a0t_hbm, a_t, isem.at[0])
    last.start()
    first[4].wait()

    @pl.loop(0, NT)
    def _(t):
        h = h1[rows(t), :].astype(f32)
        scale = norm_scale(h)
        g = da[rows(t), :].astype(bf16).astype(f32)
        along = jnp.mean(g * h, -1, keepdims=True)
        dh = (g * scale - h * (scale * scale * scale * along)).astype(bf16) + dy[rows(t), :]
        dy[rows(t), :] = dh
        dy_t[:, rows(t)] = dh.T

    last.wait()

    @pl.loop(0, NB)
    def _(b):
        comm.service(b + NB)
        slot = lax.rem(b, 2)

        @pl.when(b + 1 < NB)
        def _():
            for c in fetch0(b + 1, 1 - slot):
                c.start()

        for c in fetch0(b, slot):
            c.wait()
        for t in range(T // TB):
            r = pl.ds(t * TB, TB)
            dact = dot_t(dy[r, :], wdb[slot]).astype(bf16).astype(f32)
            dgu[r, :FB] = (dact * ab[slot, r, :]).astype(bf16)
            dgu[r, FB:] = (dact * sb[slot, r, :]).astype(bf16)
        give(lax.rem(b + NB, NS), dot(a_t[...], dgu[...]), dot(dy_t[...], act[slot]))

    @pl.loop(END + 1, END + DUE[LAST] + 1)
    def _(tick):
        comm.service(tick)
        for step in range(7):
            pl.when(tick == END + SUMMED + step)(functools.partial(comm.total, step))

    ssq_out[...] = comm.ssq[...]


OWN = ("h1", "dy", "a", "a_t", "dy_t", "da", "wgu", "wdb", "act", "dgu", "sb", "ab", "isem", "wsem")


def run_backward(*args):
    own = dict(
        h1=pltpu.VMEM((T, D), bf16),
        dy=pltpu.VMEM((T, D), bf16),
        a=pltpu.VMEM((T, D), bf16),
        a_t=pltpu.VMEM((D, T), bf16),
        dy_t=pltpu.VMEM((D, T), bf16),
        da=pltpu.VMEM((T, D), f32),
        wgu=pltpu.VMEM((2, D, 2 * FB), bf16),
        wdb=pltpu.VMEM((2, FB, D), bf16),
        act=pltpu.VMEM((2, T, FB), bf16),
        dgu=pltpu.VMEM((T, 2 * FB), bf16),
        sb=pltpu.VMEM((2, T, FB), f32),
        ab=pltpu.VMEM((2, T, FB), f32),
        isem=pltpu.SemaphoreType.DMA((5,)),
        wsem=pltpu.SemaphoreType.DMA((2, 4)),
    )
    scratch = own | comm_scratch()
    return pl.pallas_call(
        functools.partial(backward, tuple(scratch)),
        name="backward",
        out_shape=(*(sds((NBLK, HALF, 16, 128), bf16) for _ in range(Q)), sds((8, 128), f32)),
        in_specs=[ANY] * 12,
        out_specs=(*(ANY for _ in range(Q)), VMEM),
        scratch_shapes=list(scratch.values()),
        compiler_params=pltpu.CompilerParams(collective_id=0, has_side_effects=True, vmem_limit_bytes=VMEM_LIMIT),
    )(*args)


SPLIT = 3
PER = LAYERS * 2 * (NB // SPLIT)
STEPS = 2 * PER
INS, OUTS = 4, 3
SHAPES = ((112, SPLIT * FB), (112, SPLIT * FB), (SPLIT, 32, D))


def adamw(other, ssq_ref, *refs):
    gs, arrays, refs = refs[:Q], refs[Q : Q + 9], refs[Q + 9 :]
    if other:
        refs = refs[9:]
    results, g_buf, in_buf, out_buf, (gsem, isem, osem) = refs[:9], refs[9], refs[10:19], refs[19:28], refs[28:]
    factor = jnp.minimum(1.0, 0.5 * lax.rsqrt(jnp.sum(ssq_ref[...], keepdims=True) / COUNT + 1e-30))
    bits = first_bits(lax.axis_index("dp"))

    def place(t):
        w, t = lax.div(t, PER), lax.rem(t, PER)
        n, t = lax.div(t, 2 * NB // SPLIT), lax.rem(t, 2 * NB // SPLIT)
        return w, n, lax.div(t, NB // SPLIT), lax.rem(t, NB // SPLIT)

    def window(t, k, ref):
        w, n, i, f = place(t)
        half = jnp.where(w == 0, bits[2 * k], bits[2 * k + 1])
        row = 4 * w + 2 * (1 - half if other else half) + i
        if k < 2:
            return ref.at[1 - n, pl.ds(pl.multiple_of(row * 112, 16), 112), pl.ds(pl.multiple_of(f * SPLIT * FB, 128), SPLIT * FB)]
        return ref.at[1 - n, pl.ds(f * SPLIT, SPLIT), pl.ds(pl.multiple_of(row * 32, 16), 32), :]

    def inward(t):
        s = lax.rem(t, INS)
        return [pltpu.make_async_copy(window(t, k % 3, arrays[k]), in_buf[k].at[s], isem.at[s, k]) for k in range(9)]

    def g_inward(t, w):
        s = lax.rem(t, INS)
        _, n, i, f = place(t)
        at = pl.ds(n * NB + f * SPLIT, SPLIT), pl.ds(14 * i, 14)
        return [pltpu.make_async_copy(gs[2 * k + w].at[at], g_buf.at[s, k], gsem.at[s, k]) for k in range(3)]

    def outward(t):
        s = lax.rem(t, OUTS)
        return [pltpu.make_async_copy(out_buf[k].at[s], window(t, k % 3, results[k]), osem.at[s, k]) for k in range(9)]

    def fetch(t):
        for c in inward(t):
            c.start()
        for w in range(2):

            @pl.when(lax.div(t, PER) == w)
            def _():
                for c in g_inward(t, w):
                    c.start()

    for t in range(INS - 1):
        fetch(t)

    @pl.loop(0, STEPS)
    def _(t):
        s, o = lax.rem(t, INS), lax.rem(t, OUTS)

        @pl.when(t + INS - 1 < STEPS)
        def _():
            fetch(t + INS - 1)

        @pl.when(t >= OUTS)
        def _():
            for c in outward(t - OUTS):
                c.wait()

        for c in inward(t) + g_inward(t, 0):
            c.wait()

        def update(k, where, g):
            weight, m, v = (in_buf[i + k][(s, *where)].astype(f32) for i in (0, 3, 6))
            g = g.astype(f32) * factor
            m = 0.9 * m + 0.1 * g
            v = 0.95 * v + 0.05 * g * g
            step = m * lax.rsqrt(v + 1e-8) + 0.1 * weight
            out_buf[k][(o, *where)] = (weight - 0.02 * step).astype(bf16)
            out_buf[3 + k][(o, *where)] = m
            out_buf[6 + k][(o, *where)] = v

        for b in range(SPLIT):
            for k in range(3):
                if k < 2:
                    g = g_buf[s, k, b].reshape(7, 2, 16, 128)
                    for half in range(2):
                        update(k, (slice(None), slice(b * FB + half * 128, b * FB + half * 128 + 128)), g[:, half].reshape(112, 128))
                else:
                    g = g_buf[s, k, b].reshape(2, 7, 16, 128)
                    for c in range(7):
                        update(k, (b, slice(None), slice(c * 128, c * 128 + 128)), g[:, c].reshape(32, 128))
        for c in outward(t):
            c.start()

    for t in range(STEPS - OUTS, STEPS):
        for c in outward(t):
            c.wait()


def run_adamw(other, ssq, gs, arrays, so_far):
    arrays = [a.reshape(LAYERS, NB, FB, D) if k % 3 == 2 else a for k, a in enumerate(arrays)]

    def held(n):
        return [pltpu.VMEM((n, *SHAPES[k % 3]), arrays[k].dtype) for k in range(9)]

    return pl.pallas_call(
        functools.partial(adamw, other),
        name="adamw",
        in_specs=[VMEM] + [ANY] * (Q + 9 + len(so_far)),
        out_specs=(ANY,) * 9,
        out_shape=tuple(sds(a.shape, a.dtype) for a in arrays),
        scratch_shapes=[
            pltpu.VMEM((INS, 3, SPLIT, 14, 16, 128), bf16),
            *held(INS),
            *held(OUTS),
            pltpu.SemaphoreType.DMA((INS, 3)),
            pltpu.SemaphoreType.DMA((INS, 9)),
            pltpu.SemaphoreType.DMA((OUTS, 9)),
        ],
        input_output_aliases={1 + Q + 9 + k: k for k in range(len(so_far))},
        cost_estimate=pl.CostEstimate(flops=100_000_000_000, bytes_accessed=136_000_000, transcendentals=0),
        compiler_params=pltpu.CompilerParams(vmem_limit_bytes=VMEM_LIMIT),
    )(ssq, *gs, *arrays, *so_far)


def swaps(q):
    j, w = divmod(q, 2)
    s = STRIDE[j]
    out = []
    for me in range(64):
        p = me // s % 4
        out.append((me, me + ((3 - p if w else p ^ 1) - p) * s))
    return out


def solution(mesh):
    def step(x, dy, *arrays):
        wg, wu, wd = arrays[:3]
        s, a, act, h1, a0t, a1, a1t, dyt = run_forward(x[0], dy[0], wg, wu, wd)
        *mine, ssq = run_backward(h1, dy[0], a0t, s, a, act, a1, a1t, dyt, wg, wu, wd)
        theirs = [lax.ppermute(g, "dp", swaps(q)) for q, g in enumerate(mine)]
        new = run_adamw(False, ssq, mine, arrays, ())
        new = run_adamw(True, ssq, theirs, arrays, new)
        return tuple(n.reshape(a.shape) for n, a in zip(new, arrays, strict=True))

    return jax.shard_map(
        step,
        mesh=mesh,
        in_specs=(P(("rep", "dp"), None, None),) * 2 + (P(None, None, None),) * 9,
        out_specs=(P("rep", None, None),) * 9,
        check_vma=False,
    )
```

```python
import functools

import jax
import jax.numpy as jnp
from jax import lax
from jax.experimental import pallas as pl
from jax.experimental.pallas import tpu as pltpu
from jax.sharding import PartitionSpec as P

T, D, F = 2048, 896, 2304
FB = 256
NB = F // FB
LAYERS = 2
NBLK = NB * LAYERS
COUNT = 3 * LAYERS * D * F
TM = 256
NT = T // TM
TB = 512
f32, bf16 = jnp.float32, jnp.bfloat16
MESH = pl.DeviceIdType.MESH
VMEM_LIMIT = 63 * 2**20
ANY = pl.BlockSpec(memory_space=pl.ANY)
VMEM = pl.BlockSpec(memory_space=pltpu.VMEM)
sds = jax.ShapeDtypeStruct


def dot(a, b):
    return jnp.dot(a, b, preferred_element_type=f32)


def dot_t(a, b):
    return lax.dot_general(a, b, (((1,), (1,)), ((), ())), preferred_element_type=f32)


def sigmoid(x):
    return 1.0 / (1.0 + jnp.exp(-x))


def norm_scale(h):
    return lax.rsqrt(jnp.mean(h * h, -1, keepdims=True) + 1e-6)


def rows(t):
    return pl.ds(pl.multiple_of(t * TM, TM), TM)


def block(b):
    return pl.ds(pl.multiple_of(b * FB, FB), FB)


STRIDE = (16, 4, 1)
Q = 6
NS, NV, NO = 2, 5, 7
DUE = {1: 1, 2: 2, 3: 3, 4: 4, 5: 5, 6: 6, 7: 7, 8: 9, 9: 11, 10: 13, 11: 14}
SUMMED, LAST = 6, 11
END = NBLK - 1
HALF = 28
EXCHANGE = {1: 28, 2: 14, 3: 7, 4: 4, 7: 4, 8: 7, 9: 14}


def comm_scratch():
    def v(*shape, dtype=bf16):
        return pltpu.VMEM((*shape, 16, 128), dtype)

    n = len(EXCHANGE)
    return dict(
        blk=v(NS, 3, 112),
        r1=v(2, Q, 28),
        r2=v(2, Q, 14),
        r3=v(2, Q, 7),
        r4=v(2, Q, 4),
        r5=v(2, Q, 3),
        s2=v(Q, 14),
        s3=v(Q, 7),
        s4=v(Q, 4),
        s5=v(Q, 4),
        k2=v(Q, 14, dtype=f32),
        k3=v(Q, 7, dtype=f32),
        k4=v(Q, 4, dtype=f32),
        k5=v(Q, 1, dtype=f32),
        v7=v(NV, Q, 2, 4),
        mine=v(NO, Q, HALF),
        ssq=pltpu.VMEM((8, 128), f32),
        ssq_to=pltpu.VMEM((6, 8, 128), f32),
        ssq_from=pltpu.VMEM((6, 8, 128), f32),
        send=pltpu.SemaphoreType.DMA((n, 2, Q)),
        recv=pltpu.SemaphoreType.DMA((n, 4, Q)),
        send3=pltpu.SemaphoreType.DMA((2, 2, Q, 3)),
        recv3=pltpu.SemaphoreType.DMA((2, 3, Q, 3)),
        gsem=pltpu.SemaphoreType.DMA((2, Q)),
        qsend=pltpu.SemaphoreType.DMA((6,)),
        qrecv=pltpu.SemaphoreType.DMA((6,)),
    )


def parity(p):
    return lax.rem(lax.div(p + 1, 2), 2)


def upper(p):
    return lax.div(p, 2)


def position(me):
    return [lax.rem(lax.div(me, s), 4) for s in STRIDE]


def first_bits(me):
    pos = position(me)
    return [(parity, upper)[q % 2](pos[q // 2]) for q in range(Q)]


def add(*terms):
    total = terms[0].astype(f32)
    for t in terms[1:]:
        total = total + t.astype(f32)
    return total


class Comm:
    def __init__(self, refs, outs):
        self.__dict__.update(refs)
        self.outs = outs
        me = lax.axis_index("dp")
        pos = position(me)
        self.pos = pos
        self.near = []
        for p, s in zip(pos, STRIDE):
            base = me - p * s
            self.near.append((base + (p + 1 - 2 * lax.rem(p, 2)) * s, base + (3 - p) * s, base + lax.rem(p + 2, 4) * s))
        self.bits, self.peer = [], []
        for q in range(Q):
            j, w = divmod(q, 2)
            bits, peer = [], []
            for d in (j, (j + 1) % 3):
                for way in (w, 1 - w):
                    bits.append((parity, upper)[way](pos[d]))
                    peer.append(self.near[d][way])
            self.bits.append(bits)
            self.peer.append(peer)
        self.ssq[...] = jnp.zeros((8, 128), f32)

    def hello(self):
        for ring in self.near:
            for device in ring:
                pl.semaphore_signal(pltpu.get_barrier_semaphore(), inc=1, device_id={"dp": device}, device_id_type=MESH)

    def barrier(self):
        pl.semaphore_wait(pltpu.get_barrier_semaphore(), 9)

    def last(self, q):
        d = (q // 2 + 2) % 3
        p = self.pos[d]
        places = (p + 1 - 2 * lax.rem(p, 2), 3 - p, lax.rem(p + 2, 4))
        return p, tuple(zip(self.near[d], places))

    def copies(self, stage, b):
        s, bs, vs, ms = lax.rem(b, 2), lax.rem(b, NS), lax.rem(b, NV), lax.rem(b, NO)
        out = []
        for q in range(Q):
            j, w = divmod(q, 2)
            b1, b2, b3, b4 = self.bits[q]
            if stage in (5, 6):
                p, others = self.last(q)
                for way, (device, place) in enumerate(others):
                    if stage == 5:
                        src, dst = self.s5.at[q, pl.ds(place, 1)], self.r5.at[s, q, pl.ds(way, 1)]
                    else:
                        src = dst = self.v7.at[vs, q, b4, pl.ds(p, 1)]
                    sems = self.send3.at[stage - 5, s, q, way], self.recv3.at[stage - 5, lax.rem(b, 3), q, way]
                    out.append((src, dst, *sems, device))
                continue
            if stage == 1:
                src, dst = self.blk.at[bs, j, pl.ds(56 * w + 28 * (1 - b1), 28)], self.r1.at[s, q]
            elif stage == 2:
                src, dst = self.s2.at[q], self.r2.at[s, q]
            elif stage == 3:
                src, dst = self.s3.at[q], self.r3.at[s, q]
            elif stage == 4:
                src, dst = self.s4.at[q], self.r4.at[s, q]
            elif stage == 7:
                src = dst = self.v7.at[vs, q, b4]
            elif stage == 8:
                src = dst = self.mine.at[ms, q, pl.ds(14 * b2 + 7 * b3, 7)]
            else:
                src = dst = self.mine.at[ms, q, pl.ds(14 * b2, 14)]
            i = list(EXCHANGE).index(stage)
            which = stage - 1 if stage < 5 else 10 - stage
            out.append((src, dst, self.send.at[i, s, q], self.recv.at[i, lax.rem(b, 4), q], self.peer[q][which]))
        return [
            pltpu.make_async_remote_copy(src_ref=src, dst_ref=dst, send_sem=send, recv_sem=recv, device_id={"dp": device}, device_id_type=MESH)
            for src, dst, send, recv, device in out
        ]

    def math(self, stage, b):
        s, bs, vs, ms = lax.rem(b, 2), lax.rem(b, NS), lax.rem(b, NV), lax.rem(b, NO)
        for q in range(Q):
            j, w = divmod(q, 2)
            b1, b2, b3, b4 = self.bits[q]
            if stage == 2:
                for keep, at in ((True, 14 * b2), (False, 14 * (1 - b2))):
                    total = add(self.blk[bs, j, pl.ds(56 * w + 28 * b1 + at, 14)], self.r1[s, q, pl.ds(at, 14)])
                    if keep:
                        self.k2[q] = total
                    else:
                        self.s2[q] = total.astype(bf16)
            elif stage == 3:
                for keep, at in ((True, 7 * b3), (False, 7 * (1 - b3))):
                    total = add(self.k2[q, pl.ds(at, 7)], self.r2[s, q, pl.ds(at, 7)])
                    if keep:
                        self.k3[q] = total
                    else:
                        self.s3[q] = total.astype(bf16)
            elif stage == 4:
                for keep, at in ((True, 3 * b4), (False, 3 * (1 - b4))):
                    total = add(self.k3[q, pl.ds(at, 4)], self.r3[s, q, pl.ds(at, 4)])
                    if keep:
                        self.k4[q] = total
                    else:
                        self.s4[q] = total.astype(bf16)
            elif stage == 5:
                p, _ = self.last(q)
                self.k5[q] = add(self.k4[q, pl.ds(p, 1)], self.r4[s, q, pl.ds(p, 1)])
                self.s5[q] = add(self.k4[q], self.r4[s, q]).astype(bf16)
            elif stage == 6:
                p, _ = self.last(q)
                g = add(self.k5[q], *(self.r5[s, q, pl.ds(way, 1)] for way in range(3))).astype(bf16)
                self.v7[vs, q, b4, pl.ds(p, 1)] = g
                square = g.astype(f32).reshape(2, 8, 128)
                square = square * square
                counts = jnp.where((b4 == 1) & (p == 0), 0.0, 1.0)
                self.ssq[...] += (square[0] + square[1]) * counts
            elif stage == 8:
                self.mine[ms, q, pl.ds(14 * b2 + 7 * b3, 4)] = self.v7[vs, q, 0]
                self.mine[ms, q, pl.ds(14 * b2 + 7 * b3 + 4, 3)] = self.v7[vs, q, 1, 1:4]

    def out(self, b):
        return [pltpu.make_async_copy(self.mine.at[lax.rem(b, NO), q], self.outs[q].at[b], self.gsem.at[lax.rem(b, 2), q]) for q in range(Q)]

    def stage(self, k, b):
        if 2 <= k <= 10:
            for c in self.copies(k - 1, b):
                c.wait()
        if k <= 9:
            self.math(k, b)
            for c in self.copies(k, b):
                c.start()
        elif k == 10:
            for c in self.out(b):
                c.start()
        else:
            for c in self.out(b):
                c.wait()

    def service(self, tick):
        for k in (*range(SUMMED, 0, -1), *range(LAST, SUMMED, -1)):
            b = tick - DUE[k]
            pl.when((b >= 0) & (b <= END))(functools.partial(self.stage, k, b))

    def total(self, step):
        def copy(step):
            d, way = divmod(step, 2)
            return pltpu.make_async_remote_copy(
                src_ref=self.ssq_to.at[step],
                dst_ref=self.ssq_from.at[step],
                send_sem=self.qsend.at[step],
                recv_sem=self.qrecv.at[step],
                device_id={"dp": self.near[d][way]},
                device_id_type=MESH,
            )

        if step > 0:
            copy(step - 1).wait()
            self.ssq[...] += self.ssq_from[step - 1]
        if step < 6:
            self.ssq_to[step] = self.ssq[...]
            copy(step).start()


def gradients(names, x_hbm, dy_hbm, wg, wu, wd, *rest):
    outs, (ssq_out, s_hbm, ds_hbm, a0t_hbm), scratch = rest[:Q], rest[Q : Q + 4], rest[Q + 4 :]
    refs = dict(zip(names, scratch, strict=True))
    h, dy, a, a_t, dy_t, wgu, wdb, wd0, act0, act, dgu, sb, ub, xsem, isem, wsem, osem, tsem = (refs.pop(n) for n in OWN)
    comm = Comm(refs, outs)
    comm.hello()

    def fetch(layer, b, slot):
        return (
            pltpu.make_async_copy(wg.at[layer, :, block(b)], wgu.at[slot, :, 0:FB], wsem.at[slot, 0]),
            pltpu.make_async_copy(wu.at[layer, :, block(b)], wgu.at[slot, :, FB : 2 * FB], wsem.at[slot, 1]),
            *([pltpu.make_async_copy(wd.at[layer, block(b), :], wdb.at[slot], wsem.at[slot, 2])] if layer else []),
        )

    def part(t):
        return pltpu.make_async_copy(x_hbm.at[rows(t), :], h.at[rows(t), :], xsem.at[t])

    for t in range(NT):
        part(t).start()
    for c in fetch(0, 0, 0):
        c.start()
    get_dy = pltpu.make_async_copy(dy_hbm, dy, isem.at[0])
    get_dy.start()
    get_wd = pltpu.make_async_copy(wd.at[0], wd0, isem.at[1])
    get_wd.start()

    @pl.loop(0, NT)
    def _(t):
        part(t).wait()
        x = h[rows(t), :].astype(f32)
        a[rows(t), :] = (x * norm_scale(x)).astype(bf16)

    get_dy.wait()

    def kept(b, slot):
        return (
            pltpu.make_async_copy(sb.at[slot], s_hbm.at[b], osem.at[slot, 0]),
            pltpu.make_async_copy(ub.at[slot], ds_hbm.at[b], osem.at[slot, 1]),
        )

    def kept_t(t):
        return pltpu.make_async_copy(a_t.at[:, rows(t)], a0t_hbm.at[:, rows(t)], tsem.at[t])

    @pl.loop(0, NB)
    def _(b):
        slot = lax.rem(b, 2)

        @pl.when(b + 1 < NB)
        def _():
            for c in fetch(0, b + 1, 1 - slot):
                c.start()

        @pl.when(b >= 2)
        def _():
            for c in kept(b - 2, slot):
                c.wait()

        @pl.when((b >= 1) & (b < NT))
        def _():
            kept_t(b - 1).start()

        for c in fetch(0, b, slot):
            c.wait()
        turn = rows(jnp.minimum(b, NT - 1))
        a_t[:, turn] = a[turn, :].T
        dy_t[:, turn] = dy[turn, :].T
        for t in range(NT):
            r = pl.ds(t * TM, TM)
            both = dot(a[r, :], wgu[slot])
            gate, up = both[:, :FB], both[:, FB:]
            sg = sigmoid(gate)
            s = gate * sg
            act0[r, block(b)] = (s * up).astype(bf16)
            sb[slot, r, :] = s
            ub[slot, r, :] = up * (sg + (s - s * sg))
        for c in kept(b, slot):
            c.start()

    kept_t(NT - 1).start()
    for c in fetch(1, 0, 0):
        c.start()
    for t in range(NT):
        kept_t(t).wait()
    get_wd.wait()
    for t in range(NT):
        r = pl.ds(t * TM, TM)
        new = h[r, :] + dot(act0[r, :], wd0[...]).astype(bf16)
        h[r, :] = new
        new = new.astype(f32)
        new = (new * norm_scale(new)).astype(bf16)
        a[r, :] = new
        a_t[:, r] = new.T
    for b in (NB - 2, NB - 1):
        for c in kept(b, b % 2):
            c.wait()
    comm.barrier()

    def give(slot, gate_up, down):
        g = gate_up.astype(bf16)
        for j in range(2):
            for n in range(112):
                band, half = divmod(n, 2)
                comm.blk[slot, j, n] = g[16 * band : 16 * band + 16, FB * j + 128 * half : FB * j + 128 * half + 128]
        g = down.astype(bf16).T
        for n in range(112):
            band, c = divmod(n, 7)
            comm.blk[slot, 2, n] = g[16 * band : 16 * band + 16, 128 * c : 128 * c + 128]

    da = [(ref, k, min(FB, D - FB * (2 * i + k))) for i, ref in enumerate((sb, ub)) for k in range(2)]

    @pl.loop(0, NB)
    def _(b):
        comm.service(b)
        slot = lax.rem(b, 2)

        @pl.when(b + 1 < NB)
        def _():
            for c in fetch(1, b + 1, 1 - slot):
                c.start()

        for c in fetch(1, b, slot):
            c.wait()
        for t in range(T // TB):
            r = pl.ds(t * TB, TB)
            both = dot(a[r, :], wgu[slot])
            gate, up = both[:, :FB], both[:, FB:]
            dact = dot_t(dy[r, :], wdb[slot]).astype(bf16).astype(f32)
            sg = sigmoid(gate)
            s = gate * sg
            act[r, :] = (s * up).astype(bf16)
            dgu[r, :FB] = (dact * up * (sg + (s - s * sg))).astype(bf16)
            dgu[r, FB:] = (dact * s).astype(bf16)
            more = dot_t(dgu[r, :], wgu[slot])
            for i, (ref, k, n) in enumerate(da):
                ref[k, r, :n] = jnp.where(b > 0, ref[k, r, :n], 0.0) + more[:, FB * i : FB * i + n]
        give(lax.rem(b, NS), dot(a_t[...], dgu[...]), dot(dy_t[...], act[...]))

    again = pltpu.make_async_copy(a0t_hbm, a_t, isem.at[0])
    again.start()

    def back(b, slot, r=slice(None)):
        return (
            pltpu.make_async_copy(s_hbm.at[b, r], sb.at[slot, r], osem.at[slot, 0]),
            pltpu.make_async_copy(ds_hbm.at[b, r], ub.at[slot, r], osem.at[slot, 1]),
        )

    @pl.loop(0, NT)
    def _(t):
        x = h[rows(t), :].astype(f32)
        scale = norm_scale(x)
        g = jnp.concatenate([ref[k, rows(t), :n] for ref, k, n in da], axis=1).astype(bf16).astype(f32)
        along = jnp.mean(g * x, -1, keepdims=True)
        dh = (g * scale - x * (scale * scale * scale * along)).astype(bf16) + dy[rows(t), :]
        dy[rows(t), :] = dh
        dy_t[:, rows(t)] = dh.T
        for c in back(0, 0, rows(t)):
            c.start()

    again.wait()

    @pl.loop(0, NB)
    def _(b):
        comm.service(b + NB)
        slot = lax.rem(b, 2)

        @pl.when(b + 1 < NB)
        def _():
            for c in back(b + 1, 1 - slot):
                c.start()

        for c in back(b, slot):
            c.wait()
        for t in range(T // TB):
            r = pl.ds(t * TB, TB)
            dact = dot_t(dy[r, :], wd0[block(b), :]).astype(bf16).astype(f32)
            dgu[r, :FB] = (dact * ub[slot, r, :]).astype(bf16)
            dgu[r, FB:] = (dact * sb[slot, r, :]).astype(bf16)
        give(lax.rem(b + NB, NS), dot(a_t[...], dgu[...]), dot(dy_t[...], act0[:, block(b)]))

    @pl.loop(END + 1, END + DUE[LAST] + 1)
    def _(tick):
        comm.service(tick)
        for step in range(7):
            pl.when(tick == END + SUMMED + step)(functools.partial(comm.total, step))

    ssq_out[...] = comm.ssq[...]


OWN = ("h", "dy", "a", "a_t", "dy_t", "wgu", "wdb", "wd0", "act0", "act", "dgu", "sb", "ub", "xsem", "isem", "wsem", "osem", "tsem")


def run_gradients(x, dy, wg, wu, wd):
    own = dict(
        h=pltpu.VMEM((T, D), bf16),
        dy=pltpu.VMEM((T, D), bf16),
        a=pltpu.VMEM((T, D), bf16),
        a_t=pltpu.VMEM((D, T), bf16),
        dy_t=pltpu.VMEM((D, T), bf16),
        wgu=pltpu.VMEM((2, D, 2 * FB), bf16),
        wdb=pltpu.VMEM((2, FB, D), bf16),
        wd0=pltpu.VMEM((F, D), bf16),
        act0=pltpu.VMEM((T, F), bf16),
        act=pltpu.VMEM((T, FB), bf16),
        dgu=pltpu.VMEM((T, 2 * FB), bf16),
        sb=pltpu.VMEM((2, T, FB), f32),
        ub=pltpu.VMEM((2, T, FB), f32),
        xsem=pltpu.SemaphoreType.DMA((NT,)),
        isem=pltpu.SemaphoreType.DMA((2,)),
        wsem=pltpu.SemaphoreType.DMA((2, 3)),
        osem=pltpu.SemaphoreType.DMA((2, 2)),
        tsem=pltpu.SemaphoreType.DMA((NT,)),
    )
    scratch = own | comm_scratch()
    kept = sds((NB, T, FB), f32)
    *mine, ssq, _, _, _ = pl.pallas_call(
        functools.partial(gradients, tuple(scratch)),
        name="gradients",
        out_shape=(*(sds((NBLK, HALF, 16, 128), bf16) for _ in range(Q)), sds((8, 128), f32), kept, kept, sds((D, T), bf16)),
        in_specs=[ANY] * 5,
        out_specs=(*(ANY for _ in range(Q)), VMEM, ANY, ANY, ANY),
        scratch_shapes=list(scratch.values()),
        compiler_params=pltpu.CompilerParams(collective_id=0, has_side_effects=True, vmem_limit_bytes=VMEM_LIMIT),
    )(x, dy, wg, wu, wd)
    return mine, ssq


SPLIT = 3
PER = LAYERS * 2 * (NB // SPLIT)
STEPS = 2 * PER
INS, OUTS = 4, 3
SHAPES = ((112, SPLIT * FB), (112, SPLIT * FB), (SPLIT, 32, D))


def adamw(other, ssq_ref, *refs):
    gs, arrays, refs = refs[:Q], refs[Q : Q + 9], refs[Q + 9 :]
    if other:
        refs = refs[9:]
    results, g_buf, in_buf, out_buf, (gsem, isem, osem) = refs[:9], refs[9], refs[10:19], refs[19:28], refs[28:]
    factor = jnp.minimum(1.0, 0.5 * lax.rsqrt(jnp.sum(ssq_ref[...], keepdims=True) / COUNT + 1e-30))
    bits = first_bits(lax.axis_index("dp"))

    def place(t):
        w, t = lax.div(t, PER), lax.rem(t, PER)
        n, t = lax.div(t, 2 * NB // SPLIT), lax.rem(t, 2 * NB // SPLIT)
        return w, n, lax.div(t, NB // SPLIT), lax.rem(t, NB // SPLIT)

    def window(t, k, ref):
        w, n, i, f = place(t)
        half = jnp.where(w == 0, bits[2 * k], bits[2 * k + 1])
        row = 4 * w + 2 * (1 - half if other else half) + i
        if k < 2:
            return ref.at[1 - n, pl.ds(pl.multiple_of(row * 112, 16), 112), pl.ds(pl.multiple_of(f * SPLIT * FB, 128), SPLIT * FB)]
        return ref.at[1 - n, pl.ds(f * SPLIT, SPLIT), pl.ds(pl.multiple_of(row * 32, 16), 32), :]

    def inward(t):
        s = lax.rem(t, INS)
        return [pltpu.make_async_copy(window(t, k % 3, arrays[k]), in_buf[k].at[s], isem.at[s, k]) for k in range(9)]

    def g_inward(t, w):
        s = lax.rem(t, INS)
        _, n, i, f = place(t)
        at = pl.ds(n * NB + f * SPLIT, SPLIT), pl.ds(14 * i, 14)
        return [pltpu.make_async_copy(gs[2 * k + w].at[at], g_buf.at[s, k], gsem.at[s, k]) for k in range(3)]

    def outward(t):
        s = lax.rem(t, OUTS)
        return [pltpu.make_async_copy(out_buf[k].at[s], window(t, k % 3, results[k]), osem.at[s, k]) for k in range(9)]

    def fetch(t):
        for c in inward(t):
            c.start()
        for w in range(2):

            @pl.when(lax.div(t, PER) == w)
            def _():
                for c in g_inward(t, w):
                    c.start()

    for t in range(INS - 1):
        fetch(t)

    @pl.loop(0, STEPS)
    def _(t):
        s, o = lax.rem(t, INS), lax.rem(t, OUTS)

        @pl.when(t + INS - 1 < STEPS)
        def _():
            fetch(t + INS - 1)

        @pl.when(t >= OUTS)
        def _():
            for c in outward(t - OUTS):
                c.wait()

        for c in inward(t) + g_inward(t, 0):
            c.wait()

        def update(k, where, g):
            weight, m, v = (in_buf[i + k][(s, *where)].astype(f32) for i in (0, 3, 6))
            g = g.astype(f32) * factor
            m = 0.9 * m + 0.1 * g
            v = 0.95 * v + 0.05 * g * g
            step = m * lax.rsqrt(v + 1e-8) + 0.1 * weight
            out_buf[k][(o, *where)] = (weight - 0.02 * step).astype(bf16)
            out_buf[3 + k][(o, *where)] = m
            out_buf[6 + k][(o, *where)] = v

        for b in range(SPLIT):
            for k in range(3):
                if k < 2:
                    g = g_buf[s, k, b].reshape(7, 2, 16, 128)
                    for half in range(2):
                        update(k, (slice(None), slice(b * FB + half * 128, b * FB + half * 128 + 128)), g[:, half].reshape(112, 128))
                else:
                    g = g_buf[s, k, b].reshape(2, 7, 16, 128)
                    for c in range(7):
                        update(k, (b, slice(None), slice(c * 128, c * 128 + 128)), g[:, c].reshape(32, 128))
        for c in outward(t):
            c.start()

    for t in range(STEPS - OUTS, STEPS):
        for c in outward(t):
            c.wait()


def run_adamw(other, ssq, gs, arrays, so_far):
    arrays = [a.reshape(LAYERS, NB, FB, D) if k % 3 == 2 else a for k, a in enumerate(arrays)]

    def held(n):
        return [pltpu.VMEM((n, *SHAPES[k % 3]), arrays[k].dtype) for k in range(9)]

    return pl.pallas_call(
        functools.partial(adamw, other),
        name="adamw",
        in_specs=[VMEM] + [ANY] * (Q + 9 + len(so_far)),
        out_specs=(ANY,) * 9,
        out_shape=tuple(sds(a.shape, a.dtype) for a in arrays),
        scratch_shapes=[
            pltpu.VMEM((INS, 3, SPLIT, 14, 16, 128), bf16),
            *held(INS),
            *held(OUTS),
            pltpu.SemaphoreType.DMA((INS, 3)),
            pltpu.SemaphoreType.DMA((INS, 9)),
            pltpu.SemaphoreType.DMA((OUTS, 9)),
        ],
        input_output_aliases={1 + Q + 9 + k: k for k in range(len(so_far))},
        cost_estimate=pl.CostEstimate(flops=100_000_000_000, bytes_accessed=136_000_000, transcendentals=0),
        compiler_params=pltpu.CompilerParams(vmem_limit_bytes=VMEM_LIMIT),
    )(ssq, *gs, *arrays, *so_far)


def swaps(q):
    j, w = divmod(q, 2)
    s = STRIDE[j]
    out = []
    for me in range(64):
        p = me // s % 4
        out.append((me, me + ((3 - p if w else p ^ 1) - p) * s))
    return out


def solution(mesh):
    def step(x, dy, *arrays):
        mine, ssq = run_gradients(x[0], dy[0], *arrays[:3])
        theirs = [lax.ppermute(g, "dp", swaps(q)) for q, g in enumerate(mine)]
        new = run_adamw(False, ssq, mine, arrays, ())
        new = run_adamw(True, ssq, theirs, arrays, new)
        return tuple(n.reshape(a.shape) for n, a in zip(new, arrays, strict=True))

    return jax.shard_map(
        step,
        mesh=mesh,
        in_specs=(P(("rep", "dp"), None, None),) * 2 + (P(None, None, None),) * 9,
        out_specs=(P("rep", None, None),) * 9,
        check_vma=False,
    )
```

```python
import functools

import jax
import jax.numpy as jnp
from jax import lax
from jax.experimental import pallas as pl
from jax.experimental.pallas import tpu as pltpu
from jax.sharding import PartitionSpec as P

T, D, F = 2048, 896, 2304
FB = 256
NB = F // FB
LAYERS = 2
NBLK = NB * LAYERS
COUNT = 3 * LAYERS * D * F
TM = 256
NT = T // TM
TB = 512
f32, bf16 = jnp.float32, jnp.bfloat16
MESH = pl.DeviceIdType.MESH
VMEM_LIMIT = 67_043_328
ANY = pl.BlockSpec(memory_space=pl.ANY)
VMEM = pl.BlockSpec(memory_space=pltpu.VMEM)
sds = jax.ShapeDtypeStruct


def dot(a, b):
    return jnp.dot(a, b, preferred_element_type=f32)


def dot_t(a, b):
    return lax.dot_general(a, b, (((1,), (1,)), ((), ())), preferred_element_type=f32)


def sigmoid(x):
    return 1.0 / (1.0 + jnp.exp(-x))


def norm_scale(h):
    return lax.rsqrt(jnp.mean(h * h, -1, keepdims=True) + 1e-6)


def rows(t):
    return pl.ds(pl.multiple_of(t * TM, TM), TM)


def block(b):
    return pl.ds(pl.multiple_of(b * FB, FB), FB)


STRIDE = (16, 4, 1)
Q = 6
NS, NV, NO = 2, 5, 7
DUE = {1: 1, 2: 2, 3: 3, 4: 4, 5: 5, 6: 6, 7: 7, 8: 9, 9: 11, 10: 13, 11: 14}
SUMMED, LAST = 6, 11
PAUSE = 3
END = NBLK - 1 + PAUSE
HALF = 28
EXCHANGE = {1: 28, 2: 14, 3: 7, 4: 4, 7: 4, 8: 7, 9: 14}


def comm_scratch():
    def v(*shape, dtype=bf16):
        return pltpu.VMEM((*shape, 16, 128), dtype)

    n = len(EXCHANGE)
    return dict(
        blk=v(NS, 3, 112),
        r1=v(2, Q, 28),
        r2=v(2, Q, 14),
        r3=v(2, Q, 7),
        r4=v(2, Q, 4),
        r5=v(2, Q, 3),
        s2=v(Q, 14),
        s3=v(Q, 7),
        s4=v(Q, 4),
        s5=v(Q, 4),
        k2=v(Q, 14, dtype=f32),
        k3=v(Q, 7, dtype=f32),
        k4=v(Q, 4, dtype=f32),
        k5=v(Q, 1, dtype=f32),
        v7=v(NV, Q, 2, 4),
        mine=v(NO, Q, HALF),
        ssq=pltpu.VMEM((8, 128), f32),
        ssq_to=pltpu.VMEM((6, 8, 128), f32),
        ssq_from=pltpu.VMEM((6, 8, 128), f32),
        send=pltpu.SemaphoreType.DMA((n, 2, Q)),
        recv=pltpu.SemaphoreType.DMA((n, 4, Q)),
        send3=pltpu.SemaphoreType.DMA((2, 2, Q, 3)),
        recv3=pltpu.SemaphoreType.DMA((2, 3, Q, 3)),
        gsem=pltpu.SemaphoreType.DMA((2, Q)),
        qsend=pltpu.SemaphoreType.DMA((6,)),
        qrecv=pltpu.SemaphoreType.DMA((6,)),
    )


def parity(p):
    return lax.rem(lax.div(p + 1, 2), 2)


def upper(p):
    return lax.div(p, 2)


def position(me):
    return [lax.rem(lax.div(me, s), 4) for s in STRIDE]


def first_bits(me):
    pos = position(me)
    return [(parity, upper)[q % 2](pos[q // 2]) for q in range(Q)]


def add(*terms):
    total = terms[0].astype(f32)
    for t in terms[1:]:
        total = total + t.astype(f32)
    return total


class Comm:
    def __init__(self, refs, outs):
        self.__dict__.update(refs)
        self.outs = outs
        me = lax.axis_index("dp")
        pos = position(me)
        self.pos = pos
        self.near = []
        for p, s in zip(pos, STRIDE):
            base = me - p * s
            self.near.append((base + (p + 1 - 2 * lax.rem(p, 2)) * s, base + (3 - p) * s, base + lax.rem(p + 2, 4) * s))
        self.bits, self.peer = [], []
        for q in range(Q):
            j, w = divmod(q, 2)
            bits, peer = [], []
            for d in (j, (j + 1) % 3):
                for way in (w, 1 - w):
                    bits.append((parity, upper)[way](pos[d]))
                    peer.append(self.near[d][way])
            self.bits.append(bits)
            self.peer.append(peer)
        self.ssq[...] = jnp.zeros((8, 128), f32)

    def hello(self):
        for ring in self.near:
            for device in ring:
                pl.semaphore_signal(pltpu.get_barrier_semaphore(), inc=1, device_id={"dp": device}, device_id_type=MESH)

    def barrier(self):
        pl.semaphore_wait(pltpu.get_barrier_semaphore(), 9)

    def last(self, q):
        d = (q // 2 + 2) % 3
        p = self.pos[d]
        places = (p + 1 - 2 * lax.rem(p, 2), 3 - p, lax.rem(p + 2, 4))
        return p, tuple(zip(self.near[d], places))

    def copies(self, stage, b):
        s, bs, vs, ms = lax.rem(b, 2), lax.rem(b, NS), lax.rem(b, NV), lax.rem(b, NO)
        out = []
        for q in range(Q):
            j, w = divmod(q, 2)
            b1, b2, b3, b4 = self.bits[q]
            if stage in (5, 6):
                p, others = self.last(q)
                for way, (device, place) in enumerate(others):
                    if stage == 5:
                        src, dst = self.s5.at[q, pl.ds(place, 1)], self.r5.at[s, q, pl.ds(way, 1)]
                    else:
                        src = dst = self.v7.at[vs, q, b4, pl.ds(p, 1)]
                    sems = self.send3.at[stage - 5, s, q, way], self.recv3.at[stage - 5, lax.rem(b, 3), q, way]
                    out.append((src, dst, *sems, device))
                continue
            if stage == 1:
                src, dst = self.blk.at[bs, j, pl.ds(56 * w + 28 * (1 - b1), 28)], self.r1.at[s, q]
            elif stage == 2:
                src, dst = self.s2.at[q], self.r2.at[s, q]
            elif stage == 3:
                src, dst = self.s3.at[q], self.r3.at[s, q]
            elif stage == 4:
                src, dst = self.s4.at[q], self.r4.at[s, q]
            elif stage == 7:
                src = dst = self.v7.at[vs, q, b4]
            elif stage == 8:
                src = dst = self.mine.at[ms, q, pl.ds(14 * b2 + 7 * b3, 7)]
            else:
                src = dst = self.mine.at[ms, q, pl.ds(14 * b2, 14)]
            i = list(EXCHANGE).index(stage)
            which = stage - 1 if stage < 5 else 10 - stage
            out.append((src, dst, self.send.at[i, s, q], self.recv.at[i, lax.rem(b, 4), q], self.peer[q][which]))
        return [
            pltpu.make_async_remote_copy(src_ref=src, dst_ref=dst, send_sem=send, recv_sem=recv, device_id={"dp": device}, device_id_type=MESH)
            for src, dst, send, recv, device in out
        ]

    def math(self, stage, b):
        s, bs, vs, ms = lax.rem(b, 2), lax.rem(b, NS), lax.rem(b, NV), lax.rem(b, NO)
        for q in range(Q):
            j, w = divmod(q, 2)
            b1, b2, b3, b4 = self.bits[q]
            if stage == 2:
                for keep, at in ((True, 14 * b2), (False, 14 * (1 - b2))):
                    total = add(self.blk[bs, j, pl.ds(56 * w + 28 * b1 + at, 14)], self.r1[s, q, pl.ds(at, 14)])
                    if keep:
                        self.k2[q] = total
                    else:
                        self.s2[q] = total.astype(bf16)
            elif stage == 3:
                for keep, at in ((True, 7 * b3), (False, 7 * (1 - b3))):
                    total = add(self.k2[q, pl.ds(at, 7)], self.r2[s, q, pl.ds(at, 7)])
                    if keep:
                        self.k3[q] = total
                    else:
                        self.s3[q] = total.astype(bf16)
            elif stage == 4:
                for keep, at in ((True, 3 * b4), (False, 3 * (1 - b4))):
                    total = add(self.k3[q, pl.ds(at, 4)], self.r3[s, q, pl.ds(at, 4)])
                    if keep:
                        self.k4[q] = total
                    else:
                        self.s4[q] = total.astype(bf16)
            elif stage == 5:
                p, _ = self.last(q)
                self.k5[q] = add(self.k4[q, pl.ds(p, 1)], self.r4[s, q, pl.ds(p, 1)])
                self.s5[q] = add(self.k4[q], self.r4[s, q]).astype(bf16)
            elif stage == 6:
                p, _ = self.last(q)
                g = add(self.k5[q], *(self.r5[s, q, pl.ds(way, 1)] for way in range(3))).astype(bf16)
                self.v7[vs, q, b4, pl.ds(p, 1)] = g
                square = g.astype(f32).reshape(2, 8, 128)
                square = square * square
                counts = jnp.where((b4 == 1) & (p == 0), 0.0, 1.0)
                self.ssq[...] += (square[0] + square[1]) * counts
            elif stage == 8:
                self.mine[ms, q, pl.ds(14 * b2 + 7 * b3, 4)] = self.v7[vs, q, 0]
                self.mine[ms, q, pl.ds(14 * b2 + 7 * b3 + 4, 3)] = self.v7[vs, q, 1, 1:4]

    def out(self, b):
        return [pltpu.make_async_copy(self.mine.at[lax.rem(b, NO), q], self.outs[q].at[b], self.gsem.at[lax.rem(b, 2), q]) for q in range(Q)]

    def stage(self, k, b):
        if 2 <= k <= 10:
            for c in self.copies(k - 1, b):
                c.wait()
        if k <= 9:
            self.math(k, b)
            for c in self.copies(k, b):
                c.start()
        elif k == 10:
            for c in self.out(b):
                c.start()
        else:
            for c in self.out(b):
                c.wait()

    def service(self, tick):
        for k in (*range(SUMMED, 0, -1), *range(LAST, SUMMED, -1)):
            made = tick - DUE[k]
            late = made >= NB + PAUSE
            now = (made >= 0) & (made <= END) & (late | (made < NB))
            pl.when(now)(functools.partial(self.stage, k, jnp.where(late, made - PAUSE, made)))

    def total(self, step):
        def copy(step):
            d, way = divmod(step, 2)
            return pltpu.make_async_remote_copy(
                src_ref=self.ssq_to.at[step],
                dst_ref=self.ssq_from.at[step],
                send_sem=self.qsend.at[step],
                recv_sem=self.qrecv.at[step],
                device_id={"dp": self.near[d][way]},
                device_id_type=MESH,
            )

        if step > 0:
            copy(step - 1).wait()
            self.ssq[...] += self.ssq_from[step - 1]
        if step < 6:
            self.ssq_to[step] = self.ssq[...]
            copy(step).start()


def gradients(names, x_hbm, dy_hbm, wg, wu, wd, *rest):
    outs, (ssq_out, s_hbm, ds_hbm, a0t_hbm, dgu_hbm), scratch = rest[:Q], rest[Q : Q + 5], rest[Q + 5 :]
    refs = dict(zip(names, scratch, strict=True))
    h, dy, a, a_t, dy_t, wgu, wdb, wd0, act0, dgu, sb, ub, xsem, isem, wsem, osem, tsem, dsem = (refs.pop(n) for n in OWN)
    comm = Comm(refs, outs)
    comm.hello()

    def fetch(layer, b, slot):
        return (
            pltpu.make_async_copy(wg.at[layer, :, block(b)], wgu.at[slot, :, 0:FB], wsem.at[slot, 0]),
            pltpu.make_async_copy(wu.at[layer, :, block(b)], wgu.at[slot, :, FB : 2 * FB], wsem.at[slot, 1]),
            *([pltpu.make_async_copy(wd.at[layer, block(b), :], wdb.at[slot], wsem.at[slot, 2])] if layer else []),
        )

    def part(t):
        return pltpu.make_async_copy(x_hbm.at[rows(t), :], h.at[rows(t), :], xsem.at[t])

    for t in range(NT):
        part(t).start()
    for c in fetch(0, 0, 0):
        c.start()
    get_dy = pltpu.make_async_copy(dy_hbm, dy, isem.at[0])
    get_dy.start()
    get_wd = pltpu.make_async_copy(wd.at[0], wd0, isem.at[1])
    get_wd.start()

    @pl.loop(0, NT)
    def _(t):
        part(t).wait()
        x = h[rows(t), :].astype(f32)
        a[rows(t), :] = (x * norm_scale(x)).astype(bf16)

    get_dy.wait()

    def kept(b, slot):
        return (
            pltpu.make_async_copy(sb.at[slot], s_hbm.at[b], osem.at[slot, 0]),
            pltpu.make_async_copy(ub.at[slot], ds_hbm.at[b], osem.at[slot, 1]),
        )

    def kept_t(t):
        return pltpu.make_async_copy(a_t.at[:, rows(t)], a0t_hbm.at[:, rows(t)], tsem.at[t])

    @pl.loop(0, NB)
    def _(b):
        slot = lax.rem(b, 2)

        @pl.when(b + 1 < NB)
        def _():
            for c in fetch(0, b + 1, 1 - slot):
                c.start()

        @pl.when(b >= 2)
        def _():
            for c in kept(b - 2, slot):
                c.wait()

        @pl.when((b >= 1) & (b < NT))
        def _():
            kept_t(b - 1).start()

        for c in fetch(0, b, slot):
            c.wait()
        turn = rows(jnp.minimum(b, NT - 1))
        a_t[:, turn] = a[turn, :].T
        dy_t[:, turn] = dy[turn, :].T
        for t in range(NT):
            r = pl.ds(t * TM, TM)
            both = dot(a[r, :], wgu[slot])
            gate, up = both[:, :FB], both[:, FB:]
            sg = sigmoid(gate)
            s = gate * sg
            act0[r, block(b)] = (s * up).astype(bf16)
            sb[slot, r, :] = s
            ub[slot, r, :] = up * (sg + (s - s * sg))
        for c in kept(b, slot):
            c.start()

    kept_t(NT - 1).start()
    for c in fetch(1, 0, 0):
        c.start()
    for t in range(NT):
        kept_t(t).wait()
    get_wd.wait()
    for t in range(NT):
        r = pl.ds(t * TM, TM)
        new = h[r, :] + dot(act0[r, :], wd0[...]).astype(bf16)
        h[r, :] = new
        new = new.astype(f32)
        new = (new * norm_scale(new)).astype(bf16)
        a[r, :] = new
        a_t[:, r] = new.T
    for b in (NB - 2, NB - 1):
        for c in kept(b, b % 2):
            c.wait()
    comm.barrier()

    def give(slot, d_gate_up, act):
        for start, size in ((0, 512), (512, D - 512)):
            g = dot(a_t[start : start + size, :], d_gate_up).astype(bf16)
            for j in range(2):
                for n in range(size // 8):
                    band, half = divmod(n, 2)
                    comm.blk[slot, j, start // 8 + n] = g[16 * band : 16 * band + 16, FB * j + 128 * half : FB * j + 128 * half + 128]
        for start, size in ((0, 512), (512, D - 512)):
            g = dot(dy_t[start : start + size, :], act).astype(bf16).T
            for band in range(16):
                for c in range(size // 128):
                    comm.blk[slot, 2, 7 * band + start // 128 + c] = g[16 * band : 16 * band + 16, 128 * c : 128 * c + 128]

    def keep_dgu(b):
        return pltpu.make_async_copy(dgu.at[lax.rem(b, 2)], dgu_hbm.at[b], dsem.at[lax.rem(b, 2)])

    @pl.loop(0, NB)
    def _(b):
        comm.service(b)
        slot = lax.rem(b, 2)

        @pl.when(b + 1 < NB)
        def _():
            for c in fetch(1, b + 1, 1 - slot):
                c.start()

        @pl.when(b >= 2)
        def _():
            keep_dgu(b - 2).wait()

        for c in fetch(1, b, slot):
            c.wait()
        for t in range(T // TB):
            r = pl.ds(t * TB, TB)
            both = dot(a[r, :], wgu[slot])
            gate, up = both[:, :FB], both[:, FB:]
            dact = dot_t(dy[r, :], wdb[slot]).astype(bf16).astype(f32)
            sg = sigmoid(gate)
            s = gate * sg
            sb[0, r, :] = (s * up).astype(bf16).astype(f32)
            dgu[slot, r, :FB] = (dact * up * (sg + (s - s * sg))).astype(bf16)
            dgu[slot, r, FB:] = (dact * s).astype(bf16)
        give(lax.rem(b, NS), dgu[slot], sb[0].astype(bf16))

        @pl.when(b < NB - 2)
        def _():
            keep_dgu(b).start()

    da = [(ref, k, min(FB, D - FB * (2 * i + k))) for i, ref in enumerate((sb, ub)) for k in range(2)]

    def again_dgu(i):
        b, slot = NB - 1 - i, lax.rem(i, 2)
        return (*fetch(1, b, slot)[:2], pltpu.make_async_copy(dgu_hbm.at[b], dgu.at[slot], dsem.at[slot]))

    @pl.loop(0, PAUSE)
    def _(n):
        comm.service(n + NB)

        @pl.loop(n * (NB // PAUSE), (n + 1) * (NB // PAUSE))
        def _(i):
            slot = lax.rem(i, 2)

            @pl.when((i >= 1) & (i + 1 < NB))
            def _():
                for c in again_dgu(i + 1):
                    c.start()

            @pl.when(i >= 2)
            def _():
                for c in again_dgu(i):
                    c.wait()

            for t in range(T // TB):
                r = pl.ds(t * TB, TB)
                more = dot_t(dgu[slot, r, :], wgu[slot])
                for f, (ref, part_of, size) in enumerate(da):
                    ref[part_of, r, :size] = jnp.where(i > 0, ref[part_of, r, :size], 0.0) + more[:, FB * f : FB * f + size]

    again = pltpu.make_async_copy(a0t_hbm, a_t, isem.at[0])
    again.start()

    def back(b, slot, r=slice(None)):
        return (
            pltpu.make_async_copy(s_hbm.at[b, r], sb.at[slot, r], osem.at[slot, 0]),
            pltpu.make_async_copy(ds_hbm.at[b, r], ub.at[slot, r], osem.at[slot, 1]),
        )

    @pl.loop(0, NT)
    def _(t):
        x = h[rows(t), :].astype(f32)
        scale = norm_scale(x)
        g = jnp.concatenate([ref[k, rows(t), :n] for ref, k, n in da], axis=1).astype(bf16).astype(f32)
        along = jnp.mean(g * x, -1, keepdims=True)
        dh = (g * scale - x * (scale * scale * scale * along)).astype(bf16) + dy[rows(t), :]
        dy[rows(t), :] = dh
        dy_t[:, rows(t)] = dh.T
        for c in back(0, 0, rows(t)):
            c.start()

    again.wait()

    @pl.loop(0, NB)
    def _(b):
        comm.service(b + NB + PAUSE)
        slot = lax.rem(b, 2)

        @pl.when(b + 1 < NB)
        def _():
            for c in back(b + 1, 1 - slot):
                c.start()

        for c in back(b, slot):
            c.wait()
        for t in range(T // TB):
            r = pl.ds(t * TB, TB)
            dact = dot_t(dy[r, :], wd0[block(b), :]).astype(bf16).astype(f32)
            dgu[0, r, :FB] = (dact * ub[slot, r, :]).astype(bf16)
            dgu[0, r, FB:] = (dact * sb[slot, r, :]).astype(bf16)
        give(lax.rem(b + NB, NS), dgu[0], act0[:, block(b)])

    @pl.loop(END + 1, END + DUE[LAST] + 1)
    def _(tick):
        comm.service(tick)
        for step in range(7):
            pl.when(tick == END + SUMMED + step)(functools.partial(comm.total, step))

    ssq_out[...] = comm.ssq[...]


OWN = ("h", "dy", "a", "a_t", "dy_t", "wgu", "wdb", "wd0", "act0", "dgu", "sb", "ub", "xsem", "isem", "wsem", "osem", "tsem", "dsem")


def run_gradients(x, dy, wg, wu, wd):
    own = dict(
        h=pltpu.VMEM((T, D), bf16),
        dy=pltpu.VMEM((T, D), bf16),
        a=pltpu.VMEM((T, D), bf16),
        a_t=pltpu.VMEM((D, T), bf16),
        dy_t=pltpu.VMEM((D, T), bf16),
        wgu=pltpu.VMEM((2, D, 2 * FB), bf16),
        wdb=pltpu.VMEM((2, FB, D), bf16),
        wd0=pltpu.VMEM((F, D), bf16),
        act0=pltpu.VMEM((T, F), bf16),
        dgu=pltpu.VMEM((2, T, 2 * FB), bf16),
        sb=pltpu.VMEM((2, T, FB), f32),
        ub=pltpu.VMEM((2, T, FB), f32),
        xsem=pltpu.SemaphoreType.DMA((NT,)),
        isem=pltpu.SemaphoreType.DMA((2,)),
        wsem=pltpu.SemaphoreType.DMA((2, 3)),
        osem=pltpu.SemaphoreType.DMA((2, 2)),
        tsem=pltpu.SemaphoreType.DMA((NT,)),
        dsem=pltpu.SemaphoreType.DMA((2,)),
    )
    scratch = own | comm_scratch()
    kept = sds((NB, T, FB), f32)
    *mine, ssq, _, _, _, _ = pl.pallas_call(
        functools.partial(gradients, tuple(scratch)),
        name="gradients",
        out_shape=(*(sds((NBLK, HALF, 16, 128), bf16) for _ in range(Q)), sds((8, 128), f32), kept, kept, sds((D, T), bf16), sds((NB, T, 2 * FB), bf16)),
        in_specs=[ANY] * 5,
        out_specs=(*(ANY for _ in range(Q)), VMEM, ANY, ANY, ANY, ANY),
        scratch_shapes=list(scratch.values()),
        compiler_params=pltpu.CompilerParams(collective_id=0, has_side_effects=True, vmem_limit_bytes=VMEM_LIMIT),
    )(x, dy, wg, wu, wd)
    return mine, ssq


SPLIT = 3
PER = LAYERS * 2 * (NB // SPLIT)
STEPS = 2 * PER
INS, OUTS = 4, 3
SHAPES = ((112, SPLIT * FB), (112, SPLIT * FB), (SPLIT, 32, D))


def adamw(other, ssq_ref, *refs):
    gs, arrays, refs = refs[:Q], refs[Q : Q + 9], refs[Q + 9 :]
    if other:
        refs = refs[9:]
    results, g_buf, in_buf, out_buf, (gsem, isem, osem) = refs[:9], refs[9], refs[10:19], refs[19:28], refs[28:]
    factor = jnp.minimum(1.0, 0.5 * lax.rsqrt(jnp.sum(ssq_ref[...], keepdims=True) / COUNT + 1e-30))
    bits = first_bits(lax.axis_index("dp"))

    def place(t):
        w, t = lax.div(t, PER), lax.rem(t, PER)
        n, t = lax.div(t, 2 * NB // SPLIT), lax.rem(t, 2 * NB // SPLIT)
        return w, n, lax.div(t, NB // SPLIT), lax.rem(t, NB // SPLIT)

    def window(t, k, ref):
        w, n, i, f = place(t)
        half = jnp.where(w == 0, bits[2 * k], bits[2 * k + 1])
        row = 4 * w + 2 * (1 - half if other else half) + i
        if k < 2:
            return ref.at[1 - n, pl.ds(pl.multiple_of(row * 112, 16), 112), pl.ds(pl.multiple_of(f * SPLIT * FB, 128), SPLIT * FB)]
        return ref.at[1 - n, pl.ds(f * SPLIT, SPLIT), pl.ds(pl.multiple_of(row * 32, 16), 32), :]

    def inward(t):
        s = lax.rem(t, INS)
        return [pltpu.make_async_copy(window(t, k % 3, arrays[k]), in_buf[k].at[s], isem.at[s, k]) for k in range(9)]

    def g_inward(t, w):
        s = lax.rem(t, INS)
        _, n, i, f = place(t)
        at = pl.ds(n * NB + f * SPLIT, SPLIT), pl.ds(14 * i, 14)
        return [pltpu.make_async_copy(gs[2 * k + w].at[at], g_buf.at[s, k], gsem.at[s, k]) for k in range(3)]

    def outward(t):
        s = lax.rem(t, OUTS)
        return [pltpu.make_async_copy(out_buf[k].at[s], window(t, k % 3, results[k]), osem.at[s, k]) for k in range(9)]

    def fetch(t):
        for c in inward(t):
            c.start()
        for w in range(2):

            @pl.when(lax.div(t, PER) == w)
            def _():
                for c in g_inward(t, w):
                    c.start()

    for t in range(INS - 1):
        fetch(t)

    @pl.loop(0, STEPS)
    def _(t):
        s, o = lax.rem(t, INS), lax.rem(t, OUTS)

        @pl.when(t + INS - 1 < STEPS)
        def _():
            fetch(t + INS - 1)

        @pl.when(t >= OUTS)
        def _():
            for c in outward(t - OUTS):
                c.wait()

        for c in inward(t) + g_inward(t, 0):
            c.wait()

        def update(k, where, g):
            weight, m, v = (in_buf[i + k][(s, *where)].astype(f32) for i in (0, 3, 6))
            g = g.astype(f32) * factor
            m = 0.9 * m + 0.1 * g
            v = 0.95 * v + 0.05 * g * g
            step = m * lax.rsqrt(v + 1e-8) + 0.1 * weight
            out_buf[k][(o, *where)] = (weight - 0.02 * step).astype(bf16)
            out_buf[3 + k][(o, *where)] = m
            out_buf[6 + k][(o, *where)] = v

        for b in range(SPLIT):
            for k in range(3):
                if k < 2:
                    g = g_buf[s, k, b].reshape(7, 2, 16, 128)
                    for half in range(2):
                        update(k, (slice(None), slice(b * FB + half * 128, b * FB + half * 128 + 128)), g[:, half].reshape(112, 128))
                else:
                    g = g_buf[s, k, b].reshape(2, 7, 16, 128)
                    for c in range(7):
                        update(k, (b, slice(None), slice(c * 128, c * 128 + 128)), g[:, c].reshape(32, 128))
        for c in outward(t):
            c.start()

    for t in range(STEPS - OUTS, STEPS):
        for c in outward(t):
            c.wait()


def run_adamw(other, ssq, gs, arrays, so_far):
    arrays = [a.reshape(LAYERS, NB, FB, D) if k % 3 == 2 else a for k, a in enumerate(arrays)]

    def held(n):
        return [pltpu.VMEM((n, *SHAPES[k % 3]), arrays[k].dtype) for k in range(9)]

    return pl.pallas_call(
        functools.partial(adamw, other),
        name="adamw",
        in_specs=[VMEM] + [ANY] * (Q + 9 + len(so_far)),
        out_specs=(ANY,) * 9,
        out_shape=tuple(sds(a.shape, a.dtype) for a in arrays),
        scratch_shapes=[
            pltpu.VMEM((INS, 3, SPLIT, 14, 16, 128), bf16),
            *held(INS),
            *held(OUTS),
            pltpu.SemaphoreType.DMA((INS, 3)),
            pltpu.SemaphoreType.DMA((INS, 9)),
            pltpu.SemaphoreType.DMA((OUTS, 9)),
        ],
        input_output_aliases={1 + Q + 9 + k: k for k in range(len(so_far))},
        cost_estimate=pl.CostEstimate(flops=100_000_000_000, bytes_accessed=136_000_000, transcendentals=0),
        compiler_params=pltpu.CompilerParams(vmem_limit_bytes=VMEM_LIMIT),
    )(ssq, *gs, *arrays, *so_far)


def swaps(q):
    j, w = divmod(q, 2)
    s = STRIDE[j]
    out = []
    for me in range(64):
        p = me // s % 4
        out.append((me, me + ((3 - p if w else p ^ 1) - p) * s))
    return out


def solution(mesh):
    def step(x, dy, *arrays):
        mine, ssq = run_gradients(x[0], dy[0], *arrays[:3])
        theirs = [lax.ppermute(g, "dp", swaps(q)) for q, g in enumerate(mine)]
        new = run_adamw(False, ssq, mine, arrays, ())
        new = run_adamw(True, ssq, theirs, arrays, new)
        return tuple(n.reshape(a.shape) for n, a in zip(new, arrays, strict=True))

    return jax.shard_map(
        step,
        mesh=mesh,
        in_specs=(P(("rep", "dp"), None, None),) * 2 + (P(None, None, None),) * 9,
        out_specs=(P("rep", None, None),) * 9,
        check_vma=False,
    )
```

```python
import functools

import jax
import jax.numpy as jnp
from jax import lax
from jax.experimental import pallas as pl
from jax.experimental.pallas import tpu as pltpu
from jax.sharding import PartitionSpec as P

T, D, F = 2048, 896, 2304
FB = 256
NB = F // FB
LAYERS = 2
NBLK = NB * LAYERS
COUNT = 3 * LAYERS * D * F
TM = 256
NT = T // TM
TB = 512
f32, bf16 = jnp.float32, jnp.bfloat16
MESH = pl.DeviceIdType.MESH
VMEM_LIMIT = 67_043_328
ANY = pl.BlockSpec(memory_space=pl.ANY)
VMEM = pl.BlockSpec(memory_space=pltpu.VMEM)
sds = jax.ShapeDtypeStruct


def dot(a, b):
    return jnp.dot(a, b, preferred_element_type=f32)


def dot_t(a, b):
    return lax.dot_general(a, b, (((1,), (1,)), ((), ())), preferred_element_type=f32)


def sigmoid(x):
    return 1.0 / (1.0 + jnp.exp(-x))


def norm_scale(h):
    return lax.rsqrt(jnp.mean(h * h, -1, keepdims=True) + 1e-6)


def rows(t):
    return pl.ds(pl.multiple_of(t * TM, TM), TM)


def block(b):
    return pl.ds(pl.multiple_of(b * FB, FB), FB)


STRIDE = (16, 4, 1)
Q = 6
NS, NG, NV, NO = 2, 3, 4, 7
DUE = {1: 1, 2: 2, 3: 3, 4: 4, 5: 5, 6: 6, 7: 7, 8: 9, 9: 11, 10: 13, 11: 14}
SUMMED, LAST = 6, 11
PAUSE = 3
END = NBLK - 1 + PAUSE
HALF = 28


def comm_scratch():
    def v(*shape, dtype=bf16):
        return pltpu.VMEM((*shape, 16, 128), dtype)

    return dict(
        blk=v(NS, 3, 112),
        r1=v(2, Q, 28),
        r2=v(2, Q, 14),
        r3=v(2, Q, 7),
        r4=v(2, Q, 4),
        r5=v(2, 3, 3, 2),
        s2=v(Q, 14),
        s3=v(Q, 7),
        s4=v(Q, 4),
        s5=v(3, 4, 2),
        k2=v(Q, 14, dtype=f32),
        k3=v(Q, 7, dtype=f32),
        k4=v(Q, 4, dtype=f32),
        k5=v(Q, 1, dtype=f32),
        g6=v(NG, 3, 4, 2),
        v7=v(NV, Q, 2, 4),
        mine=v(NO, Q, HALF),
        ssq=pltpu.VMEM((8, 128), f32),
        ssq_at=pltpu.VMEM((3, 4, 8, 128), f32),
        send=pltpu.SemaphoreType.DMA((4, Q)),
        recv=pltpu.SemaphoreType.DMA((4, 2, Q)),
        send5=pltpu.SemaphoreType.DMA((3, 3)),
        recv5=pltpu.SemaphoreType.DMA((2, 3, 3)),
        send6=pltpu.SemaphoreType.DMA((2, 3, 3)),
        recv6=pltpu.SemaphoreType.DMA((3, 3, 3)),
        send7=pltpu.SemaphoreType.DMA((3, 2, Q)),
        recv7=pltpu.SemaphoreType.DMA((3, 4, Q)),
        gsem=pltpu.SemaphoreType.DMA((2, Q)),
        qsend=pltpu.SemaphoreType.DMA((3, 3)),
        qrecv=pltpu.SemaphoreType.DMA((3, 3)),
    )


def parity(p):
    return lax.rem(lax.div(p + 1, 2), 2)


def upper(p):
    return lax.div(p, 2)


def position(me):
    return [lax.rem(lax.div(me, s), 4) for s in STRIDE]


def first_bits(me):
    pos = position(me)
    return [(parity, upper)[q % 2](pos[q // 2]) for q in range(Q)]


def add(*terms):
    total = terms[0].astype(f32)
    for t in terms[1:]:
        total = total + t.astype(f32)
    return total


class Comm:
    def __init__(self, refs, outs):
        self.__dict__.update(refs)
        self.outs = outs
        me = lax.axis_index("dp")
        pos = position(me)
        self.pos = pos
        self.near = []
        for p, s in zip(pos, STRIDE):
            base = me - p * s
            self.near.append((base + (p + 1 - 2 * lax.rem(p, 2)) * s, base + (3 - p) * s, base + lax.rem(p + 2, 4) * s))
        self.bits, self.peer = [], []
        for q in range(Q):
            j, w = divmod(q, 2)
            bits, peer = [], []
            for d in (j, (j + 1) % 3):
                for way in (w, 1 - w):
                    bits.append((parity, upper)[way](pos[d]))
                    peer.append(self.near[d][way])
            self.bits.append(bits)
            self.peer.append(peer)
        self.ssq[...] = jnp.zeros((8, 128), f32)

    def hello(self):
        for ring in self.near:
            for device in ring:
                pl.semaphore_signal(pltpu.get_barrier_semaphore(), inc=1, device_id={"dp": device}, device_id_type=MESH)

    def barrier(self):
        pl.semaphore_wait(pltpu.get_barrier_semaphore(), 9)

    def last(self, j):
        d = (j + 2) % 3
        p = self.pos[d]
        places = (p + 1 - 2 * lax.rem(p, 2), 3 - p, lax.rem(p + 2, 4))
        return p, tuple(zip(self.near[d], places))

    def copies(self, stage, b):
        s, bs, gs, vs, ms = lax.rem(b, 2), lax.rem(b, NS), lax.rem(b, NG), lax.rem(b, NV), lax.rem(b, NO)
        out = []
        if stage in (5, 6):
            for j in range(3):
                p, others = self.last(j)
                for way, (device, place) in enumerate(others):
                    if stage == 5:
                        ends = self.s5.at[j, place], self.r5.at[s, j, way], self.send5.at[j, way], self.recv5.at[s, j, way]
                    else:
                        part = self.g6.at[gs, j, p]
                        ends = part, part, self.send6.at[s, j, way], self.recv6.at[lax.rem(b, 3), j, way]
                    out.append((*ends, device))
        else:
            for q in range(Q):
                j, w = divmod(q, 2)
                b1, b2, b3, b4 = self.bits[q]
                if stage == 1:
                    src, dst = self.blk.at[bs, j, pl.ds(56 * w + 28 * (1 - b1), 28)], self.r1.at[s, q]
                elif stage == 2:
                    src, dst = self.s2.at[q], self.r2.at[s, q]
                elif stage == 3:
                    src, dst = self.s3.at[q], self.r3.at[s, q]
                elif stage == 4:
                    src, dst = self.s4.at[q], self.r4.at[s, q]
                elif stage == 7:
                    src = dst = self.v7.at[vs, q, b4]
                elif stage == 8:
                    src = dst = self.mine.at[ms, q, pl.ds(14 * b2 + 7 * b3, 7)]
                else:
                    src = dst = self.mine.at[ms, q, pl.ds(14 * b2, 14)]
                if stage < 5:
                    out.append((src, dst, self.send.at[stage - 1, q], self.recv.at[stage - 1, s, q], self.peer[q][stage - 1]))
                else:
                    out.append((src, dst, self.send7.at[stage - 7, s, q], self.recv7.at[stage - 7, lax.rem(b, 4), q], self.peer[q][10 - stage]))
        return [
            pltpu.make_async_remote_copy(src_ref=src, dst_ref=dst, send_sem=send, recv_sem=recv, device_id={"dp": device}, device_id_type=MESH)
            for src, dst, send, recv, device in out
        ]

    def math(self, stage, b):
        s, bs, gs, vs, ms = lax.rem(b, 2), lax.rem(b, NS), lax.rem(b, NG), lax.rem(b, NV), lax.rem(b, NO)
        for q in range(Q):
            j, w = divmod(q, 2)
            b1, b2, b3, b4 = self.bits[q]
            if stage == 2:
                for keep, at in ((True, 14 * b2), (False, 14 * (1 - b2))):
                    total = add(self.blk[bs, j, pl.ds(56 * w + 28 * b1 + at, 14)], self.r1[s, q, pl.ds(at, 14)])
                    if keep:
                        self.k2[q] = total
                    else:
                        self.s2[q] = total.astype(bf16)
            elif stage == 3:
                for keep, at in ((True, 7 * b3), (False, 7 * (1 - b3))):
                    total = add(self.k2[q, pl.ds(at, 7)], self.r2[s, q, pl.ds(at, 7)])
                    if keep:
                        self.k3[q] = total
                    else:
                        self.s3[q] = total.astype(bf16)
            elif stage == 4:
                for keep, at in ((True, 3 * b4), (False, 3 * (1 - b4))):
                    total = add(self.k3[q, pl.ds(at, 4)], self.r3[s, q, pl.ds(at, 4)])
                    if keep:
                        self.k4[q] = total
                    else:
                        self.s4[q] = total.astype(bf16)
            elif stage == 5:
                p, _ = self.last(j)
                self.k5[q] = add(self.k4[q, pl.ds(p, 1)], self.r4[s, q, pl.ds(p, 1)])
                self.s5[j, :, w] = add(self.k4[q], self.r4[s, q]).astype(bf16)
            elif stage == 6:
                p, _ = self.last(j)
                g = add(self.k5[q], *(self.r5[s, j, way, pl.ds(w, 1)] for way in range(3))).astype(bf16)
                self.g6[gs, j, p, pl.ds(w, 1)] = g
                square = g.astype(f32).reshape(2, 8, 128)
                square = square * square
                counts = jnp.where((b4 == 1) & (p == 0), 0.0, 1.0)
                self.ssq[...] += (square[0] + square[1]) * counts
            elif stage == 7:
                self.v7[vs, q, b4] = self.g6[gs, j, :, w]
            elif stage == 8:
                self.mine[ms, q, pl.ds(14 * b2 + 7 * b3, 4)] = self.v7[vs, q, 0]
                self.mine[ms, q, pl.ds(14 * b2 + 7 * b3 + 4, 3)] = self.v7[vs, q, 1, 1:4]

    def out(self, b):
        return [pltpu.make_async_copy(self.mine.at[lax.rem(b, NO), q], self.outs[q].at[b], self.gsem.at[lax.rem(b, 2), q]) for q in range(Q)]

    def stage(self, k, b):
        if 2 <= k <= 10:
            for c in self.copies(k - 1, b):
                c.wait()
        if k <= 9:
            self.math(k, b)
            for c in self.copies(k, b):
                c.start()
        elif k == 10:
            for c in self.out(b):
                c.start()
        else:
            for c in self.out(b):
                c.wait()

    def service(self, tick):
        for k in (*range(SUMMED, 0, -1), *range(LAST, SUMMED, -1)):
            made = tick - DUE[k]
            late = made >= NB + PAUSE
            now = (made >= 0) & (made <= END) & (late | (made < NB))
            pl.when(now)(functools.partial(self.stage, k, jnp.where(late, made - PAUSE, made)))

    def total(self, step):
        def copies(d):
            part = self.ssq_at.at[d, self.pos[d]]
            return [
                pltpu.make_async_remote_copy(
                    src_ref=part,
                    dst_ref=part,
                    send_sem=self.qsend.at[d, way],
                    recv_sem=self.qrecv.at[d, way],
                    device_id={"dp": device},
                    device_id_type=MESH,
                )
                for way, device in enumerate(self.near[d])
            ]

        if step > 0:
            for c in copies(step - 1):
                c.wait()
            self.ssq[...] = add(*(self.ssq_at[step - 1, k] for k in range(4)))
        if step < 3:
            self.ssq_at[step, self.pos[step]] = self.ssq[...]
            for c in copies(step):
                c.start()


def gradients(names, x_hbm, dy_hbm, wg, wu, wd, *rest):
    outs, (ssq_out, s_hbm, ds_hbm, a0t_hbm, dgu_hbm), scratch = rest[:Q], rest[Q : Q + 5], rest[Q + 5 :]
    refs = dict(zip(names, scratch, strict=True))
    h, dy, a, a_t, dy_t, wgu, wdb, wd0, act0, dgu, sb, ub, xsem, isem, wsem, osem, tsem, dsem = (refs.pop(n) for n in OWN)
    comm = Comm(refs, outs)
    comm.hello()

    def fetch(layer, b, slot):
        return (
            pltpu.make_async_copy(wg.at[layer, :, block(b)], wgu.at[slot, :, 0:FB], wsem.at[slot, 0]),
            pltpu.make_async_copy(wu.at[layer, :, block(b)], wgu.at[slot, :, FB : 2 * FB], wsem.at[slot, 1]),
            *([pltpu.make_async_copy(wd.at[layer, block(b), :], wdb.at[slot], wsem.at[slot, 2])] if layer else []),
        )

    def part(t):
        return pltpu.make_async_copy(x_hbm.at[rows(t), :], h.at[rows(t), :], xsem.at[t])

    for t in range(NT):
        part(t).start()
    for c in fetch(0, 0, 0):
        c.start()
    get_dy = pltpu.make_async_copy(dy_hbm, dy, isem.at[0])
    get_dy.start()
    get_wd = pltpu.make_async_copy(wd.at[0], wd0, isem.at[1])
    get_wd.start()

    @pl.loop(0, NT)
    def _(t):
        part(t).wait()
        x = h[rows(t), :].astype(f32)
        a[rows(t), :] = (x * norm_scale(x)).astype(bf16)

    get_dy.wait()

    def kept(b, slot):
        return (
            pltpu.make_async_copy(sb.at[slot], s_hbm.at[b], osem.at[slot, 0]),
            pltpu.make_async_copy(ub.at[slot], ds_hbm.at[b], osem.at[slot, 1]),
        )

    def kept_t(t):
        return pltpu.make_async_copy(a_t.at[:, rows(t)], a0t_hbm.at[:, rows(t)], tsem.at[t])

    @pl.loop(0, NB)
    def _(b):
        slot = lax.rem(b, 2)

        @pl.when(b + 1 < NB)
        def _():
            for c in fetch(0, b + 1, 1 - slot):
                c.start()

        @pl.when(b >= 2)
        def _():
            for c in kept(b - 2, slot):
                c.wait()

        @pl.when((b >= 1) & (b < NT))
        def _():
            kept_t(b - 1).start()

        for c in fetch(0, b, slot):
            c.wait()
        turn = rows(jnp.minimum(b, NT - 1))
        a_t[:, turn] = a[turn, :].T
        dy_t[:, turn] = dy[turn, :].T
        for t in range(NT):
            r = pl.ds(t * TM, TM)
            both = dot(a[r, :], wgu[slot])
            gate, up = both[:, :FB], both[:, FB:]
            sg = sigmoid(gate)
            s = gate * sg
            act0[r, block(b)] = (s * up).astype(bf16)
            sb[slot, r, :] = s
            ub[slot, r, :] = up * (sg + (s - s * sg))
        for c in kept(b, slot):
            c.start()

    kept_t(NT - 1).start()
    for c in fetch(1, 0, 0):
        c.start()
    for t in range(NT):
        kept_t(t).wait()
    get_wd.wait()
    for t in range(NT):
        r = pl.ds(t * TM, TM)
        new = h[r, :] + dot(act0[r, :], wd0[...]).astype(bf16)
        h[r, :] = new
        new = new.astype(f32)
        new = (new * norm_scale(new)).astype(bf16)
        a[r, :] = new
        a_t[:, r] = new.T
    for b in (NB - 2, NB - 1):
        for c in kept(b, b % 2):
            c.wait()
    comm.barrier()

    def give(slot, d_gate_up, act):
        for start, size in ((0, 512), (512, D - 512)):
            g = dot(a_t[start : start + size, :], d_gate_up).astype(bf16)
            for j in range(2):
                for n in range(size // 8):
                    band, half = divmod(n, 2)
                    comm.blk[slot, j, start // 8 + n] = g[16 * band : 16 * band + 16, FB * j + 128 * half : FB * j + 128 * half + 128]
        for start, size in ((0, 512), (512, D - 512)):
            g = dot(dy_t[start : start + size, :], act).astype(bf16).T
            for band in range(16):
                for c in range(size // 128):
                    comm.blk[slot, 2, 7 * band + start // 128 + c] = g[16 * band : 16 * band + 16, 128 * c : 128 * c + 128]

    def keep_dgu(b):
        return pltpu.make_async_copy(dgu.at[lax.rem(b, 2)], dgu_hbm.at[b], dsem.at[lax.rem(b, 2)])

    @pl.loop(0, NB)
    def _(b):
        comm.service(b)
        slot = lax.rem(b, 2)

        @pl.when(b + 1 < NB)
        def _():
            for c in fetch(1, b + 1, 1 - slot):
                c.start()

        @pl.when(b >= 2)
        def _():
            keep_dgu(b - 2).wait()

        for c in fetch(1, b, slot):
            c.wait()
        for t in range(T // TB):
            r = pl.ds(t * TB, TB)
            both = dot(a[r, :], wgu[slot])
            gate, up = both[:, :FB], both[:, FB:]
            dact = dot_t(dy[r, :], wdb[slot]).astype(bf16).astype(f32)
            sg = sigmoid(gate)
            s = gate * sg
            sb[0, r, :] = (s * up).astype(bf16).astype(f32)
            dgu[slot, r, :FB] = (dact * up * (sg + (s - s * sg))).astype(bf16)
            dgu[slot, r, FB:] = (dact * s).astype(bf16)
        give(lax.rem(b, NS), dgu[slot], sb[0].astype(bf16))

        @pl.when(b < NB - 2)
        def _():
            keep_dgu(b).start()

    da = [(ref, k, min(FB, D - FB * (2 * i + k))) for i, ref in enumerate((sb, ub)) for k in range(2)]

    def again_dgu(i):
        b, slot = NB - 1 - i, lax.rem(i, 2)
        return (*fetch(1, b, slot)[:2], pltpu.make_async_copy(dgu_hbm.at[b], dgu.at[slot], dsem.at[slot]))

    @pl.loop(0, PAUSE)
    def _(n):
        comm.service(n + NB)

        @pl.loop(n * (NB // PAUSE), (n + 1) * (NB // PAUSE))
        def _(i):
            slot = lax.rem(i, 2)

            @pl.when((i >= 1) & (i + 1 < NB))
            def _():
                for c in again_dgu(i + 1):
                    c.start()

            @pl.when(i >= 2)
            def _():
                for c in again_dgu(i):
                    c.wait()

            for t in range(T // TB):
                r = pl.ds(t * TB, TB)
                more = dot_t(dgu[slot, r, :], wgu[slot])
                for f, (ref, part_of, size) in enumerate(da):
                    ref[part_of, r, :size] = jnp.where(i > 0, ref[part_of, r, :size], 0.0) + more[:, FB * f : FB * f + size]

    again = pltpu.make_async_copy(a0t_hbm, a_t, isem.at[0])
    again.start()

    def back(b, slot, r=slice(None)):
        return (
            pltpu.make_async_copy(s_hbm.at[b, r], sb.at[slot, r], osem.at[slot, 0]),
            pltpu.make_async_copy(ds_hbm.at[b, r], ub.at[slot, r], osem.at[slot, 1]),
        )

    @pl.loop(0, NT)
    def _(t):
        x = h[rows(t), :].astype(f32)
        scale = norm_scale(x)
        g = jnp.concatenate([ref[k, rows(t), :n] for ref, k, n in da], axis=1).astype(bf16).astype(f32)
        along = jnp.mean(g * x, -1, keepdims=True)
        dh = (g * scale - x * (scale * scale * scale * along)).astype(bf16) + dy[rows(t), :]
        dy[rows(t), :] = dh
        dy_t[:, rows(t)] = dh.T
        for c in back(0, 0, rows(t)):
            c.start()

    again.wait()

    @pl.loop(0, NB)
    def _(b):
        comm.service(b + NB + PAUSE)
        slot = lax.rem(b, 2)

        @pl.when(b + 1 < NB)
        def _():
            for c in back(b + 1, 1 - slot):
                c.start()

        for c in back(b, slot):
            c.wait()
        for t in range(T // TB):
            r = pl.ds(t * TB, TB)
            dact = dot_t(dy[r, :], wd0[block(b), :]).astype(bf16).astype(f32)
            dgu[0, r, :FB] = (dact * ub[slot, r, :]).astype(bf16)
            dgu[0, r, FB:] = (dact * sb[slot, r, :]).astype(bf16)
        give(lax.rem(b + NB, NS), dgu[0], act0[:, block(b)])

    @pl.loop(END + 1, END + DUE[LAST] + 1)
    def _(tick):
        comm.service(tick)
        for step in range(4):
            pl.when(tick == END + SUMMED + 2 * step)(functools.partial(comm.total, step))

    ssq_out[...] = comm.ssq[...]


OWN = ("h", "dy", "a", "a_t", "dy_t", "wgu", "wdb", "wd0", "act0", "dgu", "sb", "ub", "xsem", "isem", "wsem", "osem", "tsem", "dsem")


def run_gradients(x, dy, wg, wu, wd):
    own = dict(
        h=pltpu.VMEM((T, D), bf16),
        dy=pltpu.VMEM((T, D), bf16),
        a=pltpu.VMEM((T, D), bf16),
        a_t=pltpu.VMEM((D, T), bf16),
        dy_t=pltpu.VMEM((D, T), bf16),
        wgu=pltpu.VMEM((2, D, 2 * FB), bf16),
        wdb=pltpu.VMEM((2, FB, D), bf16),
        wd0=pltpu.VMEM((F, D), bf16),
        act0=pltpu.VMEM((T, F), bf16),
        dgu=pltpu.VMEM((2, T, 2 * FB), bf16),
        sb=pltpu.VMEM((2, T, FB), f32),
        ub=pltpu.VMEM((2, T, FB), f32),
        xsem=pltpu.SemaphoreType.DMA((NT,)),
        isem=pltpu.SemaphoreType.DMA((2,)),
        wsem=pltpu.SemaphoreType.DMA((2, 3)),
        osem=pltpu.SemaphoreType.DMA((2, 2)),
        tsem=pltpu.SemaphoreType.DMA((NT,)),
        dsem=pltpu.SemaphoreType.DMA((2,)),
    )
    scratch = own | comm_scratch()
    kept = sds((NB, T, FB), f32)
    *mine, ssq, _, _, _, _ = pl.pallas_call(
        functools.partial(gradients, tuple(scratch)),
        name="gradients",
        out_shape=(*(sds((NBLK, HALF, 16, 128), bf16) for _ in range(Q)), sds((8, 128), f32), kept, kept, sds((D, T), bf16), sds((NB, T, 2 * FB), bf16)),
        in_specs=[ANY] * 5,
        out_specs=(*(ANY for _ in range(Q)), VMEM, ANY, ANY, ANY, ANY),
        scratch_shapes=list(scratch.values()),
        compiler_params=pltpu.CompilerParams(collective_id=0, has_side_effects=True, vmem_limit_bytes=VMEM_LIMIT),
    )(x, dy, wg, wu, wd)
    return mine, ssq


SPLIT = 3
PER = LAYERS * 2 * (NB // SPLIT)
STEPS = 2 * PER
INS, OUTS = 4, 3
SHAPES = ((112, SPLIT * FB), (112, SPLIT * FB), (SPLIT, 32, D))


def adamw(other, ssq_ref, *refs):
    gs, arrays, refs = refs[:Q], refs[Q : Q + 9], refs[Q + 9 :]
    if other:
        refs = refs[9:]
    results, g_buf, in_buf, out_buf, (gsem, isem, osem) = refs[:9], refs[9], refs[10:19], refs[19:28], refs[28:]
    factor = jnp.minimum(1.0, 0.5 * lax.rsqrt(jnp.sum(ssq_ref[...], keepdims=True) / COUNT + 1e-30))
    bits = first_bits(lax.axis_index("dp"))

    def place(t):
        w, t = lax.div(t, PER), lax.rem(t, PER)
        n, t = lax.div(t, 2 * NB // SPLIT), lax.rem(t, 2 * NB // SPLIT)
        return w, n, lax.div(t, NB // SPLIT), lax.rem(t, NB // SPLIT)

    def window(t, k, ref):
        w, n, i, f = place(t)
        half = jnp.where(w == 0, bits[2 * k], bits[2 * k + 1])
        row = 4 * w + 2 * (1 - half if other else half) + i
        if k < 2:
            return ref.at[1 - n, pl.ds(pl.multiple_of(row * 112, 16), 112), pl.ds(pl.multiple_of(f * SPLIT * FB, 128), SPLIT * FB)]
        return ref.at[1 - n, pl.ds(f * SPLIT, SPLIT), pl.ds(pl.multiple_of(row * 32, 16), 32), :]

    def inward(t):
        s = lax.rem(t, INS)
        return [pltpu.make_async_copy(window(t, k % 3, arrays[k]), in_buf[k].at[s], isem.at[s, k]) for k in range(9)]

    def g_inward(t, w):
        s = lax.rem(t, INS)
        _, n, i, f = place(t)
        at = pl.ds(n * NB + f * SPLIT, SPLIT), pl.ds(14 * i, 14)
        return [pltpu.make_async_copy(gs[2 * k + w].at[at], g_buf.at[s, k], gsem.at[s, k]) for k in range(3)]

    def outward(t):
        s = lax.rem(t, OUTS)
        return [pltpu.make_async_copy(out_buf[k].at[s], window(t, k % 3, results[k]), osem.at[s, k]) for k in range(9)]

    def fetch(t):
        for c in inward(t):
            c.start()
        for w in range(2):

            @pl.when(lax.div(t, PER) == w)
            def _():
                for c in g_inward(t, w):
                    c.start()

    for t in range(INS - 1):
        fetch(t)

    @pl.loop(0, STEPS)
    def _(t):
        s, o = lax.rem(t, INS), lax.rem(t, OUTS)

        @pl.when(t + INS - 1 < STEPS)
        def _():
            fetch(t + INS - 1)

        @pl.when(t >= OUTS)
        def _():
            for c in outward(t - OUTS):
                c.wait()

        for c in inward(t) + g_inward(t, 0):
            c.wait()

        def update(k, where, g):
            weight, m, v = (in_buf[i + k][(s, *where)].astype(f32) for i in (0, 3, 6))
            g = g.astype(f32) * factor
            m = 0.9 * m + 0.1 * g
            v = 0.95 * v + 0.05 * g * g
            step = m * lax.rsqrt(v + 1e-8) + 0.1 * weight
            out_buf[k][(o, *where)] = (weight - 0.02 * step).astype(bf16)
            out_buf[3 + k][(o, *where)] = m
            out_buf[6 + k][(o, *where)] = v

        for b in range(SPLIT):
            for k in range(3):
                if k < 2:
                    g = g_buf[s, k, b].reshape(7, 2, 16, 128)
                    for half in range(2):
                        update(k, (slice(None), slice(b * FB + half * 128, b * FB + half * 128 + 128)), g[:, half].reshape(112, 128))
                else:
                    g = g_buf[s, k, b].reshape(2, 7, 16, 128)
                    for c in range(7):
                        update(k, (b, slice(None), slice(c * 128, c * 128 + 128)), g[:, c].reshape(32, 128))
        for c in outward(t):
            c.start()

    for t in range(STEPS - OUTS, STEPS):
        for c in outward(t):
            c.wait()


def run_adamw(other, ssq, gs, arrays, so_far):
    arrays = [a.reshape(LAYERS, NB, FB, D) if k % 3 == 2 else a for k, a in enumerate(arrays)]

    def held(n):
        return [pltpu.VMEM((n, *SHAPES[k % 3]), arrays[k].dtype) for k in range(9)]

    return pl.pallas_call(
        functools.partial(adamw, other),
        name="adamw",
        in_specs=[VMEM] + [ANY] * (Q + 9 + len(so_far)),
        out_specs=(ANY,) * 9,
        out_shape=tuple(sds(a.shape, a.dtype) for a in arrays),
        scratch_shapes=[
            pltpu.VMEM((INS, 3, SPLIT, 14, 16, 128), bf16),
            *held(INS),
            *held(OUTS),
            pltpu.SemaphoreType.DMA((INS, 3)),
            pltpu.SemaphoreType.DMA((INS, 9)),
            pltpu.SemaphoreType.DMA((OUTS, 9)),
        ],
        input_output_aliases={1 + Q + 9 + k: k for k in range(len(so_far))},
        cost_estimate=pl.CostEstimate(flops=100_000_000_000, bytes_accessed=136_000_000, transcendentals=0),
        compiler_params=pltpu.CompilerParams(vmem_limit_bytes=VMEM_LIMIT),
    )(ssq, *gs, *arrays, *so_far)


def swaps(q):
    j, w = divmod(q, 2)
    s = STRIDE[j]
    out = []
    for me in range(64):
        p = me // s % 4
        out.append((me, me + ((3 - p if w else p ^ 1) - p) * s))
    return out


def solution(mesh):
    def step(x, dy, *arrays):
        mine, ssq = run_gradients(x[0], dy[0], *arrays[:3])
        theirs = [lax.ppermute(g, "dp", swaps(q)) for q, g in enumerate(mine)]
        new = run_adamw(False, ssq, mine, arrays, ())
        new = run_adamw(True, ssq, theirs, arrays, new)
        return tuple(n.reshape(a.shape) for n, a in zip(new, arrays, strict=True))

    return jax.shard_map(
        step,
        mesh=mesh,
        in_specs=(P(("rep", "dp"), None, None),) * 2 + (P(None, None, None),) * 9,
        out_specs=(P("rep", None, None),) * 9,
        check_vma=False,
    )
```

```python
import functools

import jax
import jax.numpy as jnp
from jax import lax
from jax.experimental import pallas as pl
from jax.experimental.pallas import tpu as pltpu
from jax.sharding import PartitionSpec as P

T, D, F = 2048, 896, 2304
FB = 256
NB = F // FB
LAYERS = 2
NBLK = NB * LAYERS
COUNT = 3 * LAYERS * D * F
TM = 256
NT = T // TM
TB = 512
f32, bf16 = jnp.float32, jnp.bfloat16
MESH = pl.DeviceIdType.MESH
VMEM_LIMIT = 67_043_328
ANY = pl.BlockSpec(memory_space=pl.ANY)
VMEM = pl.BlockSpec(memory_space=pltpu.VMEM)
sds = jax.ShapeDtypeStruct


def dot(a, b):
    return jnp.dot(a, b, preferred_element_type=f32)


def dot_t(a, b):
    return lax.dot_general(a, b, (((1,), (1,)), ((), ())), preferred_element_type=f32)


def sigmoid(x):
    return 1.0 / (1.0 + jnp.exp(-x))


def norm_scale(h):
    return lax.rsqrt(jnp.mean(h * h, -1, keepdims=True) + 1e-6)


def rows(t):
    return pl.ds(pl.multiple_of(t * TM, TM), TM)


def block(b):
    return pl.ds(pl.multiple_of(b * FB, FB), FB)


STRIDE = (16, 4, 1)
Q = 6
NS, NG, NV, NO = 2, 3, 4, 7
DUE = {1: 1, 2: 2, 3: 3, 4: 4, 5: 5, 6: 6, 7: 7, 8: 9, 9: 11, 10: 13, 11: 14}
SUMMED, LAST = 6, 11
PAUSE = 3
END = NBLK - 1 + PAUSE
HALF = 28


def comm_scratch():
    def v(*shape, dtype=bf16):
        return pltpu.VMEM((*shape, 16, 128), dtype)

    return dict(
        blk=v(NS, 3, 112),
        r1=v(2, Q, 28),
        r2=v(2, Q, 14),
        r3=v(2, Q, 7),
        r4=v(2, Q, 4),
        r5=v(2, 3, 3, 2),
        s2=v(Q, 14),
        s3=v(Q, 7),
        s4=v(Q, 4),
        s5=v(3, 4, 2),
        k2=v(Q, 14, dtype=f32),
        k3=v(Q, 7, dtype=f32),
        k4=v(Q, 4, dtype=f32),
        k5=v(Q, 1, dtype=f32),
        g6=v(NG, 3, 4, 2),
        v7=v(NV, Q, 2, 4),
        mine=v(NO, Q, HALF),
        ssq=pltpu.VMEM((8, 128), f32),
        ssq_at=pltpu.VMEM((3, 4, 8, 128), f32),
        send=pltpu.SemaphoreType.DMA((4, Q)),
        recv=pltpu.SemaphoreType.DMA((4, 2, Q)),
        send5=pltpu.SemaphoreType.DMA((3, 3)),
        recv5=pltpu.SemaphoreType.DMA((2, 3, 3)),
        send6=pltpu.SemaphoreType.DMA((2, 3, 3)),
        recv6=pltpu.SemaphoreType.DMA((3, 3, 3)),
        send7=pltpu.SemaphoreType.DMA((3, 2, Q)),
        recv7=pltpu.SemaphoreType.DMA((3, 4, Q)),
        gsem=pltpu.SemaphoreType.DMA((2, Q)),
        qsend=pltpu.SemaphoreType.DMA((3, 3)),
        qrecv=pltpu.SemaphoreType.DMA((3, 3)),
    )


def parity(p):
    return lax.rem(lax.div(p + 1, 2), 2)


def upper(p):
    return lax.div(p, 2)


def position(me):
    return [lax.rem(lax.div(me, s), 4) for s in STRIDE]


def first_bits(me):
    pos = position(me)
    return [(parity, upper)[q % 2](pos[q // 2]) for q in range(Q)]


def add(*terms):
    total = terms[0].astype(f32)
    for t in terms[1:]:
        total = total + t.astype(f32)
    return total


class Comm:
    def __init__(self, refs, outs):
        self.__dict__.update(refs)
        self.outs = outs
        me = lax.axis_index("dp")
        pos = position(me)
        self.pos = pos
        self.near = []
        for p, s in zip(pos, STRIDE):
            base = me - p * s
            self.near.append((base + (p + 1 - 2 * lax.rem(p, 2)) * s, base + (3 - p) * s, base + lax.rem(p + 2, 4) * s))
        self.bits, self.peer = [], []
        for q in range(Q):
            j, w = divmod(q, 2)
            bits, peer = [], []
            for d in (j, (j + 1) % 3):
                for way in (w, 1 - w):
                    bits.append((parity, upper)[way](pos[d]))
                    peer.append(self.near[d][way])
            self.bits.append(bits)
            self.peer.append(peer)
        self.ssq[...] = jnp.zeros((8, 128), f32)

    def hello(self):
        for ring in self.near:
            for device in ring:
                pl.semaphore_signal(pltpu.get_barrier_semaphore(), inc=1, device_id={"dp": device}, device_id_type=MESH)

    def barrier(self):
        pl.semaphore_wait(pltpu.get_barrier_semaphore(), 9)

    def last(self, j):
        d = (j + 2) % 3
        p = self.pos[d]
        places = (p + 1 - 2 * lax.rem(p, 2), 3 - p, lax.rem(p + 2, 4))
        return p, tuple(zip(self.near[d], places))

    def copies(self, stage, b):
        s, bs, gs, vs, ms = lax.rem(b, 2), lax.rem(b, NS), lax.rem(b, NG), lax.rem(b, NV), lax.rem(b, NO)
        out = []
        if stage in (5, 6):
            for j in range(3):
                p, others = self.last(j)
                for way, (device, place) in enumerate(others):
                    if stage == 5:
                        ends = self.s5.at[j, place], self.r5.at[s, j, way], self.send5.at[j, way], self.recv5.at[s, j, way]
                    else:
                        part = self.g6.at[gs, j, p]
                        ends = part, part, self.send6.at[s, j, way], self.recv6.at[lax.rem(b, 3), j, way]
                    out.append((*ends, device))
        else:
            for q in range(Q):
                j, w = divmod(q, 2)
                b1, b2, b3, b4 = self.bits[q]
                if stage == 1:
                    src, dst = self.blk.at[bs, j, pl.ds(56 * w + 28 * (1 - b1), 28)], self.r1.at[s, q]
                elif stage == 2:
                    src, dst = self.s2.at[q], self.r2.at[s, q]
                elif stage == 3:
                    src, dst = self.s3.at[q], self.r3.at[s, q]
                elif stage == 4:
                    src, dst = self.s4.at[q], self.r4.at[s, q]
                elif stage == 7:
                    src = dst = self.v7.at[vs, q, b4]
                elif stage == 8:
                    src = dst = self.mine.at[ms, q, pl.ds(14 * b2 + 7 * b3, 7)]
                else:
                    src = dst = self.mine.at[ms, q, pl.ds(14 * b2, 14)]
                if stage < 5:
                    out.append((src, dst, self.send.at[stage - 1, q], self.recv.at[stage - 1, s, q], self.peer[q][stage - 1]))
                else:
                    out.append((src, dst, self.send7.at[stage - 7, s, q], self.recv7.at[stage - 7, lax.rem(b, 4), q], self.peer[q][10 - stage]))
        return [
            pltpu.make_async_remote_copy(src_ref=src, dst_ref=dst, send_sem=send, recv_sem=recv, device_id={"dp": device}, device_id_type=MESH)
            for src, dst, send, recv, device in out
        ]

    def math(self, stage, b):
        s, bs, gs, vs, ms = lax.rem(b, 2), lax.rem(b, NS), lax.rem(b, NG), lax.rem(b, NV), lax.rem(b, NO)
        for q in range(Q):
            j, w = divmod(q, 2)
            b1, b2, b3, b4 = self.bits[q]
            if stage == 2:
                for keep, at in ((True, 14 * b2), (False, 14 * (1 - b2))):
                    total = add(self.blk[bs, j, pl.ds(56 * w + 28 * b1 + at, 14)], self.r1[s, q, pl.ds(at, 14)])
                    if keep:
                        self.k2[q] = total
                    else:
                        self.s2[q] = total.astype(bf16)
            elif stage == 3:
                for keep, at in ((True, 7 * b3), (False, 7 * (1 - b3))):
                    total = add(self.k2[q, pl.ds(at, 7)], self.r2[s, q, pl.ds(at, 7)])
                    if keep:
                        self.k3[q] = total
                    else:
                        self.s3[q] = total.astype(bf16)
            elif stage == 4:
                for keep, at in ((True, 3 * b4), (False, 3 * (1 - b4))):
                    total = add(self.k3[q, pl.ds(at, 4)], self.r3[s, q, pl.ds(at, 4)])
                    if keep:
                        self.k4[q] = total
                    else:
                        self.s4[q] = total.astype(bf16)
            elif stage == 5:
                p, _ = self.last(j)
                self.k5[q] = add(self.k4[q, pl.ds(p, 1)], self.r4[s, q, pl.ds(p, 1)])
                self.s5[j, :, w] = add(self.k4[q], self.r4[s, q]).astype(bf16)
            elif stage == 6:
                p, _ = self.last(j)
                g = add(self.k5[q], *(self.r5[s, j, way, pl.ds(w, 1)] for way in range(3))).astype(bf16)
                self.g6[gs, j, p, pl.ds(w, 1)] = g
                square = g.astype(f32).reshape(2, 8, 128)
                square = square * square
                counts = jnp.where((b4 == 1) & (p == 0), 0.0, 1.0)
                self.ssq[...] += (square[0] + square[1]) * counts
            elif stage == 7:
                self.v7[vs, q, b4] = self.g6[gs, j, :, w]
            elif stage == 8:
                self.mine[ms, q, pl.ds(14 * b2 + 7 * b3, 4)] = self.v7[vs, q, 0]
                self.mine[ms, q, pl.ds(14 * b2 + 7 * b3 + 4, 3)] = self.v7[vs, q, 1, 1:4]

    def out(self, b):
        return [pltpu.make_async_copy(self.mine.at[lax.rem(b, NO), q], self.outs[q].at[b], self.gsem.at[lax.rem(b, 2), q]) for q in range(Q)]

    def stage(self, k, b):
        if 2 <= k <= 10:
            for c in self.copies(k - 1, b):
                c.wait()
        if k <= 9:
            self.math(k, b)
            for c in self.copies(k, b):
                c.start()
        elif k == 10:
            for c in self.out(b):
                c.start()
        else:
            for c in self.out(b):
                c.wait()

    def service(self, tick):
        for k in (*range(SUMMED, 0, -1), *range(LAST, SUMMED, -1)):
            made = tick - DUE[k]
            late = made >= NB + PAUSE
            now = (made >= 0) & (made <= END) & (late | (made < NB))
            pl.when(now)(functools.partial(self.stage, k, jnp.where(late, made - PAUSE, made)))

    def total(self, step):
        def copies(d):
            part = self.ssq_at.at[d, self.pos[d]]
            return [
                pltpu.make_async_remote_copy(
                    src_ref=part,
                    dst_ref=part,
                    send_sem=self.qsend.at[d, way],
                    recv_sem=self.qrecv.at[d, way],
                    device_id={"dp": device},
                    device_id_type=MESH,
                )
                for way, device in enumerate(self.near[d])
            ]

        if step > 0:
            for c in copies(step - 1):
                c.wait()
            self.ssq[...] = add(*(self.ssq_at[step - 1, k] for k in range(4)))
        if step < 3:
            self.ssq_at[step, self.pos[step]] = self.ssq[...]
            for c in copies(step):
                c.start()


def gradients(names, x_hbm, dy_hbm, wg, wu, wd, *rest):
    outs, (ssq_out, s_hbm, ds_hbm, a0t_hbm, dgu_hbm), scratch = rest[:Q], rest[Q : Q + 5], rest[Q + 5 :]
    refs = dict(zip(names, scratch, strict=True))
    h, dy, a, a_t, dy_t, wgu, wdb, wd0, act0, dgu, sb, ub, xsem, isem, wsem, osem, tsem, dsem = (refs.pop(n) for n in OWN)
    comm = Comm(refs, outs)
    comm.hello()

    def fetch(layer, b, slot):
        return (
            pltpu.make_async_copy(wg.at[layer, :, block(b)], wgu.at[slot, :, 0:FB], wsem.at[slot, 0]),
            pltpu.make_async_copy(wu.at[layer, :, block(b)], wgu.at[slot, :, FB : 2 * FB], wsem.at[slot, 1]),
            *([pltpu.make_async_copy(wd.at[layer, block(b), :], wdb.at[slot], wsem.at[slot, 2])] if layer else []),
        )

    def part(t):
        return pltpu.make_async_copy(x_hbm.at[rows(t), :], h.at[rows(t), :], xsem.at[t])

    for t in range(NT):
        part(t).start()
    for c in fetch(0, 0, 0):
        c.start()
    get_dy = pltpu.make_async_copy(dy_hbm, dy, isem.at[0])
    get_dy.start()
    get_wd = pltpu.make_async_copy(wd.at[0], wd0, isem.at[1])
    get_wd.start()

    @pl.loop(0, NT)
    def _(t):
        part(t).wait()
        x = h[rows(t), :].astype(f32)
        a[rows(t), :] = (x * norm_scale(x)).astype(bf16)

    get_dy.wait()

    def kept(b, slot):
        return (
            pltpu.make_async_copy(sb.at[slot], s_hbm.at[b], osem.at[slot, 0]),
            pltpu.make_async_copy(ub.at[slot], ds_hbm.at[b], osem.at[slot, 1]),
        )

    def kept_t(t):
        return pltpu.make_async_copy(a_t.at[:, rows(t)], a0t_hbm.at[:, rows(t)], tsem.at[t])

    @pl.loop(0, NB)
    def _(b):
        slot = lax.rem(b, 2)

        @pl.when(b + 1 < NB)
        def _():
            for c in fetch(0, b + 1, 1 - slot):
                c.start()

        @pl.when(b >= 2)
        def _():
            for c in kept(b - 2, slot):
                c.wait()

        @pl.when((b >= 1) & (b < NT))
        def _():
            kept_t(b - 1).start()

        for c in fetch(0, b, slot):
            c.wait()
        turn = rows(jnp.minimum(b, NT - 1))
        a_t[:, turn] = a[turn, :].T
        dy_t[:, turn] = dy[turn, :].T
        for t in range(NT):
            r = pl.ds(t * TM, TM)
            both = dot(a[r, :], wgu[slot])
            gate, up = both[:, :FB], both[:, FB:]
            sg = sigmoid(gate)
            s = gate * sg
            act0[r, block(b)] = (s * up).astype(bf16)
            sb[slot, r, :] = s
            ub[slot, r, :] = up * (sg + (s - s * sg))
        for c in kept(b, slot):
            c.start()

    kept_t(NT - 1).start()
    for c in fetch(1, 0, 0):
        c.start()
    for t in range(NT):
        kept_t(t).wait()
    get_wd.wait()
    for t in range(NT):
        r = pl.ds(t * TM, TM)
        new = h[r, :] + dot(act0[r, :], wd0[...]).astype(bf16)
        h[r, :] = new
        new = new.astype(f32)
        new = (new * norm_scale(new)).astype(bf16)
        a[r, :] = new
        a_t[:, r] = new.T
    for b in (NB - 2, NB - 1):
        for c in kept(b, b % 2):
            c.wait()
    comm.barrier()

    def give(slot, d_gate_up, act):
        for start, size in ((0, 512), (512, D - 512)):
            g = dot(a_t[start : start + size, :], d_gate_up).astype(bf16)
            for j in range(2):
                for n in range(size // 8):
                    band, half = divmod(n, 2)
                    comm.blk[slot, j, start // 8 + n] = g[16 * band : 16 * band + 16, FB * j + 128 * half : FB * j + 128 * half + 128]
        for start, size in ((0, 512), (512, D - 512)):
            g = dot(dy_t[start : start + size, :], act).astype(bf16).T
            for band in range(16):
                for c in range(size // 128):
                    comm.blk[slot, 2, 7 * band + start // 128 + c] = g[16 * band : 16 * band + 16, 128 * c : 128 * c + 128]

    def keep_dgu(b):
        return pltpu.make_async_copy(dgu.at[lax.rem(b, 2)], dgu_hbm.at[b], dsem.at[lax.rem(b, 2)])

    @pl.loop(0, NB)
    def _(b):
        comm.service(b)
        slot = lax.rem(b, 2)

        @pl.when(b + 1 < NB)
        def _():
            for c in fetch(1, b + 1, 1 - slot):
                c.start()

        @pl.when(b >= 2)
        def _():
            keep_dgu(b - 2).wait()

        for c in fetch(1, b, slot):
            c.wait()
        for t in range(T // TB):
            r = pl.ds(t * TB, TB)
            both = dot(a[r, :], wgu[slot])
            gate, up = both[:, :FB], both[:, FB:]
            dact = dot_t(dy[r, :], wdb[slot]).astype(bf16).astype(f32)
            sg = sigmoid(gate)
            s = gate * sg
            sb[0, r, :] = (s * up).astype(bf16).astype(f32)
            dgu[slot, r, :FB] = (dact * up * (sg + (s - s * sg))).astype(bf16)
            dgu[slot, r, FB:] = (dact * s).astype(bf16)
        give(lax.rem(b, NS), dgu[slot], sb[0].astype(bf16))

        @pl.when(b < NB - 2)
        def _():
            keep_dgu(b).start()

    da = [(ref, k, min(FB, D - FB * (2 * i + k))) for i, ref in enumerate((sb, ub)) for k in range(2)]

    def again_dgu(i):
        b, slot = NB - 1 - i, lax.rem(i, 2)
        return (*fetch(1, b, slot)[:2], pltpu.make_async_copy(dgu_hbm.at[b], dgu.at[slot], dsem.at[slot]))

    @pl.loop(0, PAUSE)
    def _(n):
        comm.service(n + NB)

        @pl.loop(n * (NB // PAUSE), (n + 1) * (NB // PAUSE))
        def _(i):
            slot = lax.rem(i, 2)

            @pl.when((i >= 1) & (i + 1 < NB))
            def _():
                for c in again_dgu(i + 1):
                    c.start()

            @pl.when(i >= 2)
            def _():
                for c in again_dgu(i):
                    c.wait()

            for t in range(T // TB):
                r = pl.ds(t * TB, TB)
                more = dot_t(dgu[slot, r, :], wgu[slot])
                for f, (ref, part_of, size) in enumerate(da):
                    ref[part_of, r, :size] = jnp.where(i > 0, ref[part_of, r, :size], 0.0) + more[:, FB * f : FB * f + size]

    again = pltpu.make_async_copy(a0t_hbm, a_t, isem.at[0])
    again.start()

    def back(b, slot, r=slice(None)):
        return (
            pltpu.make_async_copy(s_hbm.at[b, r], sb.at[slot, r], osem.at[slot, 0]),
            pltpu.make_async_copy(ds_hbm.at[b, r], ub.at[slot, r], osem.at[slot, 1]),
        )

    @pl.loop(0, NT)
    def _(t):
        x = h[rows(t), :].astype(f32)
        scale = norm_scale(x)
        g = jnp.concatenate([ref[k, rows(t), :n] for ref, k, n in da], axis=1).astype(bf16).astype(f32)
        along = jnp.mean(g * x, -1, keepdims=True)
        dh = (g * scale - x * (scale * scale * scale * along)).astype(bf16) + dy[rows(t), :]
        dy[rows(t), :] = dh
        dy_t[:, rows(t)] = dh.T
        for c in back(0, 0, rows(t)):
            c.start()

    again.wait()

    @pl.loop(0, NB)
    def _(b):
        comm.service(b + NB + PAUSE)
        slot = lax.rem(b, 2)

        @pl.when(b + 1 < NB)
        def _():
            for c in back(b + 1, 1 - slot):
                c.start()

        for c in back(b, slot):
            c.wait()
        for t in range(T // TB):
            r = pl.ds(t * TB, TB)
            dact = dot_t(dy[r, :], wd0[block(b), :]).astype(bf16).astype(f32)
            dgu[0, r, :FB] = (dact * ub[slot, r, :]).astype(bf16)
            dgu[0, r, FB:] = (dact * sb[slot, r, :]).astype(bf16)
        give(lax.rem(b + NB, NS), dgu[0], act0[:, block(b)])

    @pl.loop(END + 1, END + DUE[LAST] + 1)
    def _(tick):
        comm.service(tick)
        for step in range(4):
            pl.when(tick == END + SUMMED + 2 * step)(functools.partial(comm.total, step))

    ssq_out[...] = comm.ssq[...]


OWN = ("h", "dy", "a", "a_t", "dy_t", "wgu", "wdb", "wd0", "act0", "dgu", "sb", "ub", "xsem", "isem", "wsem", "osem", "tsem", "dsem")


def run_gradients(x, dy, wg, wu, wd):
    own = dict(
        h=pltpu.VMEM((T, D), bf16),
        dy=pltpu.VMEM((T, D), bf16),
        a=pltpu.VMEM((T, D), bf16),
        a_t=pltpu.VMEM((D, T), bf16),
        dy_t=pltpu.VMEM((D, T), bf16),
        wgu=pltpu.VMEM((2, D, 2 * FB), bf16),
        wdb=pltpu.VMEM((2, FB, D), bf16),
        wd0=pltpu.VMEM((F, D), bf16),
        act0=pltpu.VMEM((T, F), bf16),
        dgu=pltpu.VMEM((2, T, 2 * FB), bf16),
        sb=pltpu.VMEM((2, T, FB), f32),
        ub=pltpu.VMEM((2, T, FB), f32),
        xsem=pltpu.SemaphoreType.DMA((NT,)),
        isem=pltpu.SemaphoreType.DMA((2,)),
        wsem=pltpu.SemaphoreType.DMA((2, 3)),
        osem=pltpu.SemaphoreType.DMA((2, 2)),
        tsem=pltpu.SemaphoreType.DMA((NT,)),
        dsem=pltpu.SemaphoreType.DMA((2,)),
    )
    scratch = own | comm_scratch()
    kept = sds((NB, T, FB), f32)
    *mine, ssq, _, _, _, _ = pl.pallas_call(
        functools.partial(gradients, tuple(scratch)),
        name="gradients",
        out_shape=(*(sds((NBLK, HALF, 16, 128), bf16) for _ in range(Q)), sds((8, 128), f32), kept, kept, sds((D, T), bf16), sds((NB, T, 2 * FB), bf16)),
        in_specs=[ANY] * 5,
        out_specs=(*(ANY for _ in range(Q)), VMEM, ANY, ANY, ANY, ANY),
        scratch_shapes=list(scratch.values()),
        compiler_params=pltpu.CompilerParams(collective_id=0, has_side_effects=True, vmem_limit_bytes=VMEM_LIMIT),
    )(x, dy, wg, wu, wd)
    return mine, ssq


SPLIT = 1
PER = LAYERS * 2 * (NB // SPLIT)
STEPS = 2 * PER
INS, OUTS = 8, 6
SHAPES = ((112, SPLIT * FB), (112, SPLIT * FB), (SPLIT, 32, D))


def adamw(other, ssq_ref, *refs):
    gs, arrays, refs = refs[:Q], refs[Q : Q + 9], refs[Q + 9 :]
    if other:
        refs = refs[9:]
    results, g_buf, in_buf, out_buf, (gsem, isem, osem) = refs[:9], refs[9], refs[10:19], refs[19:28], refs[28:]
    factor = jnp.minimum(1.0, 0.5 * lax.rsqrt(jnp.sum(ssq_ref[...], keepdims=True) / COUNT + 1e-30))
    bits = first_bits(lax.axis_index("dp"))

    def place(t):
        w, t = lax.div(t, PER), lax.rem(t, PER)
        n, t = lax.div(t, 2 * NB // SPLIT), lax.rem(t, 2 * NB // SPLIT)
        return w, n, lax.div(t, NB // SPLIT), lax.rem(t, NB // SPLIT)

    def window(t, k, ref):
        w, n, i, f = place(t)
        half = jnp.where(w == 0, bits[2 * k], bits[2 * k + 1])
        row = 4 * w + 2 * (1 - half if other else half) + i
        if k < 2:
            return ref.at[1 - n, pl.ds(pl.multiple_of(row * 112, 16), 112), pl.ds(pl.multiple_of(f * SPLIT * FB, 128), SPLIT * FB)]
        return ref.at[1 - n, pl.ds(f * SPLIT, SPLIT), pl.ds(pl.multiple_of(row * 32, 16), 32), :]

    def inward(t):
        s = lax.rem(t, INS)
        return [pltpu.make_async_copy(window(t, k % 3, arrays[k]), in_buf[k].at[s], isem.at[s, k]) for k in range(9)]

    def g_inward(t, w):
        s = lax.rem(t, INS)
        _, n, i, f = place(t)
        at = pl.ds(n * NB + f * SPLIT, SPLIT), pl.ds(14 * i, 14)
        return [pltpu.make_async_copy(gs[2 * k + w].at[at], g_buf.at[s, k], gsem.at[s, k]) for k in range(3)]

    def outward(t):
        s = lax.rem(t, OUTS)
        return [pltpu.make_async_copy(out_buf[k].at[s], window(t, k % 3, results[k]), osem.at[s, k]) for k in range(9)]

    def fetch(t):
        for c in inward(t):
            c.start()
        for w in range(2):

            @pl.when(lax.div(t, PER) == w)
            def _():
                for c in g_inward(t, w):
                    c.start()

    for t in range(INS - 1):
        fetch(t)

    @pl.loop(0, STEPS)
    def _(t):
        s, o = lax.rem(t, INS), lax.rem(t, OUTS)

        @pl.when(t + INS - 1 < STEPS)
        def _():
            fetch(t + INS - 1)

        @pl.when(t >= OUTS)
        def _():
            for c in outward(t - OUTS):
                c.wait()

        for c in inward(t) + g_inward(t, 0):
            c.wait()

        def update(k, where, g):
            weight, m, v = (in_buf[i + k][(s, *where)].astype(f32) for i in (0, 3, 6))
            g = g.astype(f32) * factor
            m = 0.9 * m + 0.1 * g
            v = 0.95 * v + 0.05 * g * g
            step = m * lax.rsqrt(v + 1e-8) + 0.1 * weight
            out_buf[k][(o, *where)] = (weight - 0.02 * step).astype(bf16)
            out_buf[3 + k][(o, *where)] = m
            out_buf[6 + k][(o, *where)] = v

        for b in range(SPLIT):
            for k in range(3):
                if k < 2:
                    g = g_buf[s, k, b].reshape(7, 2, 16, 128)
                    for half in range(2):
                        update(k, (slice(None), slice(b * FB + half * 128, b * FB + half * 128 + 128)), g[:, half].reshape(112, 128))
                else:
                    g = g_buf[s, k, b].reshape(2, 7, 16, 128)
                    for c in range(7):
                        update(k, (b, slice(None), slice(c * 128, c * 128 + 128)), g[:, c].reshape(32, 128))
        for c in outward(t):
            c.start()

    for t in range(STEPS - OUTS, STEPS):
        for c in outward(t):
            c.wait()


def run_adamw(other, ssq, gs, arrays, so_far):
    arrays = [a.reshape(LAYERS, NB, FB, D) if k % 3 == 2 else a for k, a in enumerate(arrays)]

    def held(n):
        return [pltpu.VMEM((n, *SHAPES[k % 3]), arrays[k].dtype) for k in range(9)]

    return pl.pallas_call(
        functools.partial(adamw, other),
        name="adamw",
        in_specs=[VMEM] + [ANY] * (Q + 9 + len(so_far)),
        out_specs=(ANY,) * 9,
        out_shape=tuple(sds(a.shape, a.dtype) for a in arrays),
        scratch_shapes=[
            pltpu.VMEM((INS, 3, SPLIT, 14, 16, 128), bf16),
            *held(INS),
            *held(OUTS),
            pltpu.SemaphoreType.DMA((INS, 3)),
            pltpu.SemaphoreType.DMA((INS, 9)),
            pltpu.SemaphoreType.DMA((OUTS, 9)),
        ],
        input_output_aliases={1 + Q + 9 + k: k for k in range(len(so_far))},
        cost_estimate=pl.CostEstimate(flops=100_000_000_000, bytes_accessed=136_000_000, transcendentals=0),
        compiler_params=pltpu.CompilerParams(vmem_limit_bytes=VMEM_LIMIT),
    )(ssq, *gs, *arrays, *so_far)


def swaps(q):
    j, w = divmod(q, 2)
    s = STRIDE[j]
    out = []
    for me in range(64):
        p = me // s % 4
        out.append((me, me + ((3 - p if w else p ^ 1) - p) * s))
    return out


def solution(mesh):
    def step(x, dy, *arrays):
        mine, ssq = run_gradients(x[0], dy[0], *arrays[:3])
        theirs = [lax.ppermute(g, "dp", swaps(q)) for q, g in enumerate(mine)]
        new = run_adamw(False, ssq, mine, arrays, ())
        new = run_adamw(True, ssq, theirs, arrays, new)
        return tuple(n.reshape(a.shape) for n, a in zip(new, arrays, strict=True))

    return jax.shard_map(
        step,
        mesh=mesh,
        in_specs=(P(("rep", "dp"), None, None),) * 2 + (P(None, None, None),) * 9,
        out_specs=(P("rep", None, None),) * 9,
        check_vma=False,
    )
```
